128 devices in a mesh: gx: 8 (over x, z_lo), gy: 16 (over z_hi, y, core).
Axes of the slice: x: 4, y: 4, z: 4 (z_hi: 2, z_lo: 2; z = z_hi * 2 + z_lo), core: 2. Of those that a mesh axis runs over, the one named last changes fastest.
Arguments:
- velocity: float32 [2, 4096, 8192], P(None, 'gx', 'gy'), may hold values from -3 to 3
- stress: float32 [3, 4096, 8192], P(None, 'gx', 'gy'), may hold values from -3 to 3
- strength: float32 [4096, 8192], P('gx', 'gy'), may hold values from 0.5 to 4
- ice_mass: float32 [4096, 8192], P('gx', 'gy'), may hold values from 0.3 to 20, as said below
- wind_stress: float32 [2, 4096, 8192], P(None, 'gx', 'gy'), may hold values from -6 to 6
- current: float32 [2, 4096, 8192], P(None, 'gx', 'gy'), may hold values from -3 to 3
- ice_mask: int32 [4096, 8192], P('gx', 'gy'), may hold values from 0 to 1, as said below
- open_water: int32 [4096, 8192], P('gx', 'gy'), may hold values 0 or 1
Outputs:
- new_velocity: float32 [2, 4096, 8192], P(None, 'gx', 'gy')
- new_stress: float32 [3, 4096, 8192], P(None, 'gx', 'gy')
- residual: float32 [], replicated
- kinetic_energy: float32 [], replicated
The draws below stay inside these ranges and needn't reach their ends.
Inputs may be any that keep to these rules, and one draw needn't show every extreme that they name: `ice_mask`: 1 marks an ocean cell, 0 a land cell. `ice_mass`: positive everywhere.
All inputs are finite; a program needn't handle non-finite values. No bound on the sum of `open_water` on one device may be relied on, other than what follows from the above.
Results may differ from the reference program's by a relative error of at most 0.00002.
Values sent between devices are 32-bit elements; how exact they have to be, the bound alone decides.
No kernel may reach another device: no remote copies, remote signals or barrier semaphores. Data moves between devices by JAX's collectives and lax.ppermute only.
A program may use at most 128 MiB of HBM per device.

```python
import math
import jax
import jax.numpy as jnp

ITERS = 4
NX = 4096
NY = 8192


def draw_ice_mass(key, part):
    row_ramp = 1.0 + 2.0 * jnp.arange(NX, dtype=jnp.float32) / NX
    col_ramp = 1.0 + 2.0 * jnp.arange(NY, dtype=jnp.float32) / NY
    ramp = row_ramp[:, None] * col_ramp[None, :]
    rough = jax.random.uniform(key, (NX, NY), jnp.float32, 0.6, 1.4)
    return (ramp * rough).astype(jnp.float32)


def draw_ice_mask(key, part):
    row_index = jnp.arange(NX, dtype=jnp.int32)[:, None]
    col_index = jnp.arange(NY, dtype=jnp.int32)[None, :]
    land_cells = jnp.zeros((NX, NY), jnp.int32)
    for number in range(8):
        key_a, key_b, key_c, key_d = jax.random.split(jax.random.fold_in(key, number + 11), 4)
        start_x = jax.random.randint(key_a, (), 0, NX)
        width_x = jax.random.randint(key_b, (), 1, max(NX // 4, 2))
        start_y = jax.random.randint(key_c, (), 0, NY)
        width_y = jax.random.randint(key_d, (), 1, max(NY // 4, 2))
        inside = (row_index >= start_x) & (row_index < start_x + width_x) & (col_index >= start_y) & (col_index < start_y + width_y)
        land_cells = jnp.maximum(land_cells, inside.astype(jnp.int32))
    speckle = (jax.random.randint(jax.random.fold_in(key, 97), (NX, NY), 0, 16) == 0).astype(jnp.int32)
    land_cells = jnp.maximum(land_cells, speckle)
    return (1 - land_cells).astype(jnp.int32)


def set_ends(entries, own_key, low, high):
    longest = entries.shape.index(max(entries.shape))
    spots = []
    for shift in (0, 1):
        where = [jax.random.randint(jax.random.fold_in(own_key, axis), (), 0, length) for axis, length in enumerate(entries.shape)]
        where[longest] = (where[longest] + shift) % entries.shape[longest]
        spots.append(tuple(where))
    return entries.at[spots[0]].set(low).at[spots[1]].set(high)


def levels(key, extent, shards, smallest, high):
    level, own = 1.0, jax.random.fold_in(key, 6)
    for dim, blocks in shards:
        heights = jnp.exp(jax.random.uniform(jax.random.fold_in(own, dim), (blocks,), jnp.float32, smallest / len(shards), high / len(shards)))
        level = level * jnp.repeat(heights, extent[dim] // blocks).reshape([-1 if axis == dim else 1 for axis in range(len(extent))])
    return level


def normal_values(rng, dims, deviation, most, cuts=(), kind=jnp.bfloat16):
    level = levels(rng, dims, cuts, -0.22, 0.18) if cuts else 1.0
    drawn = jax.random.normal(rng, dims, jnp.float32) * deviation * level
    return jnp.minimum(jnp.maximum(drawn, -most), most).astype(kind)


def setup_inputs(seed: int = 0) -> dict:
    key_of = jax.random.split(jax.random.key(seed), 9)
    velocity = normal_values(key_of[0], (2, NX, NY), 0.5, 3.0, ((1, 8), (2, 16)), jnp.float32)
    stress = normal_values(key_of[1], (3, NX, NY), 0.5, 3.0, ((1, 8), (2, 16)), jnp.float32)
    strength = jnp.clip(jnp.exp(math.log(4.0) - 2.0794415 * jax.random.uniform(key_of[2], (NX, NY), jnp.float32) ** levels(key_of[2], (NX, NY), ((0, 8), (1, 16)), -0.2, 0.2)), 0.5, 4.0)
    ice_mass = draw_ice_mass(jax.random.fold_in(key_of[8], 71), 0)
    wind_stress = normal_values(key_of[4], (2, NX, NY), 1.0, 6.0, ((1, 8), (2, 16)), jnp.float32)
    current = normal_values(key_of[5], (2, NX, NY), 0.5, 3.0, ((1, 8), (2, 16)), jnp.float32)
    ice_mask = draw_ice_mask(jax.random.fold_in(key_of[8], 71), 0)
    open_water = set_ends((jax.random.randint(key_of[7], (NX, NY), 0, 8) < 1).astype(jnp.int32), jax.random.fold_in(key_of[7], 1), 0, 1)
    return {"velocity": velocity, "stress": stress, "strength": strength, "ice_mass": ice_mass, "wind_stress": wind_stress, "current": current, "ice_mask": ice_mask, "open_water": open_water}


relax_rate = 0.8
ecc_square = 4.0
delta_floor = 0.05
time_step = 0.5
drag_coef = 1.0
coriolis = 0.3

def corner_diffs(values):
    along_x = (values[1:, 1:] + values[1:, :-1] - values[:-1, 1:] - values[:-1, :-1]) * 0.5
    along_y = (values[1:, 1:] + values[:-1, 1:] - values[1:, :-1] - values[:-1, :-1]) * 0.5
    return (along_x, along_y)

def update_stress(velocity, stress, pressure):
    du_dx, du_dy = corner_diffs(velocity[0])
    dv_dx, dv_dy = corner_diffs(velocity[1])
    divu = du_dx + dv_dy
    tension = du_dx - dv_dy
    shear = du_dy + dv_dx
    deform = jnp.sqrt(divu * divu + (tension * tension + shear * shear) / ecc_square + delta_floor * delta_floor)
    viscous = pressure / deform
    first = (stress[0] + relax_rate * viscous * (divu - deform)) / (1.0 + relax_rate)
    second = (stress[1] + relax_rate * viscous * tension / ecc_square) / (1.0 + relax_rate)
    third = (stress[2] + relax_rate * viscous * shear * 0.5 / ecc_square) / (1.0 + relax_rate)
    return jnp.stack([first, second, third])

def stress_force(stress):
    normal_x = 0.5 * (stress[0] + stress[1])
    normal_y = 0.5 * (stress[0] - stress[1])
    normal_x_dx, unused_x = corner_diffs(normal_x)
    unused_y, normal_y_dy = corner_diffs(normal_y)
    shear_dx, shear_dy = corner_diffs(stress[2])
    return (normal_x_dx + shear_dy, shear_dx + normal_y_dy)

def advance(velocity, force_x, force_y, ice_mass, wind_stress, current, ice_weight):
    inertia = ice_mass / time_step
    diagonal = inertia + drag_coef
    turning = ice_mass * coriolis
    rhs_u = inertia * velocity[0] + force_x + wind_stress[0] + drag_coef * current[0]
    rhs_v = inertia * velocity[1] + force_y + wind_stress[1] + drag_coef * current[1]
    determinant = diagonal * diagonal + turning * turning
    new_u = (diagonal * rhs_u + turning * rhs_v) / determinant * ice_weight
    new_v = (diagonal * rhs_v - turning * rhs_u) / determinant * ice_weight
    return jnp.stack([new_u, new_v])

def reference(velocity, stress, strength, ice_mass, wind_stress, current, ice_mask, open_water):
    ice_weight = ice_mask.astype(jnp.float32) * (1.0 - open_water.astype(jnp.float32))
    pressure = strength * ice_weight
    previous = velocity
    for subcycle in range(ITERS):
        padded = jnp.pad(velocity, ((0, 0), (1, 0), (1, 0)))
        stress = update_stress(padded, stress, pressure)
        force_x, force_y = stress_force(jnp.pad(stress, ((0, 0), (0, 1), (0, 1))))
        previous = velocity
        velocity = advance(velocity, force_x, force_y, ice_mass, wind_stress, current, ice_weight)
    change = velocity - previous
    residual = jnp.sum(ice_weight * (change[0] * change[0] + change[1] * change[1])) / (NX * NY)
    kinetic = 0.5 * jnp.sum(ice_mass * ice_weight * (velocity[0] * velocity[0] + velocity[1] * velocity[1])) / (NX * NY)
    return (velocity, stress, residual, kinetic)
```

```python
import functools

import jax
import jax.numpy as jnp
from jax import lax
from jax.experimental import pallas as pl
from jax.experimental.pallas import tpu as pltpu
from jax.sharding import PartitionSpec as P

ITERS = 4
RELAX = 0.8
GROW = 1.0 / (1.0 + RELAX)
KAPPA = RELAX / (1.0 + RELAX)
PAD = 8
F32 = jnp.float32
(U_, V_, H1, H2, H12, K_, M8, FU, FV, CA, CB) = range(11)
NS = 9
NF = 11
ALL = ("gx", "gy")


def weight_of(mask, openw):
    return mask.astype(F32) * (1.0 - openw.astype(F32))


def consts(strength, mass, wind, cur, weight):
    return (KAPPA * strength) * weight, mass * 8.0, 4.0 * (wind[0] + cur[0]), 4.0 * (wind[1] + cur[1])


def coefs(m8, weight):
    a = m8 * 0.25 + 1.0
    b = m8 * 0.0375
    scale = (0.25 * weight) / (a * a + b * b)
    return a * scale, b * scale


def strain(u, v, um, vm):
    su = u + um
    du = u - um
    sv = v + vm
    dv = v - vm
    return su + dv, su - dv, du + sv, du - sv


def stress_rate(alpha, beta, gamma, alpha_m, beta_m, delta_m, k):
    d = alpha - beta_m
    t = beta - alpha_m
    s = gamma + delta_m
    q = d * d + 0.25 * (t * t + s * s) + 0.01
    r = lax.rsqrt(q)
    z = k * r
    z4 = 0.25 * z
    return z * (d - q * r), z4 * t, z4 * s


def mixes(h1, h2, h12):
    e = h1 + h2
    g = h1 - h2
    return e + h12, e - h12, h12 + g, h12 - g


def drift(u, v, fx, fy, m8, fu, fv, ca, cb):
    ru = m8 * u + (fx + fu)
    rv = m8 * v + (fy + fv)
    return ca * ru + cb * rv, ca * rv - cb * ru


def pair_rows(parts, high):
    half = lax.broadcasted_iota(jnp.int32, parts[0].shape, 0) < 4
    tiles = []
    for f in range(0, NS, 2):
        a = parts[f]
        b = parts[f + 1] if f + 1 < NS else jnp.zeros_like(a)
        if high:
            tiles.append(jnp.where(half, pltpu.roll(a, 4, 0), b))
        else:
            tiles.append(jnp.where(half, a, pltpu.roll(b, 4, 0)))
    return jnp.concatenate(tiles, 0)


def unpair(tiles, f, high):
    x = tiles[8 * (f // 2) : 8 * (f // 2) + 8]
    return x if (f % 2 == 1) == high else pltpu.roll(x, 4, 0)


def is_even(axis):
    return lax.axis_index(axis) % 2 == 0


def strip_fields(vel, strs, strength, mass, wind, cur, mask, openw):
    w = weight_of(mask[...], openw[...])
    k, m8, fu, fv = consts(strength[...], mass[...], (wind[0], wind[1]), (cur[0], cur[1]), w)
    return [vel[0], vel[1], strs[0], strs[1], 2.0 * strs[2], k, m8, fu, fv]


def rows_kernel(*refs):
    own, msg_a, msg_b = refs[16:]
    top = strip_fields(*refs[:8])
    bot = strip_fields(*refs[8:16])
    for f in range(NS):
        own[f, 0:8, :] = top[f]
        own[f, 8:16, :] = bot[f]
    low = pair_rows(top, False)
    high = pair_rows(bot, True)
    even = is_even("gx")
    msg_a[...] = jnp.where(even, high, low)
    msg_b[...] = jnp.where(even, low, high)


def cols_kernel(*refs):
    out = refs[16]
    lane = lax.broadcasted_iota(jnp.int32, (128, 128), 1)
    for side in range(2):
        fields = strip_fields(*refs[8 * side : 8 * side + 8])
        x = jnp.zeros((128, 128), F32)
        for f in range(NS):
            shift = (8 * f - 120 * side) % 128
            y = pltpu.roll(fields[f], shift, 1) if shift else fields[f]
            x = jnp.where((lane >= 8 * f) & (lane < 8 * f + 8), y, x)
        out[8 * NS * side : 8 * NS * (side + 1), :] = x.T[0 : 8 * NS]


def corners_kernel(cols, xa, xb, ya, yb, ext):
    even = is_even("gx")
    a, b = xa[...], xb[...]
    top = jnp.where(even, b, a)
    bot = jnp.where(even, a, b)
    C = cols.shape[1]
    lane = lax.broadcasted_iota(jnp.int32, (8, 128), 1)
    strips = []
    for side in range(2):
        at = side * (C - 128)
        t = jnp.concatenate([top[:, at : at + 128], bot[:, at : at + 128], jnp.zeros((48, 128), F32)], 0).T
        t = t[120 * side : 120 * side + 8]
        own = []
        for f in range(NS):
            e = jnp.where(lane >= 124, pltpu.roll(t, 124 - 4 * f, 1), 0.0)
            e = jnp.where(lane < 4, pltpu.roll(t, 128 - 40 - 4 * f, 1), e)
            base = 8 * (NS * side + f)
            ext[base : base + 8, :] = e
            own.append(jnp.concatenate([cols[base : base + 8, :], e], 1))
        strips.append(pair_rows(own, side == 1))
    low, high = strips
    even = is_even("gy")
    ya[...] = jnp.where(even, high, low)
    yb[...] = jnp.where(even, low, high)


def interior_kernel(vel, strs, strength, mass, wind, cur, mask, openw, nvel, nstr, sums, buf, ibuf, al, be, ga, de, tx, ty, nx, ny, insem, outsem, *, RB, NCH):
    R = vel.shape[1]
    NT = vel.shape[2] // 128
    CH = R // NCH

    srcs = [(vel, 0, U_), (vel, 1, V_), (strs, 0, H1), (strs, 1, H2), (strs, 2, H12), (strength, None, K_), (mass, None, M8),
            (wind, 0, FU), (wind, 1, FV), (cur, 0, CA), (cur, 1, CB)]

    for c in range(NCH):
        rows = pl.ds(c * CH, CH)
        rows_b = pl.ds(PAD + c * CH, CH)
        for t in range(NT):
            cols = pl.ds(t * 128, 128)
            for ref, lead, f in srcs:
                src = ref.at[rows, cols] if lead is None else ref.at[lead, rows, cols]
                pltpu.make_async_copy(src, buf.at[f, t, rows_b, :], insem.at[c]).start()
            for n, ref in enumerate((mask, openw)):
                pltpu.make_async_copy(ref.at[rows, cols], ibuf.at[n, t, rows, :], insem.at[NCH + c]).start()
    zero = jnp.zeros((8, 128), F32)
    for t in range(NT):
        for ref in (al, be, de):
            ref[t, 0:PAD, :] = zero
        for ref in (tx, ty):
            ref[t, PAD + R : PAD + R + 8, :] = zero
    lane = lax.broadcasted_iota(jnp.int32, (RB, 128), 1)
    row_in = lax.broadcasted_iota(jnp.int32, (RB, 128), 0)
    first = lane == 0
    last = lane == 127

    def shift_m(x):
        r = [pltpu.roll(a, 1, 1) for a in x]
        return [jnp.where(first, r[(t - 1) % NT], r[t]) for t in range(NT)]

    def shift_p(x):
        r = [pltpu.roll(a, 127, 1) for a in x]
        return [jnp.where(last, r[(t + 1) % NT], r[t]) for t in range(NT)]

    def prepare(r0):
        rows = pl.ds(PAD + r0, RB)
        irows = pl.ds(r0, RB)
        for t in range(NT):
            w = weight_of(ibuf[0, t, irows, :], ibuf[1, t, irows, :])
            wind_t = (buf[FU, t, rows, :], buf[FV, t, rows, :])
            cur_t = (buf[CA, t, rows, :], buf[CB, t, rows, :])
            k, m8, fu, fv = consts(buf[K_, t, rows, :], buf[M8, t, rows, :], wind_t, cur_t, w)
            ca, cb = coefs(m8, w)
            buf[K_, t, rows, :] = k
            buf[M8, t, rows, :] = m8
            buf[FU, t, rows, :] = fu
            buf[FV, t, rows, :] = fv
            buf[CA, t, rows, :] = ca
            buf[CB, t, rows, :] = cb
            buf[H12, t, rows, :] = buf[H12, t, rows, :] * 2.0

    def strain_rows(r0):
        rows = pl.ds(PAD + r0, RB)
        u = [buf[U_, t, rows, :] for t in range(NT)]
        v = [buf[V_, t, rows, :] for t in range(NT)]
        um, vm = shift_m(u), shift_m(v)
        for t in range(NT):
            a, b, g, d = strain(u[t], v[t], um[t], vm[t])
            al[t, rows, :] = a
            be[t, rows, :] = b
            ga[t, rows, :] = g
            de[t, rows, :] = d

    def rate_rows(r0, final):
        rows = pl.ds(PAD + r0, RB)
        above = pl.ds(PAD + r0 - 1, RB)
        mx = []
        for t in range(NT):
            d1, d2, d12 = stress_rate(al[t, rows, :], be[t, rows, :], ga[t, rows, :], al[t, above, :], be[t, above, :], de[t, above, :], buf[K_, t, rows, :])
            h1 = buf[H1, t, rows, :] * GROW + d1
            h2 = buf[H2, t, rows, :] * GROW + d2
            h12 = buf[H12, t, rows, :] * GROW + d12
            buf[H1, t, rows, :] = h1
            buf[H2, t, rows, :] = h2
            buf[H12, t, rows, :] = 0.5 * h12 if final else h12
            mx.append(mixes(h1, h2, h12))
        up, wp, xp, yp = (shift_p([m[i] for m in mx]) for i in range(4))
        for t in range(NT):
            tx[t, rows, :] = up[t] + mx[t][1]
            nx[t, rows, :] = mx[t][0] + wp[t]
            ty[t, rows, :] = xp[t] + mx[t][3]
            ny[t, rows, :] = mx[t][2] + yp[t]

    def velocity_rows(r0, acc):
        rows = pl.ds(PAD + r0, RB)
        below = pl.ds(PAD + r0 + 1, RB)
        for t in range(NT):
            u, v, m8 = buf[U_, t, rows, :], buf[V_, t, rows, :], buf[M8, t, rows, :]
            fx = tx[t, below, :] - nx[t, rows, :]
            fy = ty[t, below, :] - ny[t, rows, :]
            nu, nv = drift(u, v, fx, fy, m8, buf[FU, t, rows, :], buf[FV, t, rows, :], buf[CA, t, rows, :], buf[CB, t, rows, :])
            buf[U_, t, rows, :] = nu
            buf[V_, t, rows, :] = nv
            if acc is not None:
                keep = (buf[K_, t, rows, :] > 0.0) & (row_in + r0 >= ITERS) & (row_in + r0 < R - ITERS)
                if t == 0:
                    keep = keep & (lane >= ITERS)
                if t == NT - 1:
                    keep = keep & (lane < 128 - ITERS)
                cu, cv = nu - u, nv - v
                acc = (acc[0] + jnp.where(keep, cu * cu + cv * cv, 0.0), acc[1] + jnp.where(keep, m8 * (nu * nu + nv * nv), 0.0))
        return acc

    NB = R // RB
    nbc = CH // RB
    LV = 3

    def step(r0, acc, lo, hi, prep, final):
        if lo <= 0 < hi:
            if prep:
                prepare(r0)
            strain_rows(r0)
        if lo <= 1 < hi:
            rate_rows(r0 - RB, final)
        if lo <= LV < hi:
            acc = velocity_rows(r0 - LV * RB, acc)
        return acc

    def sweep(acc, begin, end, prep=False, final=False):
        i = begin
        while i < min(end, LV):
            acc = step(i * RB, acc, 0, i + 1, prep, final)
            i += 1
        stop = min(end, NB)
        if i < stop:
            if acc is None:

                def body(j, c):
                    step(pl.multiple_of(j * RB, RB), None, 0, LV + 1, prep, final)
                    return c

                lax.fori_loop(i, stop, body, 0)
            else:
                acc = lax.fori_loop(i, stop, lambda j, c: step(pl.multiple_of(j * RB, RB), c, 0, LV + 1, prep, final), acc)
            i = stop
        while i < end:
            acc = step(i * RB, acc, i - NB + 1, LV + 1, prep, final)
            i += 1
        return acc

    for c in range(NCH):
        whole = buf.at[:, :, pl.ds(PAD + c * CH, CH), :]
        pltpu.make_async_copy(whole, whole, insem.at[c]).wait()
        whole = ibuf.at[:, :, pl.ds(c * CH, CH), :]
        pltpu.make_async_copy(whole, whole, insem.at[NCH + c]).wait()
        sweep(None, c * nbc, (c + 1) * nbc if c < NCH - 1 else NB + LV, prep=True)
    for _ in range(1, ITERS - 1):
        sweep(None, 0, NB + LV)
    acc = (jnp.zeros((RB, 128), F32), jnp.zeros((RB, 128), F32))
    for c in range(NCH):
        acc = sweep(acc, c * nbc + (LV if c else 0), (c + 1) * nbc + LV, final=True)
        rows = pl.ds(c * CH, CH)
        rows_b = pl.ds(PAD + c * CH, CH)
        for ref, lead, f in ((nvel, 0, U_), (nvel, 1, V_), (nstr, 0, H1), (nstr, 1, H2), (nstr, 2, H12)):
            for t in range(NT):
                pltpu.make_async_copy(buf.at[f, t, rows_b, :], ref.at[lead, rows, pl.ds(t * 128, 128)], outsem.at[c]).start()
    for n in range(2):
        sums[n] = acc[n].reshape(RB // 8, 8, 128).sum(0)
    for c in range(NCH):
        whole = buf.at[pl.ds(0, 5), :, pl.ds(PAD + c * CH, CH), :]
        pltpu.make_async_copy(whole, whole, outsem.at[c]).wait()


def strip_subcycles(ref, acc_ref, rows_axis, keep):
    cols_axis = 1 - rows_axis
    back = lambda x, axis: pltpu.roll(x, 1, axis)
    ahead = lambda x, axis: pltpu.roll(x, x.shape[axis] - 1, axis)
    w = jnp.where(ref[K_] > 0.0, 1.0, 0.0)
    ca, cb = coefs(ref[M8], w)
    ref[CA] = ca
    ref[CB] = cb

    def body(_, carry):
        u, v = ref[U_], ref[V_]
        a, b, g, d = strain(u, v, back(u, cols_axis), back(v, cols_axis))
        d1, d2, d12 = stress_rate(a, b, g, back(a, rows_axis), back(b, rows_axis), back(d, rows_axis), ref[K_])
        h1 = ref[H1] * GROW + d1
        h2 = ref[H2] * GROW + d2
        h12 = ref[H12] * GROW + d12
        ref[H1] = h1
        ref[H2] = h2
        ref[H12] = h12
        up, wp, xp, yp = mixes(h1, h2, h12)
        fx = ahead(ahead(up, cols_axis) + wp, rows_axis) - (up + ahead(wp, cols_axis))
        fy = ahead(ahead(xp, cols_axis) + yp, rows_axis) - (xp + ahead(yp, cols_axis))
        m8 = ref[M8]
        nu, nv = drift(u, v, fx, fy, m8, ref[FU], ref[FV], ref[CA], ref[CB])
        ref[U_] = nu
        ref[V_] = nv
        cu, cv = nu - u, nv - v
        inside = keep & (ref[K_] > 0.0)
        acc_ref[0] = jnp.where(inside, cu * cu + cv * cv, 0.0)
        acc_ref[1] = jnp.where(inside, m8 * (nu * nu + nv * nv), 0.0)
        return carry

    lax.fori_loop(0, ITERS, body, 0)
    return [jnp.sum(acc_ref[0]), jnp.sum(acc_ref[1])]


def frame_kernel(own, cols, ext, xa, xb, ya, yb, isums, nvel_in, nstr_in, nvel, nstr, msg, cs, rs, cacc, racc, edge, mid, sem):
    R, C = nvel.shape[1:]
    outs = ((nvel, 0), (nvel, 1), (nstr, 0), (nstr, 1), (nstr, 2))

    def places(f):
        ref, lead = outs[f]
        full = ref.at[lead]
        inner = pl.ds(128, C - 256)
        return (
            (full.at[:, pl.ds(0, 128)], edge.at[0, f]),
            (full.at[:, pl.ds(C - 128, 128)], edge.at[1, f]),
            (full.at[pl.ds(0, 8), inner], mid.at[0, f]),
            (full.at[pl.ds(R - 8, 8), inner], mid.at[1, f]),
        )

    for f in range(5):
        for n, (there, here) in enumerate(places(f)):
            pltpu.make_async_copy(there, here, sem.at[0, n // 2]).start()
    even = is_even("gx")
    a, b = xa[...], xb[...]
    top = jnp.where(even, b, a)
    bot = jnp.where(even, a, b)
    even = is_even("gy")
    a, b = ya[...], yb[...]
    left = jnp.where(even, b, a)
    right = jnp.where(even, a, b)
    for f in range(NS):
        rs[f, 0:8, :] = unpair(top, f, True)
        rs[f, 8:16, :] = own[f, 0:8, :]
        rs[f, 16:24, :] = own[f, 8:16, :]
        rs[f, 24:32, :] = unpair(bot, f, False)
        cs[f, 0:8, :] = unpair(left, f, True)
        for side in range(2):
            base = 8 * (NS * side + f)
            cs[f, 8 + 8 * side : 16 + 8 * side, 0:R] = cols[base : base + 8, :]
            cs[f, 8 + 8 * side : 16 + 8 * side, R : R + 128] = ext[base : base + 8, :]
        cs[f, 24:32, :] = unpair(right, f, False)

    def rim(shape):
        sub = lax.broadcasted_iota(jnp.int32, shape, 0)
        return ((sub >= 8) & (sub < 12)) | ((sub >= 20) & (sub < 24)), lax.broadcasted_iota(jnp.int32, shape, 1)

    band, lane = rim(rs.shape[1:])
    row_sums = strip_subcycles(rs, racc, 0, band & (lane >= ITERS) & (lane < C - ITERS))
    band, lane = rim(cs.shape[1:])
    col_sums = strip_subcycles(cs, cacc, 1, band & (lane < R))
    lane = lax.broadcasted_iota(jnp.int32, msg.shape, 1)
    totals = [jnp.sum(isums[n]) + row_sums[n] + col_sums[n] for n in range(2)]
    msg[...] = jnp.where(lane == 0, totals[0], jnp.where(lane == 1, totals[1], 0.0))

    for n in range(2):
        buf = (edge, mid)[n]
        pltpu.make_async_copy(buf, buf, sem.at[0, n]).wait()
    halves = (1.0, 1.0, 1.0, 1.0, 0.5)
    low8 = lax.broadcasted_iota(jnp.int32, (8, 128), 0) < 4
    for f in range(5):
        for part, sub in ((0, 8), (1, 16)):
            x = rs[f, sub : sub + 8, 128 : C - 128] * halves[f]
            half = lax.broadcasted_iota(jnp.int32, x.shape, 0) < 4
            mid[part, f] = jnp.where(half if part == 0 else ~half, x, mid[part, f])
        for side in range(2):
            at = side * (C - 128)
            x = rs[f, 8:16, at : at + 128] * halves[f]
            edge[side, f, 0:8, :] = jnp.where(low8, x, edge[side, f, 0:8, :])
            x = rs[f, 16:24, at : at + 128] * halves[f]
            edge[side, f, R - 8 : R, :] = jnp.where(low8, edge[side, f, R - 8 : R, :], x)
    lane = lax.broadcasted_iota(jnp.int32, (128, 128), 1)
    for c in range(R // 128):
        rows = slice(c * 128, c * 128 + 128)
        parts = [cs[f, 8 + 8 * side : 16 + 8 * side, rows] * halves[f] for side in range(2) for f in range(5)]
        x = jnp.concatenate(parts + [jnp.zeros((48, 128), F32)], 0).T
        for side in range(2):
            for f in range(5):
                shift = (120 * side - 8 * (5 * side + f)) % 128
                y = pltpu.roll(x, shift, 1) if shift else x
                hit = lane >= 124 if side else lane < 4
                edge[side, f, rows, :] = jnp.where(hit, y, edge[side, f, rows, :])
    for f in range(5):
        for n, (there, here) in enumerate(places(f)):
            pltpu.make_async_copy(here, there, sem.at[1, n // 2]).start()
    for n in range(2):
        buf = (edge, mid)[n]
        pltpu.make_async_copy(buf, buf, sem.at[1, n]).wait()


def swaps(count):
    first = [(i, i ^ 1) for i in range(count)]
    second = [(i, i + 1) for i in range(1, count - 1, 2)] + [(i + 1, i) for i in range(1, count - 1, 2)]
    return first, second


def exchange(a, b, axis):
    first, second = swaps(lax.axis_size(axis))
    return lax.ppermute(a, axis, first), lax.ppermute(b, axis, second)


def sds(*shape):
    return jax.ShapeDtypeStruct(shape, F32)


def per_device(velocity, stress, strength, ice_mass, wind_stress, current, ice_mask, open_water):
    args = (velocity, stress, strength, ice_mass, wind_stress, current, ice_mask, open_water)
    R, C = strength.shape
    anyspace = pl.BlockSpec(memory_space=pl.ANY)
    vmem = pl.BlockSpec(memory_space=pltpu.VMEM)
    limit = pltpu.CompilerParams(vmem_limit_bytes=48 * 2**20)

    def blocks(shape, where):
        return [pl.BlockSpec((x.shape[0],) * (x.ndim - 2) + shape, functools.partial(lambda nd, *g: (0,) * (nd - 2) + where(*g), x.ndim)) for x in args]

    own, xa, xb = pl.pallas_call(
        rows_kernel,
        grid=(1,),
        in_specs=blocks((8, C), lambda i: (0, 0)) + blocks((8, C), lambda i: (R // 8 - 1, 0)),
        out_specs=[pl.BlockSpec((NS, 16, C), lambda i: (0, 0, 0)), pl.BlockSpec((40, C), lambda i: (0, 0)), pl.BlockSpec((40, C), lambda i: (0, 0))],
        out_shape=[sds(NS, 16, C), sds(40, C), sds(40, C)],
        name="row_edges",
    )(*args, *args)
    xa, xb = exchange(xa, xb, "gx")
    cols = pl.pallas_call(
        cols_kernel,
        grid=(R // 128,),
        in_specs=blocks((128, 128), lambda i: (i, 0)) + blocks((128, 128), lambda i: (i, C // 128 - 1)),
        out_specs=pl.BlockSpec((16 * NS, 128), lambda i: (0, i)),
        out_shape=sds(16 * NS, R),
        name="col_edges",
    )(*args, *args)
    ya, yb, ext = pl.pallas_call(
        corners_kernel,
        in_specs=[vmem] * 3,
        out_specs=[vmem] * 3,
        out_shape=[sds(40, R + 128), sds(40, R + 128), sds(16 * NS, 128)],
        name="corners",
    )(cols, xa, xb)
    ya, yb = exchange(ya, yb, "gy")
    NT = C // 128
    RP = R + 2 * PAD
    NCH = 4
    nvel, nstr, isums = pl.pallas_call(
        functools.partial(interior_kernel, RB=32, NCH=NCH),
        in_specs=[anyspace] * 8,
        out_specs=(anyspace, anyspace, vmem),
        out_shape=(sds(2, R, C), sds(3, R, C), sds(2, 8, 128)),
        scratch_shapes=[pltpu.VMEM((NF, NT, RP, 128), F32), pltpu.VMEM((2, NT, R, 128), jnp.int32)]
        + [pltpu.VMEM((NT, RP, 128), F32)] * 8
        + [pltpu.SemaphoreType.DMA((2 * NCH,)), pltpu.SemaphoreType.DMA((NCH,))],
        compiler_params=limit,
        name="interior",
    )(*args)
    ND = lax.axis_size(ALL)
    nvel, nstr, msg = pl.pallas_call(
        frame_kernel,
        in_specs=[vmem] * 8 + [anyspace] * 2,
        out_specs=(anyspace, anyspace, vmem),
        out_shape=(sds(2, R, C), sds(3, R, C), sds(ND, 128)),
        scratch_shapes=[
            pltpu.VMEM((NF, 32, R + 128), F32),
            pltpu.VMEM((NF, 32, C), F32),
            pltpu.VMEM((2, 32, R + 128), F32),
            pltpu.VMEM((2, 32, C), F32),
            pltpu.VMEM((2, 5, R, 128), F32),
            pltpu.VMEM((2, 5, 8, C - 256), F32),
            pltpu.SemaphoreType.DMA((2, 2)),
        ],
        input_output_aliases={8: 0, 9: 1},
        compiler_params=limit,
        name="frame",
    )(own, cols, ext, xa, xb, ya, yb, isums, nvel, nstr)
    parts = lax.all_to_all(msg, ALL, 0, 0, tiled=True)
    total = jnp.sum(parts, axis=0)
    cells = R * lax.axis_size("gx") * C * lax.axis_size("gy")
    return nvel, nstr, total[0] / cells, total[1] * (0.0625 / cells)


def solution(mesh):
    whole, plane = P(None, "gx", "gy"), P("gx", "gy")
    return jax.shard_map(
        per_device,
        mesh=mesh,
        in_specs=(whole, whole, plane, plane, whole, whole, plane, plane),
        out_specs=(whole, whole, P(), P()),
        check_vma=False,
    )
```

```python
import functools

import jax
import jax.numpy as jnp
from jax import lax
from jax.experimental import pallas as pl
from jax.experimental.pallas import tpu as pltpu
from jax.sharding import PartitionSpec as P

ITERS = 4
RELAX = 0.8
GROW = 1.0 / (1.0 + RELAX)
KAPPA = RELAX / (1.0 + RELAX)
PAD = 8
F32 = jnp.float32
(U_, V_, H1, H2, H12, K_, M8, FU, FV, CA, CB) = range(11)
NS = 9
NF = 11
ALL = ("gx", "gy")


def weight_of(mask, openw):
    return mask.astype(F32) * (1.0 - openw.astype(F32))


def consts(strength, mass, wind, cur, weight):
    return (KAPPA * strength) * weight, mass * 8.0, 4.0 * (wind[0] + cur[0]), 4.0 * (wind[1] + cur[1])


def coefs(m8, weight):
    a = m8 * 0.25 + 1.0
    b = m8 * 0.0375
    scale = (0.25 * weight) / (a * a + b * b)
    return a * scale, b * scale


def strain(u, v, um, vm):
    su = u + um
    du = u - um
    sv = v + vm
    dv = v - vm
    return su + dv, su - dv, du + sv, du - sv


def stress_rate(alpha, beta, gamma, alpha_m, beta_m, delta_m, k):
    d = alpha - beta_m
    t = beta - alpha_m
    s = gamma + delta_m
    q = d * d + 0.25 * (t * t + s * s) + 0.01
    r = lax.rsqrt(q)
    z = k * r
    z4 = 0.25 * z
    return z * (d - q * r), z4 * t, z4 * s


def mixes(h1, h2, h12):
    e = h1 + h2
    g = h1 - h2
    return e + h12, e - h12, h12 + g, h12 - g


def drift(u, v, fx, fy, m8, fu, fv, ca, cb):
    ru = m8 * u + (fx + fu)
    rv = m8 * v + (fy + fv)
    return ca * ru + cb * rv, ca * rv - cb * ru


def pair_rows(parts, high):
    half = lax.broadcasted_iota(jnp.int32, parts[0].shape, 0) < 4
    tiles = []
    for f in range(0, NS, 2):
        a = parts[f]
        b = parts[f + 1] if f + 1 < NS else jnp.zeros_like(a)
        if high:
            tiles.append(jnp.where(half, pltpu.roll(a, 4, 0), b))
        else:
            tiles.append(jnp.where(half, a, pltpu.roll(b, 4, 0)))
    return jnp.concatenate(tiles, 0)


def unpair(tiles, f, high):
    x = tiles[8 * (f // 2) : 8 * (f // 2) + 8]
    return x if (f % 2 == 1) == high else pltpu.roll(x, 4, 0)


def is_even(axis):
    return lax.axis_index(axis) % 2 == 0


def strip_fields(vel, strs, strength, mass, wind, cur, mask, openw):
    w = weight_of(mask[...], openw[...])
    k, m8, fu, fv = consts(strength[...], mass[...], (wind[0], wind[1]), (cur[0], cur[1]), w)
    return [vel[0], vel[1], strs[0], strs[1], 2.0 * strs[2], k, m8, fu, fv]


def rows_kernel(*refs):
    own, msg_a, msg_b = refs[16:]
    top = strip_fields(*refs[:8])
    bot = strip_fields(*refs[8:16])
    for f in range(NS):
        own[f, 0:8, :] = top[f]
        own[f, 8:16, :] = bot[f]
    low = pair_rows(top, False)
    high = pair_rows(bot, True)
    even = is_even("gx")
    msg_a[...] = jnp.where(even, high, low)
    msg_b[...] = jnp.where(even, low, high)


def load_kernel(vel, strs, strength, mass, wind, cur, mask, openw, x, cols, ibuf, sem, *, NCH):
    R, C = strength.shape
    CH = R // NCH
    srcs = [(vel, 0, U_), (vel, 1, V_), (strs, 0, H1), (strs, 1, H2), (strs, 2, H12), (strength, None, K_), (mass, None, M8),
            (wind, 0, FU), (wind, 1, FV), (cur, 0, CA), (cur, 1, CB)]
    for c in range(NCH):
        rows = pl.ds(c * CH, CH)
        for ref, lead, f in srcs:
            src = ref.at[rows] if lead is None else ref.at[lead, rows]
            pltpu.make_async_copy(src, x.at[f, rows], sem.at[c]).start()
        for n, ref in enumerate((mask, openw)):
            pltpu.make_async_copy(ref.at[rows], ibuf.at[n, rows], sem.at[NCH + c]).start()
    lane = lax.broadcasted_iota(jnp.int32, (128, 128), 1)

    def prepare(r0):
        rows = pl.ds(r0, 8)
        w = weight_of(ibuf[0, rows, :], ibuf[1, rows, :])
        k, m8, fu, fv = consts(x[K_, rows, :], x[M8, rows, :], (x[FU, rows, :], x[FV, rows, :]), (x[CA, rows, :], x[CB, rows, :]), w)
        ca, cb = coefs(m8, w)
        x[H12, rows, :] = 2.0 * x[H12, rows, :]
        for f, value in ((K_, k), (M8, m8), (FU, fu), (FV, fv), (CA, ca), (CB, cb)):
            x[f, rows, :] = value

    for c in range(NCH):
        whole = x.at[:, pl.ds(c * CH, CH), :]
        pltpu.make_async_copy(whole, whole, sem.at[c]).wait()
        whole = ibuf.at[:, pl.ds(c * CH, CH), :]
        pltpu.make_async_copy(whole, whole, sem.at[NCH + c]).wait()

        def body(i, carry):
            for n in range(4):
                prepare(pl.multiple_of(i * 32 + 8 * n, 8))
            return carry

        lax.fori_loop(c * CH // 32, (c + 1) * CH // 32, body, 0)
        for p in range(c * CH // 128, (c + 1) * CH // 128):
            rows = pl.ds(p * 128, 128)
            for side in range(2):
                packed = jnp.zeros((128, 128), F32)
                for f in range(NS):
                    shift = (8 * f - 120 * side) % 128
                    y = x[f, rows, side * (C - 128) : side * (C - 128) + 128]
                    y = pltpu.roll(y, shift, 1) if shift else y
                    packed = jnp.where((lane >= 8 * f) & (lane < 8 * f + 8), y, packed)
                cols[8 * NS * side : 8 * NS * (side + 1), p * 128 : p * 128 + 128] = packed.T[0 : 8 * NS]


def corners_kernel(cols, xa, xb, ya, yb, ext):
    even = is_even("gx")
    a, b = xa[...], xb[...]
    top = jnp.where(even, b, a)
    bot = jnp.where(even, a, b)
    C = cols.shape[1]
    lane = lax.broadcasted_iota(jnp.int32, (8, 128), 1)
    strips = []
    for side in range(2):
        at = side * (C - 128)
        t = jnp.concatenate([top[:, at : at + 128], bot[:, at : at + 128], jnp.zeros((48, 128), F32)], 0).T
        t = t[120 * side : 120 * side + 8]
        own = []
        for f in range(NS):
            e = jnp.where(lane >= 124, pltpu.roll(t, 124 - 4 * f, 1), 0.0)
            e = jnp.where(lane < 4, pltpu.roll(t, 128 - 40 - 4 * f, 1), e)
            base = 8 * (NS * side + f)
            ext[base : base + 8, :] = e
            own.append(jnp.concatenate([cols[base : base + 8, :], e], 1))
        strips.append(pair_rows(own, side == 1))
    low, high = strips
    even = is_even("gy")
    ya[...] = jnp.where(even, high, low)
    yb[...] = jnp.where(even, low, high)


def interior_kernel(x_in, x, sums, al, be, ga, de, tx, ty, nx, ny, *, RB):
    R, C = x.shape[1:]
    NT = C // 128
    NB = R // RB
    LV = 3
    zero = jnp.zeros((8, 128), F32)
    for t in range(NT):
        for ref in (al, be, de):
            ref[t, 0:PAD, :] = zero
        for ref in (tx, ty):
            ref[t, PAD + R : PAD + R + 8, :] = zero
    lane = lax.broadcasted_iota(jnp.int32, (RB, 128), 1)
    row_in = lax.broadcasted_iota(jnp.int32, (RB, 128), 0)
    first = lane == 0
    last = lane == 127

    def tile(t):
        return slice(128 * t, 128 * t + 128)

    def shift_m(v):
        r = [pltpu.roll(a, 1, 1) for a in v]
        return [jnp.where(first, r[(t - 1) % NT], r[t]) for t in range(NT)]

    def shift_p(v):
        r = [pltpu.roll(a, 127, 1) for a in v]
        return [jnp.where(last, r[(t + 1) % NT], r[t]) for t in range(NT)]

    def strain_rows(r0):
        own = pl.ds(r0, RB)
        rows = pl.ds(PAD + r0, RB)
        u = [x[U_, own, tile(t)] for t in range(NT)]
        v = [x[V_, own, tile(t)] for t in range(NT)]
        um, vm = shift_m(u), shift_m(v)
        for t in range(NT):
            a, b, g, d = strain(u[t], v[t], um[t], vm[t])
            al[t, rows, :] = a
            be[t, rows, :] = b
            ga[t, rows, :] = g
            de[t, rows, :] = d

    def rate_rows(r0, final):
        own = pl.ds(r0, RB)
        rows = pl.ds(PAD + r0, RB)
        above = pl.ds(PAD + r0 - 1, RB)
        mx = []
        for t in range(NT):
            d1, d2, d12 = stress_rate(al[t, rows, :], be[t, rows, :], ga[t, rows, :], al[t, above, :], be[t, above, :], de[t, above, :], x[K_, own, tile(t)])
            h1 = x[H1, own, tile(t)] * GROW + d1
            h2 = x[H2, own, tile(t)] * GROW + d2
            h12 = x[H12, own, tile(t)] * GROW + d12
            x[H1, own, tile(t)] = h1
            x[H2, own, tile(t)] = h2
            x[H12, own, tile(t)] = 0.5 * h12 if final else h12
            mx.append(mixes(h1, h2, h12))
        up, wp, xp, yp = (shift_p([m[i] for m in mx]) for i in range(4))
        for t in range(NT):
            tx[t, rows, :] = up[t] + mx[t][1]
            nx[t, rows, :] = mx[t][0] + wp[t]
            ty[t, rows, :] = xp[t] + mx[t][3]
            ny[t, rows, :] = mx[t][2] + yp[t]

    def velocity_rows(r0, acc):
        own = pl.ds(r0, RB)
        rows = pl.ds(PAD + r0, RB)
        below = pl.ds(PAD + r0 + 1, RB)
        for t in range(NT):
            u, v, m8 = x[U_, own, tile(t)], x[V_, own, tile(t)], x[M8, own, tile(t)]
            fx = tx[t, below, :] - nx[t, rows, :]
            fy = ty[t, below, :] - ny[t, rows, :]
            nu, nv = drift(u, v, fx, fy, m8, x[FU, own, tile(t)], x[FV, own, tile(t)], x[CA, own, tile(t)], x[CB, own, tile(t)])
            x[U_, own, tile(t)] = nu
            x[V_, own, tile(t)] = nv
            if acc is not None:
                keep = (x[K_, own, tile(t)] > 0.0) & (row_in + r0 >= ITERS) & (row_in + r0 < R - ITERS)
                if t == 0:
                    keep = keep & (lane >= ITERS)
                if t == NT - 1:
                    keep = keep & (lane < 128 - ITERS)
                cu, cv = nu - u, nv - v
                acc = (acc[0] + jnp.where(keep, cu * cu + cv * cv, 0.0), acc[1] + jnp.where(keep, m8 * (nu * nu + nv * nv), 0.0))
        return acc

    zeros = (jnp.zeros((RB, 128), F32), jnp.zeros((RB, 128), F32))
    for it in range(ITERS):
        final = it == ITERS - 1
        for i in range(LV):
            strain_rows(i * RB)
            if i:
                rate_rows((i - 1) * RB, final)
            elif it:
                rate_rows((NB - 1) * RB, False)
            if it:
                velocity_rows((NB + i - LV) * RB, None)

        def body(j, acc):
            r0 = pl.multiple_of(j * RB, RB)
            strain_rows(r0)
            rate_rows(r0 - RB, final)
            return velocity_rows(r0 - LV * RB, acc if final else None) if final else (velocity_rows(r0 - LV * RB, None), acc)[1]

        acc = lax.fori_loop(LV, NB, body, zeros if final else 0)
    rate_rows((NB - 1) * RB, True)
    for i in range(LV):
        acc = velocity_rows((NB + i - LV) * RB, acc)
    for n in range(2):
        sums[n] = acc[n].reshape(RB // 8, 8, 128).sum(0)


def strip_subcycles(ref, acc_ref, rows_axis, keep):
    cols_axis = 1 - rows_axis
    back = lambda x, axis: pltpu.roll(x, 1, axis)
    ahead = lambda x, axis: pltpu.roll(x, x.shape[axis] - 1, axis)
    w = jnp.where(ref[K_] > 0.0, 1.0, 0.0)
    ca, cb = coefs(ref[M8], w)
    ref[CA] = ca
    ref[CB] = cb

    def body(_, carry):
        u, v = ref[U_], ref[V_]
        a, b, g, d = strain(u, v, back(u, cols_axis), back(v, cols_axis))
        d1, d2, d12 = stress_rate(a, b, g, back(a, rows_axis), back(b, rows_axis), back(d, rows_axis), ref[K_])
        h1 = ref[H1] * GROW + d1
        h2 = ref[H2] * GROW + d2
        h12 = ref[H12] * GROW + d12
        ref[H1] = h1
        ref[H2] = h2
        ref[H12] = h12
        up, wp, xp, yp = mixes(h1, h2, h12)
        fx = ahead(ahead(up, cols_axis) + wp, rows_axis) - (up + ahead(wp, cols_axis))
        fy = ahead(ahead(xp, cols_axis) + yp, rows_axis) - (xp + ahead(yp, cols_axis))
        m8 = ref[M8]
        nu, nv = drift(u, v, fx, fy, m8, ref[FU], ref[FV], ref[CA], ref[CB])
        ref[U_] = nu
        ref[V_] = nv
        cu, cv = nu - u, nv - v
        inside = keep & (ref[K_] > 0.0)
        acc_ref[0] = jnp.where(inside, cu * cu + cv * cv, 0.0)
        acc_ref[1] = jnp.where(inside, m8 * (nu * nu + nv * nv), 0.0)
        return carry

    lax.fori_loop(0, ITERS, body, 0)
    return [jnp.sum(acc_ref[0]), jnp.sum(acc_ref[1])]


def frame_kernel(own, cols, ext, xa, xb, ya, yb, isums, x_in, x, nvel, nstr, msg, cs, rs, cacc, racc, sem):
    R, C = nvel.shape[1:]
    outs = ((nvel, 0), (nvel, 1), (nstr, 0), (nstr, 1), (nstr, 2))
    inner = (slice(8, R - 8), slice(128, C - 128))
    sides = ((slice(0, R), slice(0, 128)), (slice(0, R), slice(C - 128, C)), (slice(0, 8), inner[1]), (slice(R - 8, R), inner[1]))

    def copies(f, where):
        ref, lead = outs[f]
        return [pltpu.make_async_copy(x.at[(f, *w)], ref.at[(lead, *w)], sem.at[f, n]) for n, w in where]

    for f in range(5):
        for cp in copies(f, [(0, inner)]):
            cp.start()
    even = is_even("gx")
    a, b = xa[...], xb[...]
    top = jnp.where(even, b, a)
    bot = jnp.where(even, a, b)
    even = is_even("gy")
    a, b = ya[...], yb[...]
    left = jnp.where(even, b, a)
    right = jnp.where(even, a, b)
    for f in range(NS):
        rs[f, 0:8, :] = unpair(top, f, True)
        rs[f, 8:16, :] = own[f, 0:8, :]
        rs[f, 16:24, :] = own[f, 8:16, :]
        rs[f, 24:32, :] = unpair(bot, f, False)
        cs[f, 0:8, :] = unpair(left, f, True)
        for side in range(2):
            base = 8 * (NS * side + f)
            cs[f, 8 + 8 * side : 16 + 8 * side, 0:R] = cols[base : base + 8, :]
            cs[f, 8 + 8 * side : 16 + 8 * side, R : R + 128] = ext[base : base + 8, :]
        cs[f, 24:32, :] = unpair(right, f, False)

    def rim(shape):
        sub = lax.broadcasted_iota(jnp.int32, shape, 0)
        return ((sub >= 8) & (sub < 12)) | ((sub >= 20) & (sub < 24)), lax.broadcasted_iota(jnp.int32, shape, 1)

    band, lane = rim(rs.shape[1:])
    row_sums = strip_subcycles(rs, racc, 0, band & (lane >= ITERS) & (lane < C - ITERS))
    band, lane = rim(cs.shape[1:])
    col_sums = strip_subcycles(cs, cacc, 1, band & (lane < R))
    lane = lax.broadcasted_iota(jnp.int32, msg.shape, 1)
    totals = [jnp.sum(isums[n]) + row_sums[n] + col_sums[n] for n in range(2)]
    msg[...] = jnp.where(lane == 0, totals[0], jnp.where(lane == 1, totals[1], 0.0))

    halves = (1.0, 1.0, 1.0, 1.0, 0.5)
    low8 = lax.broadcasted_iota(jnp.int32, (8, C), 0) < 4
    for f in range(5):
        x[f, 0:8, :] = jnp.where(low8, rs[f, 8:16, :] * halves[f], x[f, 0:8, :])
        x[f, R - 8 : R, :] = jnp.where(low8, x[f, R - 8 : R, :], rs[f, 16:24, :] * halves[f])
    lane = lax.broadcasted_iota(jnp.int32, (128, 128), 1)
    for c in range(R // 128):
        rows = slice(c * 128, c * 128 + 128)
        parts = [cs[f, 8 + 8 * side : 16 + 8 * side, rows] * halves[f] for side in range(2) for f in range(5)]
        y = jnp.concatenate(parts + [jnp.zeros((48, 128), F32)], 0).T
        for side in range(2):
            at = slice(side * (C - 128), side * (C - 128) + 128)
            for f in range(5):
                shift = (120 * side - 8 * (5 * side + f)) % 128
                z = pltpu.roll(y, shift, 1) if shift else y
                hit = lane >= 124 if side else lane < 4
                x[f, rows, at] = jnp.where(hit, z, x[f, rows, at])
    edges = list(enumerate(sides, 1))
    for f in range(5):
        for cp in copies(f, edges):
            cp.start()
    for f in range(5):
        for cp in copies(f, [(0, inner)] + edges):
            cp.wait()


def swaps(count):
    first = [(i, i ^ 1) for i in range(count)]
    second = [(i, i + 1) for i in range(1, count - 1, 2)] + [(i + 1, i) for i in range(1, count - 1, 2)]
    return first, second


def exchange(a, b, axis):
    first, second = swaps(lax.axis_size(axis))
    return lax.ppermute(a, axis, first), lax.ppermute(b, axis, second)


def sds(*shape):
    return jax.ShapeDtypeStruct(shape, F32)


def interior(x, RB=32, flags=None):
    _, R, C = x.shape
    vmem = pl.BlockSpec(memory_space=pltpu.VMEM)
    return pl.pallas_call(
        functools.partial(interior_kernel, RB=RB),
        in_specs=[vmem],
        out_specs=(vmem, vmem),
        out_shape=(sds(*x.shape), sds(2, 8, 128)),
        scratch_shapes=[pltpu.VMEM((C // 128, R + 2 * PAD, 128), F32)] * 8,
        input_output_aliases={0: 0},
        compiler_params=pltpu.CompilerParams(vmem_limit_bytes=30 * 2**20, flags=flags),
        name="interior",
    )(x)


def per_device(velocity, stress, strength, ice_mass, wind_stress, current, ice_mask, open_water):
    args = (velocity, stress, strength, ice_mass, wind_stress, current, ice_mask, open_water)
    args = tuple(pltpu.with_memory_space_constraint(v, pltpu.HBM) for v in args)
    R, C = strength.shape
    anyspace = pl.BlockSpec(memory_space=pltpu.HBM)
    vmem = pl.BlockSpec(memory_space=pltpu.VMEM)

    def limit(mib):
        return pltpu.CompilerParams(vmem_limit_bytes=mib * 2**20)

    def blocks(shape, where):
        return [pl.BlockSpec((v.shape[0],) * (v.ndim - 2) + shape, functools.partial(lambda nd, *g: (0,) * (nd - 2) + where(*g), v.ndim)) for v in args]

    own, xa, xb = pl.pallas_call(
        rows_kernel,
        grid=(1,),
        in_specs=blocks((8, C), lambda i: (0, 0)) + blocks((8, C), lambda i: (R // 8 - 1, 0)),
        out_specs=[pl.BlockSpec((NS, 16, C), lambda i: (0, 0, 0)), pl.BlockSpec((40, C), lambda i: (0, 0)), pl.BlockSpec((40, C), lambda i: (0, 0))],
        out_shape=[sds(NS, 16, C), sds(40, C), sds(40, C)],
        compiler_params=limit(6),
        name="row_edges",
    )(*args, *args)
    xa, xb = exchange(xa, xb, "gx")
    NCH = 4
    x, cols = pl.pallas_call(
        functools.partial(load_kernel, NCH=NCH),
        in_specs=[anyspace] * 8,
        out_specs=(vmem, vmem),
        out_shape=(sds(NF, R, C), sds(16 * NS, R)),
        scratch_shapes=[pltpu.VMEM((2, R, C), jnp.int32), pltpu.SemaphoreType.DMA((2 * NCH,))],
        compiler_params=limit(16),
        name="load",
    )(*args)
    ya, yb, ext = pl.pallas_call(
        corners_kernel,
        in_specs=[vmem] * 3,
        out_specs=[vmem] * 3,
        out_shape=[sds(40, R + 128), sds(40, R + 128), sds(16 * NS, 128)],
        compiler_params=limit(6),
        name="corners",
    )(cols, xa, xb)
    ya, yb = exchange(ya, yb, "gy")
    x, isums = interior(x)
    ND = lax.axis_size(ALL)
    x, nvel, nstr, msg = pl.pallas_call(
        frame_kernel,
        in_specs=[vmem] * 9,
        out_specs=(vmem, anyspace, anyspace, vmem),
        out_shape=(sds(NF, R, C), sds(2, R, C), sds(3, R, C), sds(ND, 128)),
        scratch_shapes=[
            pltpu.VMEM((NF, 32, R + 128), F32),
            pltpu.VMEM((NF, 32, C), F32),
            pltpu.VMEM((2, 32, R + 128), F32),
            pltpu.VMEM((2, 32, C), F32),
            pltpu.SemaphoreType.DMA((5, 5)),
        ],
        input_output_aliases={8: 0},
        compiler_params=limit(20),
        name="frame",
    )(own, cols, ext, xa, xb, ya, yb, isums, x)
    parts = lax.all_to_all(msg, ALL, 0, 0, tiled=True)
    total = jnp.sum(parts, axis=0)
    cells = R * lax.axis_size("gx") * C * lax.axis_size("gy")
    return nvel, nstr, total[0] / cells, total[1] * (0.0625 / cells)


def solution(mesh):
    whole, plane = P(None, "gx", "gy"), P("gx", "gy")
    return jax.shard_map(
        per_device,
        mesh=mesh,
        in_specs=(whole, whole, plane, plane, whole, whole, plane, plane),
        out_specs=(whole, whole, P(), P()),
        check_vma=False,
    )
```

```python
import functools

import jax
import jax.numpy as jnp
from jax import lax
from jax.experimental import pallas as pl
from jax.experimental.pallas import tpu as pltpu
from jax.sharding import PartitionSpec as P

ITERS = 4
RELAX = 0.8
GROW = 1.0 / (1.0 + RELAX)
KAPPA = RELAX / (1.0 + RELAX)
PAD = 8
F32 = jnp.float32
(U_, V_, H1, H2, H12, K_, M8, FU, FV, CA, CB) = range(11)
NS = 9
NF = 11
ALL = ("gx", "gy")


def weight_of(mask, openw):
    return mask.astype(F32) * (1.0 - openw.astype(F32))


def consts(strength, mass, wind, cur, weight):
    return (KAPPA * strength) * weight, mass * 8.0, 4.0 * (wind[0] + cur[0]), 4.0 * (wind[1] + cur[1])


def coefs(m8, weight):
    a = m8 * 0.25 + 1.0
    b = m8 * 0.0375
    scale = (0.25 * weight) / (a * a + b * b)
    return a * scale, b * scale


def strain(u, v, um, vm):
    su = u + um
    du = u - um
    sv = v + vm
    dv = v - vm
    return su + dv, su - dv, du + sv, du - sv


def stress_rate(alpha, beta, gamma, alpha_m, beta_m, delta_m, k):
    d = alpha - beta_m
    t = beta - alpha_m
    s = gamma + delta_m
    q = d * d + 0.25 * (t * t + s * s) + 0.01
    r = lax.rsqrt(q)
    z = k * r
    z4 = 0.25 * z
    return z * (d - q * r), z4 * t, z4 * s


def mixes(h1, h2, h12):
    return h1 + h2, h1 - h2, h12


def spread(m, p):
    xs, xd = p[0] + m[0], p[2] - m[2]
    ys, yd = p[2] + m[2], p[1] - m[1]
    return xs + xd, xs - xd, ys + yd, ys - yd


def drift(u, v, fx, fy, m8, fu, fv, ca, cb):
    ru = m8 * u + (fx + fu)
    rv = m8 * v + (fy + fv)
    return ca * ru + cb * rv, ca * rv - cb * ru


def pair_rows(parts, high):
    half = lax.broadcasted_iota(jnp.int32, parts[0].shape, 0) < 4
    tiles = []
    for f in range(0, NS, 2):
        a = parts[f]
        b = parts[f + 1] if f + 1 < NS else jnp.zeros_like(a)
        if high:
            tiles.append(jnp.where(half, pltpu.roll(a, 4, 0), b))
        else:
            tiles.append(jnp.where(half, a, pltpu.roll(b, 4, 0)))
    return jnp.concatenate(tiles, 0)


def unpair(tiles, f, high):
    x = tiles[8 * (f // 2) : 8 * (f // 2) + 8]
    return x if (f % 2 == 1) == high else pltpu.roll(x, 4, 0)


def is_even(axis):
    return lax.axis_index(axis) % 2 == 0


def strip_fields(vel, strs, strength, mass, wind, cur, mask, openw):
    w = weight_of(mask[...], openw[...])
    k, m8, fu, fv = consts(strength[...], mass[...], (wind[0], wind[1]), (cur[0], cur[1]), w)
    return [vel[0], vel[1], strs[0], strs[1], 2.0 * strs[2], k, m8, fu, fv]


def rows_kernel(*refs):
    own, msg_a, msg_b = refs[16:]
    top = strip_fields(*refs[:8])
    bot = strip_fields(*refs[8:16])
    for f in range(NS):
        own[f, 0:8, :] = top[f]
        own[f, 8:16, :] = bot[f]
    low = pair_rows(top, False)
    high = pair_rows(bot, True)
    even = is_even("gx")
    msg_a[...] = jnp.where(even, high, low)
    msg_b[...] = jnp.where(even, low, high)


def load_kernel(vel, strs, strength, mass, wind, cur, mask, openw, x, cols):
    R, C = strength.shape
    lane = lax.broadcasted_iota(jnp.int32, (128, 128), 1)

    def prepare(r0):
        rows = pl.ds(r0, 8)
        for t in range(C // 128):
            at = (rows, slice(128 * t, 128 * t + 128))
            w = weight_of(mask[at], openw[at])
            k, m8, fu, fv = consts(strength[at], mass[at], (wind[(0, *at)], wind[(1, *at)]), (cur[(0, *at)], cur[(1, *at)]), w)
            ca, cb = coefs(m8, w)
            values = (vel[(0, *at)], vel[(1, *at)], strs[(0, *at)], strs[(1, *at)], 2.0 * strs[(2, *at)], k, m8, fu, fv, ca, cb)
            for f in range(NF):
                x[(f, *at)] = values[f]

    def body(i, carry):
        for n in range(4):
            prepare(pl.multiple_of(i * 32 + 8 * n, 8))
        return carry

    lax.fori_loop(0, R // 32, body, 0)

    def pack(p, side):
        rows = pl.ds(p * 128, 128)
        packed = jnp.zeros((128, 128), F32)
        for f in range(NS):
            shift = (8 * f - 120 * side) % 128
            y = x[f, rows, side * (C - 128) : side * (C - 128) + 128]
            y = pltpu.roll(y, shift, 1) if shift else y
            packed = jnp.where((lane >= 8 * f) & (lane < 8 * f + 8), y, packed)
        cols[8 * NS * side : 8 * NS * (side + 1), p * 128 : p * 128 + 128] = packed.T[0 : 8 * NS]

    for p in range(R // 128):
        for side in range(2):
            pack(p, side)


def corners_kernel(cols, xa, xb, ya, yb, ext):
    even = is_even("gx")
    a, b = xa[...], xb[...]
    top = jnp.where(even, b, a)
    bot = jnp.where(even, a, b)
    C = cols.shape[1]
    lane = lax.broadcasted_iota(jnp.int32, (8, 128), 1)
    strips = []
    for side in range(2):
        at = side * (C - 128)
        t = jnp.concatenate([top[:, at : at + 128], bot[:, at : at + 128], jnp.zeros((48, 128), F32)], 0).T
        t = t[120 * side : 120 * side + 8]
        own = []
        for f in range(NS):
            e = jnp.where(lane >= 124, pltpu.roll(t, 124 - 4 * f, 1), 0.0)
            e = jnp.where(lane < 4, pltpu.roll(t, 128 - 40 - 4 * f, 1), e)
            base = 8 * (NS * side + f)
            ext[base : base + 8, :] = e
            own.append(jnp.concatenate([cols[base : base + 8, :], e], 1))
        strips.append(pair_rows(own, side == 1))
    low, high = strips
    even = is_even("gy")
    ya[...] = jnp.where(even, high, low)
    yb[...] = jnp.where(even, low, high)


def interior_kernel(x_in, x, nvel, nstr, sums, al, be, ga, de, tx, ty, nx, ny, sem, *, RB, L1, L2):
    R, C = x.shape[1:]
    NT = C // 128
    zero = jnp.zeros((8, 128), F32)
    for t in range(NT):
        for ref in (al, be, de):
            ref[t, 0:PAD, :] = zero
        for ref in (tx, ty):
            ref[t, PAD + R : PAD + R + 8, :] = zero
    lane = lax.broadcasted_iota(jnp.int32, (8, 128), 1)
    row_in = lax.broadcasted_iota(jnp.int32, (8, 128), 0)
    first = lane == 0
    last = lane == 127

    def tile(t):
        return slice(128 * t, 128 * t + 128)

    def strain_rows(r0):
        own = pl.ds(r0, 8)
        rows = pl.ds(PAD + r0, 8)
        ru = rv = None
        for t in range(NT):
            u, v = x[U_, own, tile(t)], x[V_, own, tile(t)]
            qu, qv = pltpu.roll(u, 1, 1), pltpu.roll(v, 1, 1)
            um = jnp.where(first, ru, qu) if t else qu
            vm = jnp.where(first, rv, qv) if t else qv
            ru, rv = qu, qv
            al[t, rows, :], be[t, rows, :], ga[t, rows, :], de[t, rows, :] = strain(u, v, um, vm)

    def rate_rows(r0, final):
        own = pl.ds(r0, 8)
        rows = pl.ds(PAD + r0, 8)
        above = pl.ds(PAD + r0 - 1, 8)

        def emit(t, m, q, nq):
            p = [jnp.where(last, nq[i], q[i]) if nq else q[i] for i in range(3)]
            tx[t, rows, :], nx[t, rows, :], ty[t, rows, :], ny[t, rows, :] = spread(m, p)

        held = None
        for t in range(NT):
            d1, d2, d12 = stress_rate(al[t, rows, :], be[t, rows, :], ga[t, rows, :], al[t, above, :], be[t, above, :], de[t, above, :], x[K_, own, tile(t)])
            h1 = x[H1, own, tile(t)] * GROW + d1
            h2 = x[H2, own, tile(t)] * GROW + d2
            h12 = x[H12, own, tile(t)] * GROW + d12
            x[H1, own, tile(t)] = h1
            x[H2, own, tile(t)] = h2
            x[H12, own, tile(t)] = 0.5 * h12 if final else h12
            m = mixes(h1, h2, h12)
            q = [pltpu.roll(v, 127, 1) for v in m]
            if held:
                emit(t - 1, *held, q)
            held = (m, q)
        emit(NT - 1, *held, None)

    def velocity_rows(r0, acc):
        own = pl.ds(r0, 8)
        rows = pl.ds(PAD + r0, 8)
        below = pl.ds(PAD + r0 + 1, 8)
        for t in range(NT):
            u, v, m8 = x[U_, own, tile(t)], x[V_, own, tile(t)], x[M8, own, tile(t)]
            fx = tx[t, below, :] - nx[t, rows, :]
            fy = ty[t, below, :] - ny[t, rows, :]
            nu, nv = drift(u, v, fx, fy, m8, x[FU, own, tile(t)], x[FV, own, tile(t)], x[CA, own, tile(t)], x[CB, own, tile(t)])
            x[U_, own, tile(t)] = nu
            x[V_, own, tile(t)] = nv
            if acc is not None:
                keep = (x[K_, own, tile(t)] > 0.0) & (row_in + r0 >= ITERS) & (row_in + r0 < R - ITERS)
                if t == 0:
                    keep = keep & (lane >= ITERS)
                if t == NT - 1:
                    keep = keep & (lane < 128 - ITERS)
                cu, cv = nu - u, nv - v
                acc[2 * (t % 2)] += jnp.where(keep, cu * cu + cv * cv, 0.0)
                acc[2 * (t % 2) + 1] += jnp.where(keep, m8 * (nu * nu + nv * nv), 0.0)

    sent = [0]

    def send(end):
        rows = pl.ds(sent[0], end - sent[0])
        for f, (ref, lead) in enumerate(((nvel, 0), (nvel, 1), (nstr, 0), (nstr, 1), (nstr, 2))):
            pltpu.make_async_copy(x.at[f, rows], ref.at[lead, rows], sem).start()
        sent[0] = end

    acc = [zero] * 4
    peel = -(-L2 // RB) * RB
    for it in range(ITERS):
        final = it == ITERS - 1
        for r in range(0, peel, 8):
            strain_rows(r)
            if r >= L1:
                rate_rows(r - L1, final)
            elif it:
                rate_rows(R + r - L1, False)
            if r >= L2:
                velocity_rows(r - L2, acc if final else None)
            elif it:
                velocity_rows(R + r - L2, None)

        def body(j, acc):
            r0 = pl.multiple_of(j * RB, RB)
            acc = list(acc) if final else None
            for r in range(0, RB, 8):
                strain_rows(r0 + r)
                rate_rows(r0 + (r - L1), final)
                velocity_rows(r0 + (r - L2), acc)
            return tuple(acc) if final else ()

        if not final:
            lax.fori_loop(peel // RB, R // RB, body, ())
            continue
        for j in range(peel // RB, R // RB, 2):
            acc = list(lax.fori_loop(j, min(j + 2, R // RB), body, tuple(acc)))
            send(min((j + 2) * RB, R) - L2)
    for r in range(0, L2, 8):
        if r < L1:
            rate_rows(R + r - L1, True)
        velocity_rows(R + r - L2, acc)
        if r + 8 == L2 // 2:
            send(R - L2 // 2)
    send(R)
    sums[0] = acc[0] + acc[2]
    sums[1] = acc[1] + acc[3]
    whole = x.at[pl.ds(0, 5)]
    pltpu.make_async_copy(whole, whole, sem).wait()


def strip_subcycles(ref, acc_ref, rows_axis, keep):
    cols_axis = 1 - rows_axis
    back = lambda x, axis: pltpu.roll(x, 1, axis)
    ahead = lambda x, axis: pltpu.roll(x, x.shape[axis] - 1, axis)
    w = jnp.where(ref[K_] > 0.0, 1.0, 0.0)
    ca, cb = coefs(ref[M8], w)
    ref[CA] = ca
    ref[CB] = cb

    def body(_, carry):
        u, v = ref[U_], ref[V_]
        a, b, g, d = strain(u, v, back(u, cols_axis), back(v, cols_axis))
        d1, d2, d12 = stress_rate(a, b, g, back(a, rows_axis), back(b, rows_axis), back(d, rows_axis), ref[K_])
        h1 = ref[H1] * GROW + d1
        h2 = ref[H2] * GROW + d2
        h12 = ref[H12] * GROW + d12
        ref[H1] = h1
        ref[H2] = h2
        ref[H12] = h12
        m = mixes(h1, h2, h12)
        xt, xn, yt, yn = spread(m, [ahead(v, cols_axis) for v in m])
        fx = ahead(xt, rows_axis) - xn
        fy = ahead(yt, rows_axis) - yn
        m8 = ref[M8]
        nu, nv = drift(u, v, fx, fy, m8, ref[FU], ref[FV], ref[CA], ref[CB])
        ref[U_] = nu
        ref[V_] = nv
        cu, cv = nu - u, nv - v
        inside = keep & (ref[K_] > 0.0)
        acc_ref[0] = jnp.where(inside, cu * cu + cv * cv, 0.0)
        acc_ref[1] = jnp.where(inside, m8 * (nu * nu + nv * nv), 0.0)
        return carry

    lax.fori_loop(0, ITERS, body, 0)
    return [jnp.sum(acc_ref[0]), jnp.sum(acc_ref[1])]


def strips_kernel(own, cols, ext, xa, xb, ya, yb, isums, rows_out, cols_out, msg, rs, cs, cacc, racc, *, R, C):
    even = is_even("gx")
    a, b = xa[...], xb[...]
    top = jnp.where(even, b, a)
    bot = jnp.where(even, a, b)
    even = is_even("gy")
    a, b = ya[...], yb[...]
    left = jnp.where(even, b, a)
    right = jnp.where(even, a, b)
    for f in range(NS):
        rs[f, 0:8, :] = unpair(top, f, True)
        rs[f, 8:16, :] = own[f, 0:8, :]
        rs[f, 16:24, :] = own[f, 8:16, :]
        rs[f, 24:32, :] = unpair(bot, f, False)
        cs[f, 0:8, :] = unpair(left, f, True)
        for side in range(2):
            base = 8 * (NS * side + f)
            cs[f, 8 + 8 * side : 16 + 8 * side, 0:R] = cols[base : base + 8, :]
            cs[f, 8 + 8 * side : 16 + 8 * side, R : R + 128] = ext[base : base + 8, :]
        cs[f, 24:32, :] = unpair(right, f, False)

    def rim(shape):
        sub = lax.broadcasted_iota(jnp.int32, shape, 0)
        return ((sub >= 8) & (sub < 12)) | ((sub >= 20) & (sub < 24)), lax.broadcasted_iota(jnp.int32, shape, 1)

    band, lane = rim(rs.shape[1:])
    row_sums = strip_subcycles(rs, racc, 0, band & (lane >= ITERS) & (lane < C - ITERS))
    band, lane = rim(cs.shape[1:])
    col_sums = strip_subcycles(cs, cacc, 1, band & (lane < R))
    lane = lax.broadcasted_iota(jnp.int32, msg.shape, 1)
    totals = [jnp.sum(isums[n]) + row_sums[n] + col_sums[n] for n in range(2)]
    msg[...] = jnp.where(lane == 0, totals[0], jnp.where(lane == 1, totals[1], 0.0))
    for f in range(5):
        half = 0.5 if f == H12 else 1.0
        rows_out[f] = half * rs[f, 8:24, :]
        cols_out[f] = half * cs[f, 8:24, 0:R]


def merge_kernel(rows_in, cols_in, nvel_in, nstr_in, nvel, nstr, edge, mid, sem):
    R, C = nvel.shape[1:]
    outs = ((nvel, 0), (nvel, 1), (nstr, 0), (nstr, 1), (nstr, 2))
    inner = pl.ds(128, C - 256)

    def places(f):
        ref, lead = outs[f]
        full = ref.at[lead]
        return (
            (full.at[:, pl.ds(0, 128)], edge.at[0, f]),
            (full.at[:, pl.ds(C - 128, 128)], edge.at[1, f]),
            (full.at[pl.ds(0, 8), inner], mid.at[0, f]),
            (full.at[pl.ds(R - 8, 8), inner], mid.at[1, f]),
        )

    for f in range(5):
        for n, (there, here) in enumerate(places(f)):
            pltpu.make_async_copy(there, here, sem.at[0, n // 2]).start()
    for n, buf in enumerate((edge, mid)):
        pltpu.make_async_copy(buf, buf, sem.at[0, n]).wait()
    low = lax.broadcasted_iota(jnp.int32, (8, C), 0) < 4
    for f in range(5):
        for part in range(2):
            x = rows_in[f, 8 * part : 8 * part + 8, :]
            keep = ~low if part == 0 else low
            rows = slice(part * (R - 8), part * (R - 8) + 8)
            mid[part, f] = jnp.where(keep[:, 128 : C - 128], mid[part, f], x[:, 128 : C - 128])
            for side in range(2):
                at = slice(side * (C - 128), side * (C - 128) + 128)
                edge[side, f, rows, :] = jnp.where(keep[:, at], edge[side, f, rows, :], x[:, at])
    lane = lax.broadcasted_iota(jnp.int32, (128, 128), 1)
    for c in range(R // 128):
        rows = slice(c * 128, c * 128 + 128)
        parts = [cols_in[f, 8 * side : 8 * side + 8, rows] for side in range(2) for f in range(5)]
        x = jnp.concatenate(parts + [jnp.zeros((48, 128), F32)], 0).T
        for side in range(2):
            for f in range(5):
                shift = (120 * side - 8 * (5 * side + f)) % 128
                y = pltpu.roll(x, shift, 1) if shift else x
                hit = lane >= 124 if side else lane < 4
                edge[side, f, rows, :] = jnp.where(hit, y, edge[side, f, rows, :])
    for f in range(5):
        for n, (there, here) in enumerate(places(f)):
            pltpu.make_async_copy(here, there, sem.at[1, n // 2]).start()
    for n, buf in enumerate((edge, mid)):
        pltpu.make_async_copy(buf, buf, sem.at[1, n]).wait()


def swaps(count):
    first = [(i, i ^ 1) for i in range(count)]
    second = [(i, i + 1) for i in range(1, count - 1, 2)] + [(i + 1, i) for i in range(1, count - 1, 2)]
    return first, second


def exchange(a, b, axis):
    first, second = swaps(lax.axis_size(axis))
    return lax.ppermute(a, axis, first), lax.ppermute(b, axis, second)


def sds(*shape):
    return jax.ShapeDtypeStruct(shape, F32)


def interior(x, RB=64, L1=64, L2=128, flags=None, mib=12):
    _, R, C = x.shape
    hbm = pl.BlockSpec(memory_space=pltpu.HBM)
    vmem = pl.BlockSpec(memory_space=pltpu.VMEM)
    return pl.pallas_call(
        functools.partial(interior_kernel, RB=RB, L1=L1, L2=L2),
        in_specs=[vmem],
        out_specs=(vmem, hbm, hbm, vmem),
        out_shape=(sds(*x.shape), sds(2, R, C), sds(3, R, C), sds(2, 8, 128)),
        scratch_shapes=[pltpu.VMEM((C // 128, R + 2 * PAD, 128), F32)] * 8 + [pltpu.SemaphoreType.DMA(())],
        input_output_aliases={0: 0},
        compiler_params=pltpu.CompilerParams(vmem_limit_bytes=mib * 2**20, flags=flags),
        name="interior",
    )(x)


def per_device(velocity, stress, strength, ice_mass, wind_stress, current, ice_mask, open_water):
    args = (velocity, stress, strength, ice_mass, wind_stress, current, ice_mask, open_water)
    R, C = strength.shape
    hbm = pl.BlockSpec(memory_space=pltpu.HBM)
    vmem = pl.BlockSpec(memory_space=pltpu.VMEM)

    def limit(mib):
        return pltpu.CompilerParams(vmem_limit_bytes=mib * 2**20)

    def blocks(shape, where):
        return [pl.BlockSpec((v.shape[0],) * (v.ndim - 2) + shape, functools.partial(lambda nd, *g: (0,) * (nd - 2) + where(*g), v.ndim)) for v in args]

    edges = [pltpu.with_memory_space_constraint(v, pltpu.HBM) for v in args]
    own, xa, xb = pl.pallas_call(
        rows_kernel,
        grid=(1,),
        in_specs=blocks((8, C), lambda i: (0, 0)) + blocks((8, C), lambda i: (R // 8 - 1, 0)),
        out_specs=[pl.BlockSpec((NS, 16, C), lambda i: (0, 0, 0)), pl.BlockSpec((40, C), lambda i: (0, 0)), pl.BlockSpec((40, C), lambda i: (0, 0))],
        out_shape=[sds(NS, 16, C), sds(40, C), sds(40, C)],
        compiler_params=limit(6),
        name="row_edges",
    )(*edges, *edges)
    xa, xb, *args = lax.optimization_barrier((xa, xb, *args))
    xa, xb = exchange(xa, xb, "gx")
    x, cols = pl.pallas_call(
        load_kernel,
        in_specs=[vmem] * 8,
        out_specs=(vmem, vmem),
        out_shape=(sds(NF, R, C), sds(16 * NS, R)),
        compiler_params=limit(16),
        name="load",
    )(*args)
    ya, yb, ext = pl.pallas_call(
        corners_kernel,
        in_specs=[vmem] * 3,
        out_specs=[vmem] * 3,
        out_shape=[sds(40, R + 128), sds(40, R + 128), sds(16 * NS, 128)],
        compiler_params=limit(6),
        name="corners",
    )(cols, xa, xb)
    ya, yb = exchange(ya, yb, "gy")
    _, nvel, nstr, isums = interior(x)
    ND = lax.axis_size(ALL)
    rows_out, cols_out, msg = pl.pallas_call(
        functools.partial(strips_kernel, R=R, C=C),
        in_specs=[vmem] * 8,
        out_specs=(vmem, vmem, vmem),
        out_shape=(sds(5, 16, C), sds(5, 16, R), sds(ND, 128)),
        scratch_shapes=[
            pltpu.VMEM((NF, 32, C), F32),
            pltpu.VMEM((NF, 32, R + 128), F32),
            pltpu.VMEM((2, 32, R + 128), F32),
            pltpu.VMEM((2, 32, C), F32),
        ],
        compiler_params=limit(12),
        name="strips",
    )(own, cols, ext, xa, xb, ya, yb, isums)
    parts = lax.all_to_all(msg, ALL, 0, 0, tiled=True)
    nvel, nstr = pl.pallas_call(
        merge_kernel,
        in_specs=[vmem] * 2 + [hbm] * 2,
        out_specs=(hbm, hbm),
        out_shape=(sds(2, R, C), sds(3, R, C)),
        scratch_shapes=[pltpu.VMEM((2, 5, R, 128), F32), pltpu.VMEM((2, 5, 8, C - 256), F32), pltpu.SemaphoreType.DMA((2, 2))],
        input_output_aliases={2: 0, 3: 1},
        compiler_params=limit(12),
        name="merge",
    )(rows_out, cols_out, nvel, nstr)
    total = jnp.sum(parts, axis=0)
    cells = R * lax.axis_size("gx") * C * lax.axis_size("gy")
    return nvel, nstr, total[0] / cells, total[1] * (0.0625 / cells)


def solution(mesh):
    whole, plane = P(None, "gx", "gy"), P("gx", "gy")
    return jax.shard_map(
        per_device,
        mesh=mesh,
        in_specs=(whole, whole, plane, plane, whole, whole, plane, plane),
        out_specs=(whole, whole, P(), P()),
        check_vma=False,
    )
```

```python
import functools

import jax
import jax.numpy as jnp
from jax import lax
from jax.experimental import pallas as pl
from jax.experimental.pallas import tpu as pltpu
from jax.sharding import PartitionSpec as P

ITERS = 4
RELAX = 0.8
GROW = 1.0 / (1.0 + RELAX)
KAPPA = RELAX / (1.0 + RELAX)
PAD = 8
F32 = jnp.float32
(U_, V_, H1, H2, H12, K_, M8, FU, FV, CA, CB) = range(11)
NS = 9
NF = 11
ALL = ("gx", "gy")


def weight_of(mask, openw):
    return mask.astype(F32) * (1.0 - openw.astype(F32))


def consts(strength, mass, wind, cur, weight):
    return (KAPPA * strength) * weight, mass * 8.0, 4.0 * (wind[0] + cur[0]), 4.0 * (wind[1] + cur[1])


def coefs(m8, weight):
    a = m8 * 0.25 + 1.0
    b = m8 * 0.0375
    scale = (0.25 * weight) / (a * a + b * b)
    return a * scale, b * scale


def strain(u, v, um, vm):
    su = u + um
    du = u - um
    sv = v + vm
    dv = v - vm
    return su + dv, su - dv, du + sv, du - sv


def stress_rate(alpha, beta, gamma, alpha_m, beta_m, delta_m, k):
    d = alpha - beta_m
    t = beta - alpha_m
    s = gamma + delta_m
    q = d * d + 0.25 * (t * t + s * s) + 0.01
    r = lax.rsqrt(q)
    z = k * r
    z4 = 0.25 * z
    return z * (d - q * r), z4 * t, z4 * s


def mixes(h1, h2, h12):
    return h1 + h2, h1 - h2, h12


def spread(m, p):
    xs, xd = p[0] + m[0], p[2] - m[2]
    ys, yd = p[2] + m[2], p[1] - m[1]
    return xs + xd, xs - xd, ys + yd, ys - yd


def drift(u, v, fx, fy, m8, fu, fv, ca, cb):
    ru = m8 * u + (fx + fu)
    rv = m8 * v + (fy + fv)
    return ca * ru + cb * rv, ca * rv - cb * ru


def pair_rows(parts, high):
    half = lax.broadcasted_iota(jnp.int32, parts[0].shape, 0) < 4
    tiles = []
    for f in range(0, NS, 2):
        a = parts[f]
        b = parts[f + 1] if f + 1 < NS else jnp.zeros_like(a)
        if high:
            tiles.append(jnp.where(half, pltpu.roll(a, 4, 0), b))
        else:
            tiles.append(jnp.where(half, a, pltpu.roll(b, 4, 0)))
    return jnp.concatenate(tiles, 0)


def unpair(tiles, f, high):
    x = tiles[8 * (f // 2) : 8 * (f // 2) + 8]
    return x if (f % 2 == 1) == high else pltpu.roll(x, 4, 0)


def is_even(axis):
    return lax.axis_index(axis) % 2 == 0


def strip_fields(vel, strs, strength, mass, wind, cur, mask, openw):
    w = weight_of(mask[...], openw[...])
    k, m8, fu, fv = consts(strength[...], mass[...], (wind[0], wind[1]), (cur[0], cur[1]), w)
    return [vel[0], vel[1], strs[0], strs[1], 2.0 * strs[2], k, m8, fu, fv]


def rows_kernel(*refs):
    own, msg_a, msg_b = refs[16:]
    top = strip_fields(*refs[:8])
    bot = strip_fields(*refs[8:16])
    for f in range(NS):
        own[f, 0:8, :] = top[f]
        own[f, 8:16, :] = bot[f]
    low = pair_rows(top, False)
    high = pair_rows(bot, True)
    even = is_even("gx")
    msg_a[...] = jnp.where(even, high, low)
    msg_b[...] = jnp.where(even, low, high)


def load_kernel(vel, strs, strength, mass, wind, cur, mask, openw, x, cols):
    R, C = strength.shape

    def prepare(r0):
        rows = pl.ds(r0, 8)
        for t in range(C // 128):
            at = (rows, slice(128 * t, 128 * t + 128))
            w = weight_of(mask[at], openw[at])
            k, m8, fu, fv = consts(strength[at], mass[at], (wind[(0, *at)], wind[(1, *at)]), (cur[(0, *at)], cur[(1, *at)]), w)
            ca, cb = coefs(m8, w)
            for f, value in enumerate((k, m8, fu, fv, ca, cb)):
                x[(f, *at)] = value

    def body(i, carry):
        for n in range(4):
            prepare(pl.multiple_of(i * 32 + 8 * n, 8))
        return carry

    lax.fori_loop(0, R // 32, body, 0)
    lane = lax.broadcasted_iota(jnp.int32, (8, 128), 1)
    low = lane < 64
    fields = [(vel, 0), (vel, 1), (strs, 0), (strs, 1), (strs, 2)] + [(x, f - K_) for f in range(K_, NS)]

    def pack(p, carry):
        groups = ([], [])
        for g in range(16):
            rows = pl.ds(pl.multiple_of(p * 128 + 8 * g, 8), 8)
            packed = [None, None]
            for f, (ref, lead) in enumerate(fields):
                y = jnp.where(low, ref[lead, rows, 0:128], ref[lead, rows, C - 128 : C])
                if f == H12:
                    y = 2.0 * y
                if f:
                    y = pltpu.roll(y, 8 * f, 1)
                for side in range(2):
                    begin = 8 * (f - side) % 128
                    hit = (lane >= begin) & (lane < begin + 8)
                    packed[side] = y if packed[side] is None else jnp.where(hit, y, packed[side])
            for side in range(2):
                groups[side].append(packed[side])
        at = pl.ds(pl.multiple_of(p * 128, 128), 128)
        y = jnp.concatenate(groups[0], 0).T
        cols[0 : 8 * NS, at] = y[0 : 8 * NS]
        y = jnp.concatenate(groups[1], 0).T
        cols[8 * NS : 8 * NS + 8, at] = y[120:128]
        cols[8 * NS + 8 : 16 * NS, at] = y[0 : 8 * (NS - 1)]
        return carry

    lax.fori_loop(0, R // 128, pack, 0)


def corners_kernel(cols, xa, xb, ya, yb, ext):
    even = is_even("gx")
    a, b = xa[...], xb[...]
    top = jnp.where(even, b, a)
    bot = jnp.where(even, a, b)
    C = cols.shape[1]
    lane = lax.broadcasted_iota(jnp.int32, (8, 128), 1)
    strips = []
    for side in range(2):
        at = side * (C - 128)
        t = jnp.concatenate([top[:, at : at + 128], bot[:, at : at + 128], jnp.zeros((48, 128), F32)], 0).T
        t = t[120 * side : 120 * side + 8]
        own = []
        for f in range(NS):
            e = jnp.where(lane >= 124, pltpu.roll(t, 124 - 4 * f, 1), 0.0)
            e = jnp.where(lane < 4, pltpu.roll(t, 128 - 40 - 4 * f, 1), e)
            base = 8 * (NS * side + f)
            ext[base : base + 8, :] = e
            own.append(jnp.concatenate([cols[base : base + 8, :], e], 1))
        strips.append(pair_rows(own, side == 1))
    low, high = strips
    even = is_even("gy")
    ya[...] = jnp.where(even, high, low)
    yb[...] = jnp.where(even, low, high)


def interior_kernel(vel, strs, con, nvel, nstr, sums, x, al, be, ga, de, tx, ty, nx, ny, sem, *, RB, L1, L2):
    R, C = x.shape[1:]
    NT = C // 128
    k, m8_, fu_, fv_, ca_, cb_ = range(6)
    zero = jnp.zeros((8, 128), F32)
    for t in range(NT):
        for ref in (al, be, de):
            ref[t, 0:PAD, :] = zero
        for ref in (tx, ty):
            ref[t, PAD + R : PAD + R + 8, :] = zero
    lane = lax.broadcasted_iota(jnp.int32, (8, 128), 1)
    row_in = lax.broadcasted_iota(jnp.int32, (8, 128), 0)
    first = lane == 0
    last = lane == 127

    def tile(t):
        return slice(128 * t, 128 * t + 128)

    def strain_rows(r0, src):
        own = pl.ds(r0, 8)
        rows = pl.ds(PAD + r0, 8)
        ru = rv = None
        for t in range(NT):
            u, v = src[0, own, tile(t)], src[1, own, tile(t)]
            qu, qv = pltpu.roll(u, 1, 1), pltpu.roll(v, 1, 1)
            um = jnp.where(first, ru, qu) if t else qu
            vm = jnp.where(first, rv, qv) if t else qv
            ru, rv = qu, qv
            al[t, rows, :], be[t, rows, :], ga[t, rows, :], de[t, rows, :] = strain(u, v, um, vm)

    def rate_rows(r0, it):
        own = pl.ds(r0, 8)
        rows = pl.ds(PAD + r0, 8)
        above = pl.ds(PAD + r0 - 1, 8)

        def emit(t, m, q, nq):
            p = [jnp.where(last, nq[i], q[i]) if nq else q[i] for i in range(3)]
            tx[t, rows, :], nx[t, rows, :], ty[t, rows, :], ny[t, rows, :] = spread(m, p)

        held = None
        for t in range(NT):
            d1, d2, d12 = stress_rate(al[t, rows, :], be[t, rows, :], ga[t, rows, :], al[t, above, :], be[t, above, :], de[t, above, :], con[k, own, tile(t)])
            if it:
                old = [x[f, own, tile(t)] for f in (H1, H2, H12)]
            else:
                old = [strs[f, own, tile(t)] for f in range(3)]
            h1 = old[0] * GROW + d1
            h2 = old[1] * GROW + d2
            h12 = old[2] * (GROW if it else 2.0 * GROW) + d12
            x[H1, own, tile(t)] = h1
            x[H2, own, tile(t)] = h2
            x[H12, own, tile(t)] = 0.5 * h12 if it == ITERS - 1 else h12
            m = mixes(h1, h2, h12)
            q = [pltpu.roll(v, 127, 1) for v in m]
            if held:
                emit(t - 1, *held, q)
            held = (m, q)
        emit(NT - 1, *held, None)

    def velocity_rows(r0, src, acc):
        own = pl.ds(r0, 8)
        rows = pl.ds(PAD + r0, 8)
        below = pl.ds(PAD + r0 + 1, 8)
        for t in range(NT):
            u, v, m8 = src[0, own, tile(t)], src[1, own, tile(t)], con[m8_, own, tile(t)]
            fx = tx[t, below, :] - nx[t, rows, :]
            fy = ty[t, below, :] - ny[t, rows, :]
            nu, nv = drift(u, v, fx, fy, m8, con[fu_, own, tile(t)], con[fv_, own, tile(t)], con[ca_, own, tile(t)], con[cb_, own, tile(t)])
            x[U_, own, tile(t)] = nu
            x[V_, own, tile(t)] = nv
            if acc is not None:
                keep = (con[k, own, tile(t)] > 0.0) & (row_in + r0 >= ITERS) & (row_in + r0 < R - ITERS)
                if t == 0:
                    keep = keep & (lane >= ITERS)
                if t == NT - 1:
                    keep = keep & (lane < 128 - ITERS)
                cu, cv = nu - u, nv - v
                acc[2 * (t % 2)] += jnp.where(keep, cu * cu + cv * cv, 0.0)
                acc[2 * (t % 2) + 1] += jnp.where(keep, m8 * (nu * nu + nv * nv), 0.0)

    sent = [0]

    def send(end):
        rows = pl.ds(sent[0], end - sent[0])
        for f, (ref, lead) in enumerate(((nvel, 0), (nvel, 1), (nstr, 0), (nstr, 1), (nstr, 2))):
            pltpu.make_async_copy(x.at[f, rows], ref.at[lead, rows], sem).start()
        sent[0] = end

    acc = [zero] * 4
    peel = -(-L2 // RB) * RB
    for it in range(ITERS):
        final = it == ITERS - 1
        src, before = (x if n > 0 else vel for n in (it, it - 1))
        for r in range(0, peel, 8):
            strain_rows(r, src)
            if r >= L1:
                rate_rows(r - L1, it)
            elif it:
                rate_rows(R + r - L1, it - 1)
            if r >= L2:
                velocity_rows(r - L2, src, acc if final else None)
            elif it:
                velocity_rows(R + r - L2, before, None)

        def body(j, acc):
            r0 = pl.multiple_of(j * RB, RB)
            acc = list(acc) if final else None
            for r in range(0, RB, 8):
                strain_rows(r0 + r, src)
                rate_rows(r0 + (r - L1), it)
                velocity_rows(r0 + (r - L2), src, acc)
            return tuple(acc) if final else ()

        if not final:
            lax.fori_loop(peel // RB, R // RB, body, ())
            continue
        for j in range(peel // RB, R // RB, 2):
            acc = list(lax.fori_loop(j, min(j + 2, R // RB), body, tuple(acc)))
            send(min((j + 2) * RB, R) - L2)
    for r in range(0, L2, 8):
        if r < L1:
            rate_rows(R + r - L1, ITERS - 1)
        velocity_rows(R + r - L2, x, acc)
        if r + 8 == L2 // 2:
            send(R - L2 // 2)
    send(R)
    sums[0] = acc[0] + acc[2]
    sums[1] = acc[1] + acc[3]
    pltpu.make_async_copy(x, x, sem).wait()


def strip_begin(ref):
    w = jnp.where(ref[K_] > 0.0, 1.0, 0.0)
    ref[CA], ref[CB] = coefs(ref[M8], w)


def strip_subcycle(ref, rows_axis, keep=None):
    cols_axis = 1 - rows_axis
    back = lambda x, axis: pltpu.roll(x, 1, axis)
    ahead = lambda x, axis: pltpu.roll(x, x.shape[axis] - 1, axis)
    u, v = ref[U_], ref[V_]
    a, b, g, d = strain(u, v, back(u, cols_axis), back(v, cols_axis))
    d1, d2, d12 = stress_rate(a, b, g, back(a, rows_axis), back(b, rows_axis), back(d, rows_axis), ref[K_])
    h1 = ref[H1] * GROW + d1
    h2 = ref[H2] * GROW + d2
    h12 = ref[H12] * GROW + d12
    ref[H1], ref[H2], ref[H12] = h1, h2, h12
    m = mixes(h1, h2, h12)
    xt, xn, yt, yn = spread(m, [ahead(v, cols_axis) for v in m])
    fx = ahead(xt, rows_axis) - xn
    fy = ahead(yt, rows_axis) - yn
    m8 = ref[M8]
    nu, nv = drift(u, v, fx, fy, m8, ref[FU], ref[FV], ref[CA], ref[CB])
    ref[U_], ref[V_] = nu, nv
    if keep is None:
        return None
    cu, cv = nu - u, nv - v
    inside = keep & (ref[K_] > 0.0)
    pair = (jnp.where(inside, cu * cu + cv * cv, 0.0), jnp.where(inside, m8 * (nu * nu + nv * nv), 0.0))
    return [sum(p[i : i + 8, j : j + 128] for i in range(0, p.shape[0], 8) for j in range(0, p.shape[1], 128)) for p in pair]


def strips_kernel(own, cols, ext, xa, xb, ya, yb, isums, rows_out, cols_out, msg, rs, cs, *, R, C):
    even = is_even("gx")
    a, b = xa[...], xb[...]
    top = jnp.where(even, b, a)
    bot = jnp.where(even, a, b)
    even = is_even("gy")
    a, b = ya[...], yb[...]
    left = jnp.where(even, b, a)
    right = jnp.where(even, a, b)
    for f in range(NS):
        rs[f, 0:8, :] = unpair(top, f, True)
        rs[f, 8:16, :] = own[f, 0:8, :]
        rs[f, 16:24, :] = own[f, 8:16, :]
        rs[f, 24:32, :] = unpair(bot, f, False)
        cs[f, 0:8, :] = unpair(left, f, True)
        for side in range(2):
            base = 8 * (NS * side + f)
            cs[f, 8 + 8 * side : 16 + 8 * side, 0:R] = cols[base : base + 8, :]
            cs[f, 8 + 8 * side : 16 + 8 * side, R : R + 128] = ext[base : base + 8, :]
        cs[f, 24:32, :] = unpair(right, f, False)

    def rim(shape):
        sub = lax.broadcasted_iota(jnp.int32, shape, 0)
        return ((sub >= 8) & (sub < 12)) | ((sub >= 20) & (sub < 24)), lax.broadcasted_iota(jnp.int32, shape, 1)

    strip_begin(rs)
    strip_begin(cs)

    def body(_, carry):
        strip_subcycle(rs, 0)
        strip_subcycle(cs, 1)
        return carry

    lax.fori_loop(0, ITERS - 1, body, 0)
    band, lane = rim(rs.shape[1:])
    row_sums = strip_subcycle(rs, 0, band & (lane >= ITERS) & (lane < C - ITERS))
    band, lane = rim(cs.shape[1:])
    col_sums = strip_subcycle(cs, 1, band & (lane < R))
    lane = lax.broadcasted_iota(jnp.int32, msg.shape, 1)
    totals = [jnp.sum(isums[n] + row_sums[n] + col_sums[n]) for n in range(2)]
    msg[...] = jnp.where(lane == 0, totals[0], jnp.where(lane == 1, totals[1], 0.0))
    for f in range(5):
        half = 0.5 if f == H12 else 1.0
        rows_out[f] = half * rs[f, 8:24, :]
        cols_out[f] = half * cs[f, 8:24, 0:R]


def merge_kernel(rows_in, cols_in, nvel_in, nstr_in, nvel, nstr, edge, mid, sem):
    R, C = nvel.shape[1:]
    outs = ((nvel, 0), (nvel, 1), (nstr, 0), (nstr, 1), (nstr, 2))
    inner = pl.ds(128, C - 256)

    def places(f):
        ref, lead = outs[f]
        full = ref.at[lead]
        return (
            (full.at[:, pl.ds(0, 128)], edge.at[0, f]),
            (full.at[:, pl.ds(C - 128, 128)], edge.at[1, f]),
            (full.at[pl.ds(0, 8), inner], mid.at[0, f]),
            (full.at[pl.ds(R - 8, 8), inner], mid.at[1, f]),
        )

    for f in range(5):
        for n, (there, here) in enumerate(places(f)):
            pltpu.make_async_copy(there, here, sem.at[0, n // 2]).start()
    for n, buf in enumerate((edge, mid)):
        pltpu.make_async_copy(buf, buf, sem.at[0, n]).wait()
    low = lax.broadcasted_iota(jnp.int32, (8, C), 0) < 4
    for f in range(5):
        for part in range(2):
            x = rows_in[f, 8 * part : 8 * part + 8, :]
            keep = ~low if part == 0 else low
            rows = slice(part * (R - 8), part * (R - 8) + 8)
            mid[part, f] = jnp.where(keep[:, 128 : C - 128], mid[part, f], x[:, 128 : C - 128])
            for side in range(2):
                at = slice(side * (C - 128), side * (C - 128) + 128)
                edge[side, f, rows, :] = jnp.where(keep[:, at], edge[side, f, rows, :], x[:, at])
    lane = lax.broadcasted_iota(jnp.int32, (128, 128), 1)
    for c in range(R // 128):
        rows = slice(c * 128, c * 128 + 128)
        parts = [cols_in[f, 8 * side : 8 * side + 8, rows] for side in range(2) for f in range(5)]
        x = jnp.concatenate(parts + [jnp.zeros((48, 128), F32)], 0).T
        for side in range(2):
            for f in range(5):
                shift = (120 * side - 8 * (5 * side + f)) % 128
                y = pltpu.roll(x, shift, 1) if shift else x
                hit = lane >= 124 if side else lane < 4
                edge[side, f, rows, :] = jnp.where(hit, y, edge[side, f, rows, :])
    for f in range(5):
        for n, (there, here) in enumerate(places(f)):
            pltpu.make_async_copy(here, there, sem.at[1, n // 2]).start()
    for n, buf in enumerate((edge, mid)):
        pltpu.make_async_copy(buf, buf, sem.at[1, n]).wait()


def swaps(count):
    first = [(i, i ^ 1) for i in range(count)]
    second = [(i, i + 1) for i in range(1, count - 1, 2)] + [(i + 1, i) for i in range(1, count - 1, 2)]
    return first, second


def exchange(a, b, axis):
    first, second = swaps(lax.axis_size(axis))
    return lax.ppermute(a, axis, first), lax.ppermute(b, axis, second)


def sds(*shape):
    return jax.ShapeDtypeStruct(shape, F32)


def interior(vel, strs, con, RB=64, L1=64, L2=128, flags=None, mib=16):
    _, R, C = con.shape
    hbm = pl.BlockSpec(memory_space=pltpu.HBM)
    vmem = pl.BlockSpec(memory_space=pltpu.VMEM)
    return pl.pallas_call(
        functools.partial(interior_kernel, RB=RB, L1=L1, L2=L2),
        in_specs=[vmem] * 3,
        out_specs=(hbm, hbm, vmem),
        out_shape=(sds(2, R, C), sds(3, R, C), sds(2, 8, 128)),
        scratch_shapes=[pltpu.VMEM((5, R, C), F32)] + [pltpu.VMEM((C // 128, R + 2 * PAD, 128), F32)] * 8 + [pltpu.SemaphoreType.DMA(())],
        compiler_params=pltpu.CompilerParams(vmem_limit_bytes=mib * 2**20, flags=flags),
        name="interior",
    )(vel, strs, con)


def per_device(velocity, stress, strength, ice_mass, wind_stress, current, ice_mask, open_water):
    args = (velocity, stress, strength, ice_mass, wind_stress, current, ice_mask, open_water)
    R, C = strength.shape
    hbm = pl.BlockSpec(memory_space=pltpu.HBM)
    vmem = pl.BlockSpec(memory_space=pltpu.VMEM)

    def limit(mib):
        return pltpu.CompilerParams(vmem_limit_bytes=mib * 2**20)

    def blocks(shape, where):
        return [pl.BlockSpec((v.shape[0],) * (v.ndim - 2) + shape, functools.partial(lambda nd, *g: (0,) * (nd - 2) + where(*g), v.ndim)) for v in args]

    edges = [pltpu.with_memory_space_constraint(v, pltpu.HBM) for v in args]
    own, xa, xb = pl.pallas_call(
        rows_kernel,
        grid=(1,),
        in_specs=blocks((8, C), lambda i: (0, 0)) + blocks((8, C), lambda i: (R // 8 - 1, 0)),
        out_specs=[pl.BlockSpec((NS, 16, C), lambda i: (0, 0, 0)), pl.BlockSpec((40, C), lambda i: (0, 0)), pl.BlockSpec((40, C), lambda i: (0, 0))],
        out_shape=[sds(NS, 16, C), sds(40, C), sds(40, C)],
        compiler_params=limit(6),
        name="row_edges",
    )(*edges, *edges)
    xa, xb, *args = lax.optimization_barrier((xa, xb, *args))
    xa, xb = exchange(xa, xb, "gx")
    con, cols = pl.pallas_call(
        load_kernel,
        in_specs=[vmem] * 8,
        out_specs=(vmem, vmem),
        out_shape=(sds(6, R, C), sds(16 * NS, R)),
        compiler_params=limit(16),
        name="load",
    )(*args)
    ya, yb, ext = pl.pallas_call(
        corners_kernel,
        in_specs=[vmem] * 3,
        out_specs=[vmem] * 3,
        out_shape=[sds(40, R + 128), sds(40, R + 128), sds(16 * NS, 128)],
        compiler_params=limit(6),
        name="corners",
    )(cols, xa, xb)
    ya, yb = exchange(ya, yb, "gy")
    nvel, nstr, isums = interior(args[0], args[1], con)
    ND = lax.axis_size(ALL)
    rows_out, cols_out, msg = pl.pallas_call(
        functools.partial(strips_kernel, R=R, C=C),
        in_specs=[vmem] * 8,
        out_specs=(vmem, vmem, vmem),
        out_shape=(sds(5, 16, C), sds(5, 16, R), sds(ND, 128)),
        scratch_shapes=[
            pltpu.VMEM((NF, 32, C), F32),
            pltpu.VMEM((NF, 32, R + 128), F32),
        ],
        compiler_params=limit(12),
        name="strips",
    )(own, cols, ext, xa, xb, ya, yb, isums)
    parts = lax.all_to_all(msg, ALL, 0, 0, tiled=True)
    nvel, nstr = pl.pallas_call(
        merge_kernel,
        in_specs=[vmem] * 2 + [hbm] * 2,
        out_specs=(hbm, hbm),
        out_shape=(sds(2, R, C), sds(3, R, C)),
        scratch_shapes=[pltpu.VMEM((2, 5, R, 128), F32), pltpu.VMEM((2, 5, 8, C - 256), F32), pltpu.SemaphoreType.DMA((2, 2))],
        input_output_aliases={2: 0, 3: 1},
        compiler_params=limit(12),
        name="merge",
    )(rows_out, cols_out, nvel, nstr)
    total = jnp.sum(parts, axis=0)
    cells = R * lax.axis_size("gx") * C * lax.axis_size("gy")
    return nvel, nstr, total[0] / cells, total[1] * (0.0625 / cells)


def solution(mesh):
    whole, plane = P(None, "gx", "gy"), P("gx", "gy")
    return jax.shard_map(
        per_device,
        mesh=mesh,
        in_specs=(whole, whole, plane, plane, whole, whole, plane, plane),
        out_specs=(whole, whole, P(), P()),
        check_vma=False,
    )
```

```python
import functools

import jax
import jax.numpy as jnp
from jax import lax
from jax.experimental import pallas as pl
from jax.experimental.pallas import tpu as pltpu
from jax.sharding import PartitionSpec as P

ITERS = 4
RELAX = 0.8
GROW = 1.0 / (1.0 + RELAX)
KAPPA = RELAX / (1.0 + RELAX)
PAD = 8
F32 = jnp.float32
(U_, V_, H1, H2, H12, K_, M8, FU, FV, CA, CB) = range(11)
NS = 9
NF = 11
ALL = ("gx", "gy")


def weight_of(mask, openw):
    return mask.astype(F32) * (1.0 - openw.astype(F32))


def consts(strength, mass, wind, cur, weight):
    return (KAPPA * strength) * weight, mass * 8.0, 4.0 * (wind[0] + cur[0]), 4.0 * (wind[1] + cur[1])


def coefs(m8, weight):
    a = m8 * 0.25 + 1.0
    b = m8 * 0.0375
    scale = (0.25 * weight) / (a * a + b * b)
    return a * scale, b * scale


def strain(u, v, um, vm):
    su = u + um
    du = u - um
    sv = v + vm
    dv = v - vm
    return su + dv, su - dv, du + sv, du - sv


def stress_rate(alpha, beta, gamma, alpha_m, beta_m, delta_m, k):
    d = alpha - beta_m
    t = beta - alpha_m
    s = gamma + delta_m
    q = d * d + 0.25 * (t * t + s * s) + 0.01
    r = lax.rsqrt(q)
    z = k * r
    z4 = 0.25 * z
    return z * (d - q * r), z4 * t, z4 * s


def mixes(h1, h2, h12):
    return h1 + h2, h1 - h2, h12


def spread(m, p):
    xs, xd = p[0] + m[0], p[2] - m[2]
    ys, yd = p[2] + m[2], p[1] - m[1]
    return xs + xd, xs - xd, ys + yd, ys - yd


def drift(u, v, fx, fy, m8, fu, fv, ca, cb):
    ru = m8 * u + (fx + fu)
    rv = m8 * v + (fy + fv)
    return ca * ru + cb * rv, ca * rv - cb * ru


def pair_rows(parts, high):
    half = lax.broadcasted_iota(jnp.int32, parts[0].shape, 0) < 4
    tiles = []
    for f in range(0, NS, 2):
        a = parts[f]
        b = parts[f + 1] if f + 1 < NS else jnp.zeros_like(a)
        if high:
            tiles.append(jnp.where(half, pltpu.roll(a, 4, 0), b))
        else:
            tiles.append(jnp.where(half, a, pltpu.roll(b, 4, 0)))
    return jnp.concatenate(tiles, 0)


def unpair(tiles, f, high):
    x = tiles[8 * (f // 2) : 8 * (f // 2) + 8]
    return x if (f % 2 == 1) == high else pltpu.roll(x, 4, 0)


def is_even(axis):
    return lax.axis_index(axis) % 2 == 0


def strip_fields(vel, strs, strength, mass, wind, cur, mask, openw):
    w = weight_of(mask[...], openw[...])
    k, m8, fu, fv = consts(strength[...], mass[...], (wind[0], wind[1]), (cur[0], cur[1]), w)
    return [vel[0], vel[1], strs[0], strs[1], 2.0 * strs[2], k, m8, fu, fv]


def rows_kernel(*refs):
    own, msg_a, msg_b = refs[16:]
    top = strip_fields(*refs[:8])
    bot = strip_fields(*refs[8:16])
    for f in range(NS):
        own[f, 0:8, :] = top[f]
        own[f, 8:16, :] = bot[f]
    low = pair_rows(top, False)
    high = pair_rows(bot, True)
    even = is_even("gx")
    msg_a[...] = jnp.where(even, high, low)
    msg_b[...] = jnp.where(even, low, high)


def load_kernel(vel, strs, strength, mass, wind, cur, mask, openw, x, cols):
    R, C = strength.shape

    def prepare(r0):
        rows = pl.ds(r0, 8)
        for t in range(C // 128):
            at = (rows, slice(128 * t, 128 * t + 128))
            w = weight_of(mask[at], openw[at])
            k, m8, fu, fv = consts(strength[at], mass[at], (wind[(0, *at)], wind[(1, *at)]), (cur[(0, *at)], cur[(1, *at)]), w)
            ca, cb = coefs(m8, w)
            for f, value in enumerate((k, m8, fu, fv, ca, cb)):
                x[(f, *at)] = value

    def body(i, carry):
        for n in range(4):
            prepare(pl.multiple_of(i * 32 + 8 * n, 8))
        return carry

    lax.fori_loop(0, R // 32, body, 0)
    lane = lax.broadcasted_iota(jnp.int32, (8, 128), 1)
    low = lane < 64
    fields = [(vel, 0), (vel, 1), (strs, 0), (strs, 1), (strs, 2)] + [(x, f - K_) for f in range(K_, NS)]

    def pack(p, carry):
        groups = ([], [])
        for g in range(16):
            rows = pl.ds(pl.multiple_of(p * 128 + 8 * g, 8), 8)
            packed = [None, None]
            for f, (ref, lead) in enumerate(fields):
                y = jnp.where(low, ref[lead, rows, 0:128], ref[lead, rows, C - 128 : C])
                if f == H12:
                    y = 2.0 * y
                if f:
                    y = pltpu.roll(y, 8 * f, 1)
                for side in range(2):
                    begin = 8 * (f - side) % 128
                    hit = (lane >= begin) & (lane < begin + 8)
                    packed[side] = y if packed[side] is None else jnp.where(hit, y, packed[side])
            for side in range(2):
                groups[side].append(packed[side])
        at = pl.ds(pl.multiple_of(p * 128, 128), 128)
        y = jnp.concatenate(groups[0], 0).T
        cols[0 : 8 * NS, at] = y[0 : 8 * NS]
        y = jnp.concatenate(groups[1], 0).T
        cols[8 * NS : 8 * NS + 8, at] = y[120:128]
        cols[8 * NS + 8 : 16 * NS, at] = y[0 : 8 * (NS - 1)]
        return carry

    lax.fori_loop(0, R // 128, pack, 0)


def corners_kernel(cols, xa, xb, ya, yb, ext):
    even = is_even("gx")
    a, b = xa[...], xb[...]
    top = jnp.where(even, b, a)
    bot = jnp.where(even, a, b)
    C = cols.shape[1]
    lane = lax.broadcasted_iota(jnp.int32, (8, 128), 1)
    strips = []
    for side in range(2):
        at = side * (C - 128)
        t = jnp.concatenate([top[:, at : at + 128], bot[:, at : at + 128], jnp.zeros((48, 128), F32)], 0).T
        t = t[120 * side : 120 * side + 8]
        own = []
        for f in range(NS):
            e = jnp.where(lane >= 124, pltpu.roll(t, 124 - 4 * f, 1), 0.0)
            e = jnp.where(lane < 4, pltpu.roll(t, 128 - 40 - 4 * f, 1), e)
            base = 8 * (NS * side + f)
            ext[base : base + 8, :] = e
            own.append(jnp.concatenate([cols[base : base + 8, :], e], 1))
        strips.append(pair_rows(own, side == 1))
    low, high = strips
    even = is_even("gy")
    ya[...] = jnp.where(even, high, low)
    yb[...] = jnp.where(even, low, high)


def sweep_subcycles(its, vel, strs, con, x, nvel, nstr, sums, al, be, ga, de, tx, ty, nx, ny, sem, *, RB, L1, L2):
    R, C = x.shape[1:]
    NT = C // 128
    k, m8_, fu_, fv_, ca_, cb_ = range(6)
    zero = jnp.zeros((8, 128), F32)
    for t in range(NT):
        for ref in (al, be, de):
            ref[t, 0:PAD, :] = zero
        for ref in (tx, ty):
            ref[t, PAD + R : PAD + R + 8, :] = zero
    lane = lax.broadcasted_iota(jnp.int32, (8, 128), 1)
    row_in = lax.broadcasted_iota(jnp.int32, (8, 128), 0)
    first = lane == 0
    last = lane == 127

    def tile(t):
        return slice(128 * t, 128 * t + 128)

    def strain_rows(r0, src):
        own = pl.ds(r0, 8)
        rows = pl.ds(PAD + r0, 8)
        ru = rv = None
        for t in range(NT):
            u, v = src[0, own, tile(t)], src[1, own, tile(t)]
            qu, qv = pltpu.roll(u, 1, 1), pltpu.roll(v, 1, 1)
            um = jnp.where(first, ru, qu) if t else qu
            vm = jnp.where(first, rv, qv) if t else qv
            ru, rv = qu, qv
            al[t, rows, :], be[t, rows, :], ga[t, rows, :], de[t, rows, :] = strain(u, v, um, vm)

    def rate_rows(r0, it):
        own = pl.ds(r0, 8)
        rows = pl.ds(PAD + r0, 8)
        above = pl.ds(PAD + r0 - 1, 8)

        def emit(t, m, q, nq):
            p = [jnp.where(last, nq[i], q[i]) if nq else q[i] for i in range(3)]
            tx[t, rows, :], nx[t, rows, :], ty[t, rows, :], ny[t, rows, :] = spread(m, p)

        held = None
        for t in range(NT):
            d1, d2, d12 = stress_rate(al[t, rows, :], be[t, rows, :], ga[t, rows, :], al[t, above, :], be[t, above, :], de[t, above, :], con[k, own, tile(t)])
            if it:
                old = [x[f, own, tile(t)] for f in (H1, H2, H12)]
            else:
                old = [strs[f, own, tile(t)] for f in range(3)]
            h1 = old[0] * GROW + d1
            h2 = old[1] * GROW + d2
            h12 = old[2] * (GROW if it else 2.0 * GROW) + d12
            x[H1, own, tile(t)] = h1
            x[H2, own, tile(t)] = h2
            x[H12, own, tile(t)] = 0.5 * h12 if it == ITERS - 1 else h12
            m = mixes(h1, h2, h12)
            q = [pltpu.roll(v, 127, 1) for v in m]
            if held:
                emit(t - 1, *held, q)
            held = (m, q)
        emit(NT - 1, *held, None)

    def velocity_rows(r0, src, acc):
        own = pl.ds(r0, 8)
        rows = pl.ds(PAD + r0, 8)
        below = pl.ds(PAD + r0 + 1, 8)
        for t in range(NT):
            u, v, m8 = src[0, own, tile(t)], src[1, own, tile(t)], con[m8_, own, tile(t)]
            fx = tx[t, below, :] - nx[t, rows, :]
            fy = ty[t, below, :] - ny[t, rows, :]
            nu, nv = drift(u, v, fx, fy, m8, con[fu_, own, tile(t)], con[fv_, own, tile(t)], con[ca_, own, tile(t)], con[cb_, own, tile(t)])
            x[U_, own, tile(t)] = nu
            x[V_, own, tile(t)] = nv
            if acc is not None:
                keep = (con[k, own, tile(t)] > 0.0) & (row_in + r0 >= ITERS) & (row_in + r0 < R - ITERS)
                if t == 0:
                    keep = keep & (lane >= ITERS)
                if t == NT - 1:
                    keep = keep & (lane < 128 - ITERS)
                cu, cv = nu - u, nv - v
                acc[2 * (t % 2)] += jnp.where(keep, cu * cu + cv * cv, 0.0)
                acc[2 * (t % 2) + 1] += jnp.where(keep, m8 * (nu * nu + nv * nv), 0.0)

    sent = [0]

    def send(end):
        rows = pl.ds(sent[0], end - sent[0])
        for f, (ref, lead) in enumerate(((nvel, 0), (nvel, 1), (nstr, 0), (nstr, 1), (nstr, 2))):
            pltpu.make_async_copy(x.at[f, rows], ref.at[lead, rows], sem).start()
        sent[0] = end

    acc = [zero] * 4
    peel = -(-L2 // RB) * RB
    for it in its:
        start = it == its[0]
        final = it == ITERS - 1
        src, before = (x if n > 0 else vel for n in (it, it - 1))
        for r in range(0, peel, 8):
            strain_rows(r, src)
            if r >= L1:
                rate_rows(r - L1, it)
            elif not start:
                rate_rows(R + r - L1, it - 1)
            if r >= L2:
                velocity_rows(r - L2, src, acc if final else None)
            elif not start:
                velocity_rows(R + r - L2, before, None)

        def body(j, acc):
            r0 = pl.multiple_of(j * RB, RB)
            acc = list(acc) if final else None
            for r in range(0, RB, 8):
                strain_rows(r0 + r, src)
                rate_rows(r0 + (r - L1), it)
                velocity_rows(r0 + (r - L2), src, acc)
            return tuple(acc) if final else ()

        if not final:
            lax.fori_loop(peel // RB, R // RB, body, ())
            continue
        for j in range(peel // RB, R // RB, 2):
            acc = list(lax.fori_loop(j, min(j + 2, R // RB), body, tuple(acc)))
            send(min((j + 2) * RB, R) - L2)
    for r in range(0, L2, 8):
        if r < L1:
            rate_rows(R + r - L1, its[-1])
        velocity_rows(R + r - L2, src, acc if final else None)
        if final and r + 8 == L2 // 2:
            send(R - L2 // 2)
    if not final:
        return
    send(R)
    sums[0] = acc[0] + acc[2]
    sums[1] = acc[1] + acc[3]
    pltpu.make_async_copy(x, x, sem).wait()


def first_kernel(vel, strs, con, x, *work, **kw):
    sweep_subcycles([0], vel, strs, con, x, None, None, None, *work, None, **kw)


def rest_kernel(x_in, con, x, nvel, nstr, sums, *work, **kw):
    sweep_subcycles(list(range(1, ITERS)), None, None, con, x, nvel, nstr, sums, *work, **kw)


def strip_begin(ref):
    w = jnp.where(ref[K_] > 0.0, 1.0, 0.0)
    ref[CA], ref[CB] = coefs(ref[M8], w)


def strip_subcycle(ref, rows_axis, keep=None):
    cols_axis = 1 - rows_axis
    back = lambda x, axis: pltpu.roll(x, 1, axis)
    ahead = lambda x, axis: pltpu.roll(x, x.shape[axis] - 1, axis)
    u, v = ref[U_], ref[V_]
    a, b, g, d = strain(u, v, back(u, cols_axis), back(v, cols_axis))
    d1, d2, d12 = stress_rate(a, b, g, back(a, rows_axis), back(b, rows_axis), back(d, rows_axis), ref[K_])
    h1 = ref[H1] * GROW + d1
    h2 = ref[H2] * GROW + d2
    h12 = ref[H12] * GROW + d12
    ref[H1], ref[H2], ref[H12] = h1, h2, h12
    m = mixes(h1, h2, h12)
    xt, xn, yt, yn = spread(m, [ahead(v, cols_axis) for v in m])
    fx = ahead(xt, rows_axis) - xn
    fy = ahead(yt, rows_axis) - yn
    m8 = ref[M8]
    nu, nv = drift(u, v, fx, fy, m8, ref[FU], ref[FV], ref[CA], ref[CB])
    ref[U_], ref[V_] = nu, nv
    if keep is None:
        return None
    cu, cv = nu - u, nv - v
    inside = keep & (ref[K_] > 0.0)
    pair = (jnp.where(inside, cu * cu + cv * cv, 0.0), jnp.where(inside, m8 * (nu * nu + nv * nv), 0.0))
    return [sum(p[i : i + 8, j : j + 128] for i in range(0, p.shape[0], 8) for j in range(0, p.shape[1], 128)) for p in pair]


def strips_kernel(own, cols, ext, xa, xb, ya, yb, isums, rows_out, cols_out, msg, rs, cs, *, R, C):
    even = is_even("gx")
    a, b = xa[...], xb[...]
    top = jnp.where(even, b, a)
    bot = jnp.where(even, a, b)
    even = is_even("gy")
    a, b = ya[...], yb[...]
    left = jnp.where(even, b, a)
    right = jnp.where(even, a, b)
    for f in range(NS):
        rs[f, 0:8, :] = unpair(top, f, True)
        rs[f, 8:16, :] = own[f, 0:8, :]
        rs[f, 16:24, :] = own[f, 8:16, :]
        rs[f, 24:32, :] = unpair(bot, f, False)
        cs[f, 0:8, :] = unpair(left, f, True)
        for side in range(2):
            base = 8 * (NS * side + f)
            cs[f, 8 + 8 * side : 16 + 8 * side, 0:R] = cols[base : base + 8, :]
            cs[f, 8 + 8 * side : 16 + 8 * side, R : R + 128] = ext[base : base + 8, :]
        cs[f, 24:32, :] = unpair(right, f, False)

    def rim(shape):
        sub = lax.broadcasted_iota(jnp.int32, shape, 0)
        return ((sub >= 8) & (sub < 12)) | ((sub >= 20) & (sub < 24)), lax.broadcasted_iota(jnp.int32, shape, 1)

    strip_begin(rs)
    strip_begin(cs)

    def body(_, carry):
        strip_subcycle(rs, 0)
        strip_subcycle(cs, 1)
        return carry

    lax.fori_loop(0, ITERS - 1, body, 0)
    band, lane = rim(rs.shape[1:])
    row_sums = strip_subcycle(rs, 0, band & (lane >= ITERS) & (lane < C - ITERS))
    band, lane = rim(cs.shape[1:])
    col_sums = strip_subcycle(cs, 1, band & (lane < R))
    lane = lax.broadcasted_iota(jnp.int32, msg.shape, 1)
    totals = [jnp.sum(isums[n] + row_sums[n] + col_sums[n]) for n in range(2)]
    msg[...] = jnp.where(lane == 0, totals[0], jnp.where(lane == 1, totals[1], 0.0))
    for f in range(5):
        half = 0.5 if f == H12 else 1.0
        rows_out[f] = half * rs[f, 8:24, :]
        cols_out[f] = half * cs[f, 8:24, 0:R]


def merge_kernel(rows_in, cols_in, nvel_in, nstr_in, nvel, nstr, edge, mid, sem):
    R, C = nvel.shape[1:]
    outs = ((nvel, 0), (nvel, 1), (nstr, 0), (nstr, 1), (nstr, 2))
    inner = pl.ds(128, C - 256)

    def places(f):
        ref, lead = outs[f]
        full = ref.at[lead]
        return (
            (full.at[:, pl.ds(0, 128)], edge.at[0, f]),
            (full.at[:, pl.ds(C - 128, 128)], edge.at[1, f]),
            (full.at[pl.ds(0, 8), inner], mid.at[0, f]),
            (full.at[pl.ds(R - 8, 8), inner], mid.at[1, f]),
        )

    for f in range(5):
        for n, (there, here) in enumerate(places(f)):
            pltpu.make_async_copy(there, here, sem.at[0, n // 2]).start()
    for n, buf in enumerate((edge, mid)):
        pltpu.make_async_copy(buf, buf, sem.at[0, n]).wait()
    low = lax.broadcasted_iota(jnp.int32, (8, C), 0) < 4
    for f in range(5):
        for part in range(2):
            x = rows_in[f, 8 * part : 8 * part + 8, :]
            keep = ~low if part == 0 else low
            rows = slice(part * (R - 8), part * (R - 8) + 8)
            mid[part, f] = jnp.where(keep[:, 128 : C - 128], mid[part, f], x[:, 128 : C - 128])
            for side in range(2):
                at = slice(side * (C - 128), side * (C - 128) + 128)
                edge[side, f, rows, :] = jnp.where(keep[:, at], edge[side, f, rows, :], x[:, at])
    lane = lax.broadcasted_iota(jnp.int32, (128, 128), 1)
    for c in range(R // 128):
        rows = slice(c * 128, c * 128 + 128)
        parts = [cols_in[f, 8 * side : 8 * side + 8, rows] for side in range(2) for f in range(5)]
        x = jnp.concatenate(parts + [jnp.zeros((48, 128), F32)], 0).T
        for side in range(2):
            for f in range(5):
                shift = (120 * side - 8 * (5 * side + f)) % 128
                y = pltpu.roll(x, shift, 1) if shift else x
                hit = lane >= 124 if side else lane < 4
                edge[side, f, rows, :] = jnp.where(hit, y, edge[side, f, rows, :])
    for f in range(5):
        for n, (there, here) in enumerate(places(f)):
            pltpu.make_async_copy(here, there, sem.at[1, n // 2]).start()
    for n, buf in enumerate((edge, mid)):
        pltpu.make_async_copy(buf, buf, sem.at[1, n]).wait()


def swaps(count):
    first = [(i, i ^ 1) for i in range(count)]
    second = [(i, i + 1) for i in range(1, count - 1, 2)] + [(i + 1, i) for i in range(1, count - 1, 2)]
    return first, second


def exchange(a, b, axis):
    first, second = swaps(lax.axis_size(axis))
    return lax.ppermute(a, axis, first), lax.ppermute(b, axis, second)


def sds(*shape):
    return jax.ShapeDtypeStruct(shape, F32)


def interior_first(vel, strs, con, RB=64, L1=64, L2=128):
    _, R, C = con.shape
    vmem = pl.BlockSpec(memory_space=pltpu.VMEM)
    return pl.pallas_call(
        functools.partial(first_kernel, RB=RB, L1=L1, L2=L2),
        in_specs=[vmem] * 3,
        out_specs=vmem,
        out_shape=sds(5, R, C),
        scratch_shapes=[pltpu.VMEM((C // 128, R + 2 * PAD, 128), F32)] * 8,
        compiler_params=pltpu.CompilerParams(vmem_limit_bytes=12 * 2**20),
        name="first",
    )(vel, strs, con)


def interior_rest(x, con, RB=64, L1=64, L2=128):
    _, R, C = con.shape
    hbm = pl.BlockSpec(memory_space=pltpu.HBM)
    vmem = pl.BlockSpec(memory_space=pltpu.VMEM)
    return pl.pallas_call(
        functools.partial(rest_kernel, RB=RB, L1=L1, L2=L2),
        in_specs=[vmem] * 2,
        out_specs=(vmem, hbm, hbm, vmem),
        out_shape=(sds(5, R, C), sds(2, R, C), sds(3, R, C), sds(2, 8, 128)),
        scratch_shapes=[pltpu.VMEM((C // 128, R + 2 * PAD, 128), F32)] * 8 + [pltpu.SemaphoreType.DMA(())],
        input_output_aliases={0: 0},
        compiler_params=pltpu.CompilerParams(vmem_limit_bytes=12 * 2**20),
        name="rest",
    )(x, con)


def per_device(velocity, stress, strength, ice_mass, wind_stress, current, ice_mask, open_water):
    args = (velocity, stress, strength, ice_mass, wind_stress, current, ice_mask, open_water)
    R, C = strength.shape
    hbm = pl.BlockSpec(memory_space=pltpu.HBM)
    vmem = pl.BlockSpec(memory_space=pltpu.VMEM)

    def limit(mib):
        return pltpu.CompilerParams(vmem_limit_bytes=mib * 2**20)

    def blocks(shape, where):
        return [pl.BlockSpec((v.shape[0],) * (v.ndim - 2) + shape, functools.partial(lambda nd, *g: (0,) * (nd - 2) + where(*g), v.ndim)) for v in args]

    edges = [pltpu.with_memory_space_constraint(v, pltpu.HBM) for v in args]
    own, xa, xb = pl.pallas_call(
        rows_kernel,
        grid=(1,),
        in_specs=blocks((8, C), lambda i: (0, 0)) + blocks((8, C), lambda i: (R // 8 - 1, 0)),
        out_specs=[pl.BlockSpec((NS, 16, C), lambda i: (0, 0, 0)), pl.BlockSpec((40, C), lambda i: (0, 0)), pl.BlockSpec((40, C), lambda i: (0, 0))],
        out_shape=[sds(NS, 16, C), sds(40, C), sds(40, C)],
        compiler_params=limit(6),
        name="row_edges",
    )(*edges, *edges)
    xa, xb, *args = lax.optimization_barrier((xa, xb, *args))
    xa, xb = exchange(xa, xb, "gx")
    con, cols = pl.pallas_call(
        load_kernel,
        in_specs=[vmem] * 8,
        out_specs=(vmem, vmem),
        out_shape=(sds(6, R, C), sds(16 * NS, R)),
        compiler_params=limit(16),
        name="load",
    )(*args)
    x = interior_first(args[0], args[1], con)
    cols, x = lax.optimization_barrier((cols, x))
    ya, yb, ext = pl.pallas_call(
        corners_kernel,
        in_specs=[vmem] * 3,
        out_specs=[vmem] * 3,
        out_shape=[sds(40, R + 128), sds(40, R + 128), sds(16 * NS, 128)],
        compiler_params=limit(6),
        name="corners",
    )(cols, xa, xb)
    ya, yb = exchange(ya, yb, "gy")
    _, nvel, nstr, isums = interior_rest(x, con)
    ND = lax.axis_size(ALL)
    rows_out, cols_out, msg = pl.pallas_call(
        functools.partial(strips_kernel, R=R, C=C),
        in_specs=[vmem] * 8,
        out_specs=(vmem, vmem, vmem),
        out_shape=(sds(5, 16, C), sds(5, 16, R), sds(ND, 128)),
        scratch_shapes=[
            pltpu.VMEM((NF, 32, C), F32),
            pltpu.VMEM((NF, 32, R + 128), F32),
        ],
        compiler_params=limit(12),
        name="strips",
    )(own, cols, ext, xa, xb, ya, yb, isums)
    parts = lax.all_to_all(msg, ALL, 0, 0, tiled=True)
    nvel, nstr = pl.pallas_call(
        merge_kernel,
        in_specs=[vmem] * 2 + [hbm] * 2,
        out_specs=(hbm, hbm),
        out_shape=(sds(2, R, C), sds(3, R, C)),
        scratch_shapes=[pltpu.VMEM((2, 5, R, 128), F32), pltpu.VMEM((2, 5, 8, C - 256), F32), pltpu.SemaphoreType.DMA((2, 2))],
        input_output_aliases={2: 0, 3: 1},
        compiler_params=limit(12),
        name="merge",
    )(rows_out, cols_out, nvel, nstr)
    total = jnp.sum(parts, axis=0)
    cells = R * lax.axis_size("gx") * C * lax.axis_size("gy")
    return nvel, nstr, total[0] / cells, total[1] * (0.0625 / cells)


def solution(mesh):
    whole, plane = P(None, "gx", "gy"), P("gx", "gy")
    return jax.shard_map(
        per_device,
        mesh=mesh,
        in_specs=(whole, whole, plane, plane, whole, whole, plane, plane),
        out_specs=(whole, whole, P(), P()),
        check_vma=False,
    )
```

```python
import functools

import jax
import jax.numpy as jnp
from jax import lax
from jax.experimental import pallas as pl
from jax.experimental.pallas import tpu as pltpu
from jax.sharding import PartitionSpec as P

ITERS = 4
RELAX = 0.8
GROW = 1.0 / (1.0 + RELAX)
KAPPA = RELAX / (1.0 + RELAX)
PAD = 8
F32 = jnp.float32
(U_, V_, H1, H2, H12, K_, M8, FU, FV, CA, CB) = range(11)
NS = 9
NF = 11
ALL = ("gx", "gy")


def weight_of(mask, openw):
    return mask.astype(F32) * (1.0 - openw.astype(F32))


def consts(strength, mass, wind, cur, weight):
    return (KAPPA * strength) * weight, mass * 8.0, 4.0 * (wind[0] + cur[0]), 4.0 * (wind[1] + cur[1])


def coefs(m8, weight):
    a = m8 * 0.25 + 1.0
    b = m8 * 0.0375
    scale = (0.25 * weight) / (a * a + b * b)
    return a * scale, b * scale


def strain(u, v, um, vm):
    su = u + um
    du = u - um
    sv = v + vm
    dv = v - vm
    return su + dv, su - dv, du + sv, du - sv


def stress_rate(alpha, beta, gamma, alpha_m, beta_m, delta_m, k):
    d = alpha - beta_m
    t = beta - alpha_m
    s = gamma + delta_m
    q = d * d + 0.25 * (t * t + s * s) + 0.01
    r = lax.rsqrt(q)
    z = k * r
    z4 = 0.25 * z
    return z * (d - q * r), z4 * t, z4 * s


def mixes(h1, h2, h12):
    return h1 + h2, h1 - h2, h12


def spread(m, p):
    xs, xd = p[0] + m[0], p[2] - m[2]
    ys, yd = p[2] + m[2], p[1] - m[1]
    return xs + xd, xs - xd, ys + yd, ys - yd


def drift(u, v, fx, fy, m8, fu, fv, ca, cb):
    ru = m8 * u + (fx + fu)
    rv = m8 * v + (fy + fv)
    return ca * ru + cb * rv, ca * rv - cb * ru


def pair_rows(parts, high):
    half = lax.broadcasted_iota(jnp.int32, parts[0].shape, 0) < 4
    tiles = []
    for f in range(0, NS, 2):
        a = parts[f]
        b = parts[f + 1] if f + 1 < NS else jnp.zeros_like(a)
        if high:
            tiles.append(jnp.where(half, pltpu.roll(a, 4, 0), b))
        else:
            tiles.append(jnp.where(half, a, pltpu.roll(b, 4, 0)))
    return jnp.concatenate(tiles, 0)


def unpair(tiles, f, high):
    x = tiles[8 * (f // 2) : 8 * (f // 2) + 8]
    return x if (f % 2 == 1) == high else pltpu.roll(x, 4, 0)


def is_even(axis):
    return lax.axis_index(axis) % 2 == 0


def strip_fields(vel, strs, strength, mass, wind, cur, mask, openw):
    w = weight_of(mask[...], openw[...])
    k, m8, fu, fv = consts(strength[...], mass[...], (wind[0], wind[1]), (cur[0], cur[1]), w)
    return [vel[0], vel[1], strs[0], strs[1], 2.0 * strs[2], k, m8, fu, fv]


def rows_kernel(*refs):
    own, msg_a, msg_b = refs[16:]
    top = strip_fields(*refs[:8])
    bot = strip_fields(*refs[8:16])
    for f in range(NS):
        own[f, 0:8, :] = top[f]
        own[f, 8:16, :] = bot[f]
    low = pair_rows(top, False)
    high = pair_rows(bot, True)
    even = is_even("gx")
    msg_a[...] = jnp.where(even, high, low)
    msg_b[...] = jnp.where(even, low, high)


def load_kernel(vel, strs, strength, mass, wind, cur, mask, openw, x, cols):
    R, C = strength.shape

    def prepare(r0):
        rows = pl.ds(r0, 8)
        for t in range(C // 128):
            at = (rows, slice(128 * t, 128 * t + 128))
            w = weight_of(mask[at], openw[at])
            k, m8, fu, fv = consts(strength[at], mass[at], (wind[(0, *at)], wind[(1, *at)]), (cur[(0, *at)], cur[(1, *at)]), w)
            ca, cb = coefs(m8, w)
            for f, value in enumerate((k, m8, fu, fv, ca, cb)):
                x[(f, *at)] = value

    def body(i, carry):
        for n in range(4):
            prepare(pl.multiple_of(i * 32 + 8 * n, 8))
        return carry

    lax.fori_loop(0, R // 32, body, 0)
    lane = lax.broadcasted_iota(jnp.int32, (8, 128), 1)
    low = lane < 64
    fields = [(vel, 0), (vel, 1), (strs, 0), (strs, 1), (strs, 2)] + [(x, f - K_) for f in range(K_, NS)]

    def pack(p, carry):
        groups = ([], [])
        for g in range(16):
            rows = pl.ds(pl.multiple_of(p * 128 + 8 * g, 8), 8)
            packed = [None, None]
            for f, (ref, lead) in enumerate(fields):
                y = jnp.where(low, ref[lead, rows, 0:128], ref[lead, rows, C - 128 : C])
                if f == H12:
                    y = 2.0 * y
                if f:
                    y = pltpu.roll(y, 8 * f, 1)
                for side in range(2):
                    begin = 8 * (f - side) % 128
                    hit = (lane >= begin) & (lane < begin + 8)
                    packed[side] = y if packed[side] is None else jnp.where(hit, y, packed[side])
            for side in range(2):
                groups[side].append(packed[side])
        at = pl.ds(pl.multiple_of(p * 128, 128), 128)
        y = jnp.concatenate(groups[0], 0).T
        cols[0 : 8 * NS, at] = y[0 : 8 * NS]
        y = jnp.concatenate(groups[1], 0).T
        cols[8 * NS : 8 * NS + 8, at] = y[120:128]
        cols[8 * NS + 8 : 16 * NS, at] = y[0 : 8 * (NS - 1)]
        return carry

    lax.fori_loop(0, R // 128, pack, 0)


def corners_kernel(cols, xa, xb, ya, yb, ext):
    even = is_even("gx")
    a, b = xa[...], xb[...]
    top = jnp.where(even, b, a)
    bot = jnp.where(even, a, b)
    C = cols.shape[1]
    lane = lax.broadcasted_iota(jnp.int32, (8, 128), 1)
    strips = []
    for side in range(2):
        at = side * (C - 128)
        t = jnp.concatenate([top[:, at : at + 128], bot[:, at : at + 128], jnp.zeros((48, 128), F32)], 0).T
        t = t[120 * side : 120 * side + 8]
        own = []
        for f in range(NS):
            e = jnp.where(lane >= 124, pltpu.roll(t, 124 - 4 * f, 1), 0.0)
            e = jnp.where(lane < 4, pltpu.roll(t, 128 - 40 - 4 * f, 1), e)
            base = 8 * (NS * side + f)
            ext[base : base + 8, :] = e
            own.append(jnp.concatenate([cols[base : base + 8, :], e], 1))
        strips.append(pair_rows(own, side == 1))
    low, high = strips
    even = is_even("gy")
    ya[...] = jnp.where(even, high, low)
    yb[...] = jnp.where(even, low, high)


def sweep_subcycles(its, vel, strs, con, x, nvel, nstr, sums, al, be, ga, de, tx, ty, nx, ny, sem, *, RB, L1, L2):
    R, C = x.shape[1:]
    NT = C // 128
    k, m8_, fu_, fv_, ca_, cb_ = range(6)
    zero = jnp.zeros((8, 128), F32)
    for t in range(NT):
        for ref in (al, be, de):
            ref[t, 0:PAD, :] = zero
        for ref in (tx, ty):
            ref[t, PAD + R : PAD + R + 8, :] = zero
    lane = lax.broadcasted_iota(jnp.int32, (8, 128), 1)
    row_in = lax.broadcasted_iota(jnp.int32, (8, 128), 0)
    first = lane == 0
    last = lane == 127

    def tile(t):
        return slice(128 * t, 128 * t + 128)

    def strain_rows(r0, src):
        own = pl.ds(r0, 8)
        rows = pl.ds(PAD + r0, 8)
        ru = rv = None
        for t in range(NT):
            u, v = src[0, own, tile(t)], src[1, own, tile(t)]
            qu, qv = pltpu.roll(u, 1, 1), pltpu.roll(v, 1, 1)
            um = jnp.where(first, ru, qu) if t else qu
            vm = jnp.where(first, rv, qv) if t else qv
            ru, rv = qu, qv
            al[t, rows, :], be[t, rows, :], ga[t, rows, :], de[t, rows, :] = strain(u, v, um, vm)

    def rate_rows(r0, it):
        own = pl.ds(r0, 8)
        rows = pl.ds(PAD + r0, 8)
        above = pl.ds(PAD + r0 - 1, 8)

        def emit(t, m, q, nq):
            p = [jnp.where(last, nq[i], q[i]) if nq else q[i] for i in range(3)]
            tx[t, rows, :], nx[t, rows, :], ty[t, rows, :], ny[t, rows, :] = spread(m, p)

        held = None
        for t in range(NT):
            d1, d2, d12 = stress_rate(al[t, rows, :], be[t, rows, :], ga[t, rows, :], al[t, above, :], be[t, above, :], de[t, above, :], con[k, own, tile(t)])
            if it:
                old = [x[f, own, tile(t)] for f in (H1, H2, H12)]
            else:
                old = [strs[f, own, tile(t)] for f in range(3)]
            h1 = old[0] * GROW + d1
            h2 = old[1] * GROW + d2
            h12 = old[2] * (GROW if it else 2.0 * GROW) + d12
            x[H1, own, tile(t)] = h1
            x[H2, own, tile(t)] = h2
            x[H12, own, tile(t)] = 0.5 * h12 if it == ITERS - 1 else h12
            m = mixes(h1, h2, h12)
            q = [pltpu.roll(v, 127, 1) for v in m]
            if held:
                emit(t - 1, *held, q)
            held = (m, q)
        emit(NT - 1, *held, None)

    def velocity_rows(r0, src, acc):
        own = pl.ds(r0, 8)
        rows = pl.ds(PAD + r0, 8)
        below = pl.ds(PAD + r0 + 1, 8)
        for t in range(NT):
            u, v, m8 = src[0, own, tile(t)], src[1, own, tile(t)], con[m8_, own, tile(t)]
            fx = tx[t, below, :] - nx[t, rows, :]
            fy = ty[t, below, :] - ny[t, rows, :]
            nu, nv = drift(u, v, fx, fy, m8, con[fu_, own, tile(t)], con[fv_, own, tile(t)], con[ca_, own, tile(t)], con[cb_, own, tile(t)])
            x[U_, own, tile(t)] = nu
            x[V_, own, tile(t)] = nv
            if acc is not None:
                keep = (con[k, own, tile(t)] > 0.0) & (row_in + r0 >= ITERS) & (row_in + r0 < R - ITERS)
                if t == 0:
                    keep = keep & (lane >= ITERS)
                if t == NT - 1:
                    keep = keep & (lane < 128 - ITERS)
                cu, cv = nu - u, nv - v
                acc[2 * (t % 2)] += jnp.where(keep, cu * cu + cv * cv, 0.0)
                acc[2 * (t % 2) + 1] += jnp.where(keep, m8 * (nu * nu + nv * nv), 0.0)

    sent = [0]

    def send(end):
        rows = pl.ds(sent[0], end - sent[0])
        for f, (ref, lead) in enumerate(((nvel, 0), (nvel, 1), (nstr, 0), (nstr, 1), (nstr, 2))):
            pltpu.make_async_copy(x.at[f, rows], ref.at[lead, rows], sem).start()
        sent[0] = end

    acc = [zero] * 4
    peel = -(-L2 // RB) * RB
    for it in its:
        start = it == its[0]
        final = it == ITERS - 1
        src, before = (x if n > 0 else vel for n in (it, it - 1))
        for r in range(0, peel, 8):
            strain_rows(r, src)
            if r >= L1:
                rate_rows(r - L1, it)
            elif not start:
                rate_rows(R + r - L1, it - 1)
            if r >= L2:
                velocity_rows(r - L2, src, acc if final else None)
            elif not start:
                velocity_rows(R + r - L2, before, None)

        def body(j, acc):
            r0 = pl.multiple_of(j * RB, RB)
            acc = list(acc) if final else None
            for r in range(0, RB, 8):
                strain_rows(r0 + r, src)
                rate_rows(r0 + (r - L1), it)
                velocity_rows(r0 + (r - L2), src, acc)
            return tuple(acc) if final else ()

        if not final:
            lax.fori_loop(peel // RB, R // RB, body, ())
            continue
        for j in range(peel // RB, R // RB, 2):
            acc = list(lax.fori_loop(j, min(j + 2, R // RB), body, tuple(acc)))
            send(min((j + 2) * RB, R) - L2)
    for r in range(0, L2, 8):
        if r < L1:
            rate_rows(R + r - L1, its[-1])
        velocity_rows(R + r - L2, src, acc if final else None)
        if final and r + 8 == L2 // 2:
            send(R - L2 // 2)
    if not final:
        return
    send(R)
    sums[0] = acc[0] + acc[2]
    sums[1] = acc[1] + acc[3]
    pltpu.make_async_copy(x, x, sem).wait()


def first_kernel(vel, strs, con, x, *work, **kw):
    sweep_subcycles([0], vel, strs, con, x, None, None, None, *work, None, **kw)


def rest_kernel(x_in, con, x, nvel, nstr, sums, *work, **kw):
    sweep_subcycles(list(range(1, ITERS)), None, None, con, x, nvel, nstr, sums, *work, **kw)


def strip_begin(ref):
    w = jnp.where(ref[K_] > 0.0, 1.0, 0.0)
    ref[CA], ref[CB] = coefs(ref[M8], w)


def strip_subcycle(ref, rows_axis, keep=None):
    cols_axis = 1 - rows_axis
    back = lambda x, axis: pltpu.roll(x, 1, axis)
    ahead = lambda x, axis: pltpu.roll(x, x.shape[axis] - 1, axis)
    u, v = ref[U_], ref[V_]
    a, b, g, d = strain(u, v, back(u, cols_axis), back(v, cols_axis))
    d1, d2, d12 = stress_rate(a, b, g, back(a, rows_axis), back(b, rows_axis), back(d, rows_axis), ref[K_])
    h1 = ref[H1] * GROW + d1
    h2 = ref[H2] * GROW + d2
    h12 = ref[H12] * GROW + d12
    ref[H1], ref[H2], ref[H12] = h1, h2, h12
    m = mixes(h1, h2, h12)
    xt, xn, yt, yn = spread(m, [ahead(v, cols_axis) for v in m])
    fx = ahead(xt, rows_axis) - xn
    fy = ahead(yt, rows_axis) - yn
    m8 = ref[M8]
    nu, nv = drift(u, v, fx, fy, m8, ref[FU], ref[FV], ref[CA], ref[CB])
    ref[U_], ref[V_] = nu, nv
    if keep is None:
        return None
    cu, cv = nu - u, nv - v
    inside = keep & (ref[K_] > 0.0)
    pair = (jnp.where(inside, cu * cu + cv * cv, 0.0), jnp.where(inside, m8 * (nu * nu + nv * nv), 0.0))
    return [sum(p[i : i + 8, j : j + 128] for i in range(0, p.shape[0], 8) for j in range(0, p.shape[1], 128)) for p in pair]


def strips_kernel(own, cols, ext, xa, xb, ya, yb, isums, rows_out, cols_out, msg, rs, cs, *, R, C):
    even = is_even("gx")
    a, b = xa[...], xb[...]
    top = jnp.where(even, b, a)
    bot = jnp.where(even, a, b)
    even = is_even("gy")
    a, b = ya[...], yb[...]
    left = jnp.where(even, b, a)
    right = jnp.where(even, a, b)
    for f in range(NS):
        rs[f, 0:8, :] = unpair(top, f, True)
        rs[f, 8:16, :] = own[f, 0:8, :]
        rs[f, 16:24, :] = own[f, 8:16, :]
        rs[f, 24:32, :] = unpair(bot, f, False)
        cs[f, 0:8, :] = unpair(left, f, True)
        for side in range(2):
            base = 8 * (NS * side + f)
            cs[f, 8 + 8 * side : 16 + 8 * side, 0:R] = cols[base : base + 8, :]
            cs[f, 8 + 8 * side : 16 + 8 * side, R : R + 128] = ext[base : base + 8, :]
        cs[f, 24:32, :] = unpair(right, f, False)

    def rim(shape):
        sub = lax.broadcasted_iota(jnp.int32, shape, 0)
        return ((sub >= 8) & (sub < 12)) | ((sub >= 20) & (sub < 24)), lax.broadcasted_iota(jnp.int32, shape, 1)

    strip_begin(rs)
    strip_begin(cs)

    def body(_, carry):
        strip_subcycle(rs, 0)
        strip_subcycle(cs, 1)
        return carry

    lax.fori_loop(0, ITERS - 1, body, 0)
    band, lane = rim(rs.shape[1:])
    row_sums = strip_subcycle(rs, 0, band & (lane >= ITERS) & (lane < C - ITERS))
    band, lane = rim(cs.shape[1:])
    col_sums = strip_subcycle(cs, 1, band & (lane < R))
    lane = lax.broadcasted_iota(jnp.int32, msg.shape, 1)
    totals = [jnp.sum(isums[n] + row_sums[n] + col_sums[n]) for n in range(2)]
    msg[...] = jnp.where(lane == 0, totals[0], jnp.where(lane == 1, totals[1], 0.0))
    for f in range(5):
        half = 0.5 if f == H12 else 1.0
        rows_out[f] = half * rs[f, 8:24, :]
        cols_out[f] = half * cs[f, 8:24, 0:R]


def merge_kernel(rows_in, cols_in, nvel_in, nstr_in, nvel, nstr, edge, mid, sem):
    R, C = nvel.shape[1:]
    outs = ((nvel, 0), (nvel, 1), (nstr, 0), (nstr, 1), (nstr, 2))
    inner = pl.ds(128, C - 256)

    def places(f):
        ref, lead = outs[f]
        full = ref.at[lead]
        return (
            (full.at[:, pl.ds(0, 128)], edge.at[0, f]),
            (full.at[:, pl.ds(C - 128, 128)], edge.at[1, f]),
            (full.at[pl.ds(0, 8), inner], mid.at[0, f]),
            (full.at[pl.ds(R - 8, 8), inner], mid.at[1, f]),
        )

    for f in range(5):
        for n, (there, here) in enumerate(places(f)):
            pltpu.make_async_copy(there, here, sem.at[0, n // 2]).start()
    for n, buf in enumerate((edge, mid)):
        pltpu.make_async_copy(buf, buf, sem.at[0, n]).wait()
    low = lax.broadcasted_iota(jnp.int32, (8, C), 0) < 4
    for f in range(5):
        for part in range(2):
            x = rows_in[f, 8 * part : 8 * part + 8, :]
            keep = ~low if part == 0 else low
            rows = slice(part * (R - 8), part * (R - 8) + 8)
            mid[part, f] = jnp.where(keep[:, 128 : C - 128], mid[part, f], x[:, 128 : C - 128])
            for side in range(2):
                at = slice(side * (C - 128), side * (C - 128) + 128)
                edge[side, f, rows, :] = jnp.where(keep[:, at], edge[side, f, rows, :], x[:, at])
    lane = lax.broadcasted_iota(jnp.int32, (128, 128), 1)
    for c in range(R // 128):
        rows = slice(c * 128, c * 128 + 128)
        parts = [cols_in[f, 8 * side : 8 * side + 8, rows] for side in range(2) for f in range(5)]
        x = jnp.concatenate(parts + [jnp.zeros((48, 128), F32)], 0).T
        for side in range(2):
            for f in range(5):
                shift = (120 * side - 8 * (5 * side + f)) % 128
                y = pltpu.roll(x, shift, 1) if shift else x
                hit = lane >= 124 if side else lane < 4
                edge[side, f, rows, :] = jnp.where(hit, y, edge[side, f, rows, :])
    for f in range(5):
        for n, (there, here) in enumerate(places(f)):
            pltpu.make_async_copy(here, there, sem.at[1, n // 2]).start()
    for n, buf in enumerate((edge, mid)):
        pltpu.make_async_copy(buf, buf, sem.at[1, n]).wait()


def total_kernel(parts, residual, kinetic, *, cells):
    lane = lax.broadcasted_iota(jnp.int32, parts.shape, 1)
    x = parts[...]
    residual[0] = jnp.sum(jnp.where(lane == 0, x, 0.0)) * (1.0 / cells)
    kinetic[0] = jnp.sum(jnp.where(lane == 1, x, 0.0)) * (0.0625 / cells)


def swaps(count):
    first = [(i, i ^ 1) for i in range(count)]
    second = [(i, i + 1) for i in range(1, count - 1, 2)] + [(i + 1, i) for i in range(1, count - 1, 2)]
    return first, second


def exchange(a, b, axis):
    first, second = swaps(lax.axis_size(axis))
    return lax.ppermute(a, axis, first), lax.ppermute(b, axis, second)


def sds(*shape):
    return jax.ShapeDtypeStruct(shape, F32)


def interior_first(vel, strs, con, RB=64, L1=64, L2=128):
    _, R, C = con.shape
    vmem = pl.BlockSpec(memory_space=pltpu.VMEM)
    return pl.pallas_call(
        functools.partial(first_kernel, RB=RB, L1=L1, L2=L2),
        in_specs=[vmem] * 3,
        out_specs=vmem,
        out_shape=sds(5, R, C),
        scratch_shapes=[pltpu.VMEM((C // 128, R + 2 * PAD, 128), F32)] * 8,
        compiler_params=pltpu.CompilerParams(vmem_limit_bytes=12 * 2**20),
        name="first",
    )(vel, strs, con)


def interior_rest(x, con, RB=64, L1=64, L2=128):
    _, R, C = con.shape
    hbm = pl.BlockSpec(memory_space=pltpu.HBM)
    vmem = pl.BlockSpec(memory_space=pltpu.VMEM)
    return pl.pallas_call(
        functools.partial(rest_kernel, RB=RB, L1=L1, L2=L2),
        in_specs=[vmem] * 2,
        out_specs=(vmem, hbm, hbm, vmem),
        out_shape=(sds(5, R, C), sds(2, R, C), sds(3, R, C), sds(2, 8, 128)),
        scratch_shapes=[pltpu.VMEM((C // 128, R + 2 * PAD, 128), F32)] * 8 + [pltpu.SemaphoreType.DMA(())],
        input_output_aliases={0: 0},
        compiler_params=pltpu.CompilerParams(vmem_limit_bytes=12 * 2**20),
        name="rest",
    )(x, con)


def per_device(velocity, stress, strength, ice_mass, wind_stress, current, ice_mask, open_water):
    args = (velocity, stress, strength, ice_mass, wind_stress, current, ice_mask, open_water)
    R, C = strength.shape
    hbm = pl.BlockSpec(memory_space=pltpu.HBM)
    vmem = pl.BlockSpec(memory_space=pltpu.VMEM)

    def limit(mib):
        return pltpu.CompilerParams(vmem_limit_bytes=mib * 2**20)

    def blocks(shape, where):
        return [pl.BlockSpec((v.shape[0],) * (v.ndim - 2) + shape, functools.partial(lambda nd, *g: (0,) * (nd - 2) + where(*g), v.ndim)) for v in args]

    edges = [pltpu.with_memory_space_constraint(v, pltpu.HBM) for v in args]
    own, xa, xb = pl.pallas_call(
        rows_kernel,
        grid=(1,),
        in_specs=blocks((8, C), lambda i: (0, 0)) + blocks((8, C), lambda i: (R // 8 - 1, 0)),
        out_specs=[pl.BlockSpec((NS, 16, C), lambda i: (0, 0, 0)), pl.BlockSpec((40, C), lambda i: (0, 0)), pl.BlockSpec((40, C), lambda i: (0, 0))],
        out_shape=[sds(NS, 16, C), sds(40, C), sds(40, C)],
        compiler_params=limit(6),
        name="row_edges",
    )(*edges, *edges)
    xa, xb, *args = lax.optimization_barrier((xa, xb, *args))
    xa, xb = exchange(xa, xb, "gx")
    con, cols = pl.pallas_call(
        load_kernel,
        in_specs=[vmem] * 8,
        out_specs=(vmem, vmem),
        out_shape=(sds(6, R, C), sds(16 * NS, R)),
        compiler_params=limit(16),
        name="load",
    )(*args)
    x = interior_first(args[0], args[1], con)
    cols, x = lax.optimization_barrier((cols, x))
    ya, yb, ext = pl.pallas_call(
        corners_kernel,
        in_specs=[vmem] * 3,
        out_specs=[vmem] * 3,
        out_shape=[sds(40, R + 128), sds(40, R + 128), sds(16 * NS, 128)],
        compiler_params=limit(6),
        name="corners",
    )(cols, xa, xb)
    ya, yb = exchange(ya, yb, "gy")
    _, nvel, nstr, isums = interior_rest(x, con)
    ND = lax.axis_size(ALL)
    rows_out, cols_out, msg = pl.pallas_call(
        functools.partial(strips_kernel, R=R, C=C),
        in_specs=[vmem] * 8,
        out_specs=(vmem, vmem, vmem),
        out_shape=(sds(5, 16, C), sds(5, 16, R), sds(ND, 128)),
        scratch_shapes=[
            pltpu.VMEM((NF, 32, C), F32),
            pltpu.VMEM((NF, 32, R + 128), F32),
        ],
        compiler_params=limit(12),
        name="strips",
    )(own, cols, ext, xa, xb, ya, yb, isums)
    msg = pltpu.with_memory_space_constraint(msg, pltpu.VMEM)
    parts = lax.all_to_all(msg, ALL, 0, 0, tiled=True)
    nvel, nstr = pl.pallas_call(
        merge_kernel,
        in_specs=[vmem] * 2 + [hbm] * 2,
        out_specs=(hbm, hbm),
        out_shape=(sds(2, R, C), sds(3, R, C)),
        scratch_shapes=[pltpu.VMEM((2, 5, R, 128), F32), pltpu.VMEM((2, 5, 8, C - 256), F32), pltpu.SemaphoreType.DMA((2, 2))],
        input_output_aliases={2: 0, 3: 1},
        compiler_params=limit(12),
        name="merge",
    )(rows_out, cols_out, nvel, nstr)
    cells = R * lax.axis_size("gx") * C * lax.axis_size("gy")
    smem = pl.BlockSpec(memory_space=pltpu.SMEM)
    residual, kinetic = pl.pallas_call(
        functools.partial(total_kernel, cells=cells),
        in_specs=[vmem],
        out_specs=(smem, smem),
        out_shape=(sds(1), sds(1)),
        compiler_params=limit(2),
        name="total",
    )(parts)
    return nvel, nstr, residual.reshape(()), kinetic.reshape(())


def solution(mesh):
    whole, plane = P(None, "gx", "gy"), P("gx", "gy")
    return jax.shard_map(
        per_device,
        mesh=mesh,
        in_specs=(whole, whole, plane, plane, whole, whole, plane, plane),
        out_specs=(whole, whole, P(), P()),
        check_vma=False,
    )
```

```python
import functools

import jax
import jax.numpy as jnp
from jax import lax
from jax.experimental import pallas as pl
from jax.experimental.pallas import tpu as pltpu
from jax.sharding import PartitionSpec as P

ITERS = 4
RELAX = 0.8
GROW = 1.0 / (1.0 + RELAX)
KAPPA = RELAX / (1.0 + RELAX)
PAD = 8
F32 = jnp.float32
(U_, V_, H1, H2, H12, K_, M8, FU, FV, CA, CB) = range(11)
NS = 9
NF = 11
ALL = ("gx", "gy")


def weight_of(mask, openw):
    return mask.astype(F32) * (1.0 - openw.astype(F32))


def consts(strength, mass, wind, cur, weight):
    return (KAPPA * strength) * weight, mass * 8.0, 4.0 * (wind[0] + cur[0]), 4.0 * (wind[1] + cur[1])


def coefs(m8, weight):
    a = m8 * 0.25 + 1.0
    b = m8 * 0.0375
    scale = (0.25 * weight) / (a * a + b * b)
    return a * scale, b * scale


def strain(u, v, um, vm):
    su = u + um
    du = u - um
    sv = v + vm
    dv = v - vm
    return su + dv, su - dv, du + sv, du - sv


def stress_rate(alpha, beta, gamma, alpha_m, beta_m, delta_m, k):
    d = alpha - beta_m
    t = beta - alpha_m
    s = gamma + delta_m
    q = d * d + 0.25 * (t * t + s * s) + 0.01
    r = lax.rsqrt(q)
    z = k * r
    z4 = 0.25 * z
    return z * (d - q * r), z4 * t, z4 * s


def mixes(h1, h2, h12):
    return h1 + h2, h1 - h2, h12


def spread(m, p):
    xs, xd = p[0] + m[0], p[2] - m[2]
    ys, yd = p[2] + m[2], p[1] - m[1]
    return xs + xd, xs - xd, ys + yd, ys - yd


def drift(u, v, fx, fy, m8, fu, fv, ca, cb):
    ru = m8 * u + (fx + fu)
    rv = m8 * v + (fy + fv)
    return ca * ru + cb * rv, ca * rv - cb * ru


def pair_rows(parts, high):
    half = lax.broadcasted_iota(jnp.int32, parts[0].shape, 0) < 4
    tiles = []
    for f in range(0, NS, 2):
        a = parts[f]
        b = parts[f + 1] if f + 1 < NS else jnp.zeros_like(a)
        if high:
            tiles.append(jnp.where(half, pltpu.roll(a, 4, 0), b))
        else:
            tiles.append(jnp.where(half, a, pltpu.roll(b, 4, 0)))
    return jnp.concatenate(tiles, 0)


def unpair(tiles, f, high):
    x = tiles[8 * (f // 2) : 8 * (f // 2) + 8]
    return x if (f % 2 == 1) == high else pltpu.roll(x, 4, 0)


def is_even(axis):
    return lax.axis_index(axis) % 2 == 0


def strip_fields(vel, strs, strength, mass, wind, cur, mask, openw):
    w = weight_of(mask[...], openw[...])
    k, m8, fu, fv = consts(strength[...], mass[...], (wind[0], wind[1]), (cur[0], cur[1]), w)
    return [vel[0], vel[1], strs[0], strs[1], 2.0 * strs[2], k, m8, fu, fv]


def rows_kernel(*refs):
    own, msg_a, msg_b = refs[16:]
    top = strip_fields(*refs[:8])
    bot = strip_fields(*refs[8:16])
    for f in range(NS):
        own[f, 0:8, :] = top[f]
        own[f, 8:16, :] = bot[f]
    low = pair_rows(top, False)
    high = pair_rows(bot, True)
    even = is_even("gx")
    msg_a[...] = jnp.where(even, high, low)
    msg_b[...] = jnp.where(even, low, high)


def load_kernel(vel, strs, strength, mass, wind, cur, mask, openw, x, cols):
    R, C = strength.shape

    def prepare(r0):
        rows = pl.ds(r0, 8)
        for t in range(C // 128):
            at = (rows, slice(128 * t, 128 * t + 128))
            w = weight_of(mask[at], openw[at])
            k, m8, fu, fv = consts(strength[at], mass[at], (wind[(0, *at)], wind[(1, *at)]), (cur[(0, *at)], cur[(1, *at)]), w)
            ca, cb = coefs(m8, w)
            for f, value in enumerate((k, m8, fu, fv, ca, cb)):
                x[(f, *at)] = value

    def body(i, carry):
        for n in range(4):
            prepare(pl.multiple_of(i * 32 + 8 * n, 8))
        return carry

    lax.fori_loop(0, R // 32, body, 0)
    lane = lax.broadcasted_iota(jnp.int32, (8, 128), 1)
    low = lane < 64
    fields = [(vel, 0), (vel, 1), (strs, 0), (strs, 1), (strs, 2)] + [(x, f - K_) for f in range(K_, NS)]

    def pack(p, carry):
        groups = ([], [])
        for g in range(16):
            rows = pl.ds(pl.multiple_of(p * 128 + 8 * g, 8), 8)
            packed = [None, None]
            for f, (ref, lead) in enumerate(fields):
                y = jnp.where(low, ref[lead, rows, 0:128], ref[lead, rows, C - 128 : C])
                if f == H12:
                    y = 2.0 * y
                if f:
                    y = pltpu.roll(y, 8 * f, 1)
                for side in range(2):
                    begin = 8 * (f - side) % 128
                    hit = (lane >= begin) & (lane < begin + 8)
                    packed[side] = y if packed[side] is None else jnp.where(hit, y, packed[side])
            for side in range(2):
                groups[side].append(packed[side])
        at = pl.ds(pl.multiple_of(p * 128, 128), 128)
        y = jnp.concatenate(groups[0], 0).T
        cols[0 : 8 * NS, at] = y[0 : 8 * NS]
        y = jnp.concatenate(groups[1], 0).T
        cols[8 * NS : 8 * NS + 8, at] = y[120:128]
        cols[8 * NS + 8 : 16 * NS, at] = y[0 : 8 * (NS - 1)]
        return carry

    lax.fori_loop(0, R // 128, pack, 0)


def corners_kernel(cols, xa, xb, ya, yb, ext):
    even = is_even("gx")
    a, b = xa[...], xb[...]
    top = jnp.where(even, b, a)
    bot = jnp.where(even, a, b)
    C = cols.shape[1]
    lane = lax.broadcasted_iota(jnp.int32, (8, 128), 1)
    strips = []
    for side in range(2):
        at = side * (C - 128)
        t = jnp.concatenate([top[:, at : at + 128], bot[:, at : at + 128], jnp.zeros((48, 128), F32)], 0).T
        t = t[120 * side : 120 * side + 8]
        own = []
        for f in range(NS):
            e = jnp.where(lane >= 124, pltpu.roll(t, 124 - 4 * f, 1), 0.0)
            e = jnp.where(lane < 4, pltpu.roll(t, 128 - 40 - 4 * f, 1), e)
            base = 8 * (NS * side + f)
            ext[base : base + 8, :] = e
            own.append(jnp.concatenate([cols[base : base + 8, :], e], 1))
        strips.append(pair_rows(own, side == 1))
    low, high = strips
    even = is_even("gy")
    ya[...] = jnp.where(even, high, low)
    yb[...] = jnp.where(even, low, high)


def sweep_subcycles(its, vel, strs, con, x, nvel, nstr, sums, al, be, ga, de, tx, ty, nx, ny, sem, *, RB, L1, L2):
    R, C = x.shape[1:]
    NT = C // 128
    k, m8_, fu_, fv_, ca_, cb_ = range(6)
    zero = jnp.zeros((8, 128), F32)
    for t in range(NT):
        for ref in (al, be, de):
            ref[t, 0:PAD, :] = zero
        for ref in (tx, ty):
            ref[t, PAD + R : PAD + R + 8, :] = zero
    lane = lax.broadcasted_iota(jnp.int32, (8, 128), 1)
    row_in = lax.broadcasted_iota(jnp.int32, (8, 128), 0)
    first = lane == 0
    last = lane == 127

    def tile(t):
        return slice(128 * t, 128 * t + 128)

    def strain_rows(r0, src):
        own = pl.ds(r0, 8)
        rows = pl.ds(PAD + r0, 8)
        ru = rv = None
        for t in range(NT):
            u, v = src[0, own, tile(t)], src[1, own, tile(t)]
            qu, qv = pltpu.roll(u, 1, 1), pltpu.roll(v, 1, 1)
            um = jnp.where(first, ru, qu) if t else qu
            vm = jnp.where(first, rv, qv) if t else qv
            ru, rv = qu, qv
            al[t, rows, :], be[t, rows, :], ga[t, rows, :], de[t, rows, :] = strain(u, v, um, vm)

    def rate_rows(r0, it):
        own = pl.ds(r0, 8)
        rows = pl.ds(PAD + r0, 8)
        above = pl.ds(PAD + r0 - 1, 8)

        def emit(t, m, q, nq):
            p = [jnp.where(last, nq[i], q[i]) if nq else q[i] for i in range(3)]
            tx[t, rows, :], nx[t, rows, :], ty[t, rows, :], ny[t, rows, :] = spread(m, p)

        held = None
        for t in range(NT):
            d1, d2, d12 = stress_rate(al[t, rows, :], be[t, rows, :], ga[t, rows, :], al[t, above, :], be[t, above, :], de[t, above, :], con[k, own, tile(t)])
            if it:
                old = [x[f, own, tile(t)] for f in (H1, H2, H12)]
            else:
                old = [strs[f, own, tile(t)] for f in range(3)]
            h1 = old[0] * GROW + d1
            h2 = old[1] * GROW + d2
            h12 = old[2] * (GROW if it else 2.0 * GROW) + d12
            x[H1, own, tile(t)] = h1
            x[H2, own, tile(t)] = h2
            x[H12, own, tile(t)] = 0.5 * h12 if it == ITERS - 1 else h12
            m = mixes(h1, h2, h12)
            q = [pltpu.roll(v, 127, 1) for v in m]
            if held:
                emit(t - 1, *held, q)
            held = (m, q)
        emit(NT - 1, *held, None)

    def velocity_rows(r0, src, acc, may_start=False):
        own = pl.ds(r0, 8)
        rows = pl.ds(PAD + r0, 8)
        below = pl.ds(PAD + r0 + 1, 8)
        for t in range(NT):
            u, v, m8 = src[0, own, tile(t)], src[1, own, tile(t)], con[m8_, own, tile(t)]
            fx = tx[t, below, :] - nx[t, rows, :]
            fy = ty[t, below, :] - ny[t, rows, :]
            nu, nv = drift(u, v, fx, fy, m8, con[fu_, own, tile(t)], con[fv_, own, tile(t)], con[ca_, own, tile(t)], con[cb_, own, tile(t)])
            x[U_, own, tile(t)] = nu
            x[V_, own, tile(t)] = nv
            if acc is not None:
                keep = con[k, own, tile(t)] > 0.0
                if may_start if not isinstance(r0, int) else r0 == 0:
                    keep = keep & (row_in + r0 >= ITERS)
                if isinstance(r0, int) and r0 == R - 8:
                    keep = keep & (row_in < 8 - ITERS)
                if t == 0:
                    keep = keep & (lane >= ITERS)
                if t == NT - 1:
                    keep = keep & (lane < 128 - ITERS)
                cu, cv = nu - u, nv - v
                acc[2 * (t % 2)] += jnp.where(keep, cu * cu + cv * cv, 0.0)
                acc[2 * (t % 2) + 1] += jnp.where(keep, m8 * (nu * nu + nv * nv), 0.0)

    sent = [0]

    def send(end):
        rows = pl.ds(sent[0], end - sent[0])
        for f, (ref, lead) in enumerate(((nvel, 0), (nvel, 1), (nstr, 0), (nstr, 1), (nstr, 2))):
            pltpu.make_async_copy(x.at[f, rows], ref.at[lead, rows], sem).start()
        sent[0] = end

    acc = [zero] * 4
    peel = -(-L2 // RB) * RB
    for it in its:
        start = it == its[0]
        final = it == ITERS - 1
        src, before = (x if n > 0 else vel for n in (it, it - 1))
        for r in range(0, peel, 8):
            strain_rows(r, src)
            if r >= L1:
                rate_rows(r - L1, it)
            elif not start:
                rate_rows(R + r - L1, it - 1)
            if r >= L2:
                velocity_rows(r - L2, src, acc if final else None)
            elif not start:
                velocity_rows(R + r - L2, before, None)

        def body(j, acc):
            r0 = pl.multiple_of(j * RB, RB)
            acc = list(acc) if final else None
            for r in range(0, RB, 8):
                strain_rows(r0 + r, src)
                rate_rows(r0 + (r - L1), it)
                velocity_rows(r0 + (r - L2), src, acc, r == L2 % RB)
            return tuple(acc) if final else ()

        if not final:
            lax.fori_loop(peel // RB, R // RB, body, ())
            continue
        for j in range(peel // RB, R // RB, 2):
            acc = list(lax.fori_loop(j, min(j + 2, R // RB), body, tuple(acc)))
            send(min((j + 2) * RB, R) - L2)
    for r in range(0, L2, 8):
        if r < L1:
            rate_rows(R + r - L1, its[-1])
        velocity_rows(R + r - L2, src, acc if final else None)
        if final and (r + 8) % 32 == 0 and r + 8 < L2:
            send(R - L2 + r + 8)
    if not final:
        return
    send(R)
    sums[0] = acc[0] + acc[2]
    sums[1] = acc[1] + acc[3]
    pltpu.make_async_copy(x, x, sem).wait()


def first_kernel(vel, strs, con, x, *work, **kw):
    sweep_subcycles([0], vel, strs, con, x, None, None, None, *work, None, **kw)


def rest_kernel(x_in, con, x, nvel, nstr, sums, *work, **kw):
    sweep_subcycles(list(range(1, ITERS)), None, None, con, x, nvel, nstr, sums, *work, **kw)


def strip_begin(ref):
    w = jnp.where(ref[K_] > 0.0, 1.0, 0.0)
    ref[CA], ref[CB] = coefs(ref[M8], w)


def strip_subcycle(ref, rows_axis, keep=None):
    cols_axis = 1 - rows_axis
    back = lambda x, axis: pltpu.roll(x, 1, axis)
    ahead = lambda x, axis: pltpu.roll(x, x.shape[axis] - 1, axis)
    u, v = ref[U_], ref[V_]
    a, b, g, d = strain(u, v, back(u, cols_axis), back(v, cols_axis))
    d1, d2, d12 = stress_rate(a, b, g, back(a, rows_axis), back(b, rows_axis), back(d, rows_axis), ref[K_])
    h1 = ref[H1] * GROW + d1
    h2 = ref[H2] * GROW + d2
    h12 = ref[H12] * GROW + d12
    ref[H1], ref[H2], ref[H12] = h1, h2, h12
    m = mixes(h1, h2, h12)
    xt, xn, yt, yn = spread(m, [ahead(v, cols_axis) for v in m])
    fx = ahead(xt, rows_axis) - xn
    fy = ahead(yt, rows_axis) - yn
    m8 = ref[M8]
    nu, nv = drift(u, v, fx, fy, m8, ref[FU], ref[FV], ref[CA], ref[CB])
    ref[U_], ref[V_] = nu, nv
    if keep is None:
        return None
    cu, cv = nu - u, nv - v
    inside = keep & (ref[K_] > 0.0)
    pair = (jnp.where(inside, cu * cu + cv * cv, 0.0), jnp.where(inside, m8 * (nu * nu + nv * nv), 0.0))
    return [sum(p[i : i + 8, j : j + 128] for i in range(0, p.shape[0], 8) for j in range(0, p.shape[1], 128)) for p in pair]


def strips_kernel(own, cols, ext, xa, xb, ya, yb, isums, rows_out, cols_out, msg, rs, cs, *, R, C):
    even = is_even("gx")
    a, b = xa[...], xb[...]
    top = jnp.where(even, b, a)
    bot = jnp.where(even, a, b)
    even = is_even("gy")
    a, b = ya[...], yb[...]
    left = jnp.where(even, b, a)
    right = jnp.where(even, a, b)
    half_r = lax.broadcasted_iota(jnp.int32, (8, C), 0) < 4
    half_c = lax.broadcasted_iota(jnp.int32, (8, R + 128), 0) < 4
    for f in range(NS):
        rs[f, 0:8, :] = jnp.where(half_r, unpair(bot, f, False), unpair(top, f, True))
        rs[f, 8:24, :] = own[f]
        cs[f, 0:8, :] = jnp.where(half_c, unpair(right, f, False), unpair(left, f, True))
        for side in range(2):
            base = 8 * (NS * side + f)
            cs[f, 8 + 8 * side : 16 + 8 * side, 0:R] = cols[base : base + 8, :]
            cs[f, 8 + 8 * side : 16 + 8 * side, R : R + 128] = ext[base : base + 8, :]

    def rim(shape):
        sub = lax.broadcasted_iota(jnp.int32, shape, 0)
        return ((sub >= 8) & (sub < 12)) | ((sub >= 20) & (sub < 24)), lax.broadcasted_iota(jnp.int32, shape, 1)

    strip_begin(rs)
    strip_begin(cs)

    def body(_, carry):
        strip_subcycle(rs, 0)
        strip_subcycle(cs, 1)
        return carry

    lax.fori_loop(0, ITERS - 1, body, 0)
    band, lane = rim(rs.shape[1:])
    row_sums = strip_subcycle(rs, 0, band & (lane >= ITERS) & (lane < C - ITERS))
    band, lane = rim(cs.shape[1:])
    col_sums = strip_subcycle(cs, 1, band & (lane < R))
    lane = lax.broadcasted_iota(jnp.int32, msg.shape, 1)
    totals = [jnp.sum(isums[n] + row_sums[n] + col_sums[n]) for n in range(2)]
    msg[...] = jnp.where(lane == 0, totals[0], jnp.where(lane == 1, totals[1], 0.0))
    for f in range(5):
        half = 0.5 if f == H12 else 1.0
        rows_out[f] = half * rs[f, 8:24, :]
        cols_out[f] = half * cs[f, 8:24, 0:R]


def merge_kernel(rows_in, cols_in, nvel_in, nstr_in, nvel, nstr, edge, mid, sem):
    R, C = nvel.shape[1:]
    outs = ((nvel, 0), (nvel, 1), (nstr, 0), (nstr, 1), (nstr, 2))
    inner = pl.ds(128, C - 256)

    def places(f):
        ref, lead = outs[f]
        full = ref.at[lead]
        return (
            (full.at[:, pl.ds(0, 128)], edge.at[0, f]),
            (full.at[:, pl.ds(C - 128, 128)], edge.at[1, f]),
            (full.at[pl.ds(0, 8), inner], mid.at[0, f]),
            (full.at[pl.ds(R - 8, 8), inner], mid.at[1, f]),
        )

    for f in range(5):
        for n, (there, here) in enumerate(places(f)):
            pltpu.make_async_copy(there, here, sem.at[0, n // 2]).start()
    for n, buf in enumerate((edge, mid)):
        pltpu.make_async_copy(buf, buf, sem.at[0, n]).wait()
    low = lax.broadcasted_iota(jnp.int32, (8, C), 0) < 4
    for f in range(5):
        for part in range(2):
            x = rows_in[f, 8 * part : 8 * part + 8, :]
            keep = ~low if part == 0 else low
            rows = slice(part * (R - 8), part * (R - 8) + 8)
            mid[part, f] = jnp.where(keep[:, 128 : C - 128], mid[part, f], x[:, 128 : C - 128])
            for side in range(2):
                at = slice(side * (C - 128), side * (C - 128) + 128)
                edge[side, f, rows, :] = jnp.where(keep[:, at], edge[side, f, rows, :], x[:, at])
    lane = lax.broadcasted_iota(jnp.int32, (128, 128), 1)
    for c in range(R // 128):
        rows = slice(c * 128, c * 128 + 128)
        parts = [cols_in[f, 8 * side : 8 * side + 8, rows] for side in range(2) for f in range(5)]
        x = jnp.concatenate(parts + [jnp.zeros((48, 128), F32)], 0).T
        for side in range(2):
            for f in range(5):
                shift = (120 * side - 8 * (5 * side + f)) % 128
                y = pltpu.roll(x, shift, 1) if shift else x
                hit = lane >= 124 if side else lane < 4
                edge[side, f, rows, :] = jnp.where(hit, y, edge[side, f, rows, :])
    for f in range(5):
        for n, (there, here) in enumerate(places(f)):
            pltpu.make_async_copy(here, there, sem.at[1, n // 2]).start()
    for n, buf in enumerate((edge, mid)):
        pltpu.make_async_copy(buf, buf, sem.at[1, n]).wait()


def total_kernel(parts, residual, kinetic, *, cells):
    lane = lax.broadcasted_iota(jnp.int32, parts.shape, 1)
    x = parts[...]
    residual[0] = jnp.sum(jnp.where(lane == 0, x, 0.0)) * (1.0 / cells)
    kinetic[0] = jnp.sum(jnp.where(lane == 1, x, 0.0)) * (0.0625 / cells)


def swaps(count):
    first = [(i, i ^ 1) for i in range(count)]
    second = [(i, i + 1) for i in range(1, count - 1, 2)] + [(i + 1, i) for i in range(1, count - 1, 2)]
    return first, second


def exchange(a, b, axis):
    first, second = swaps(lax.axis_size(axis))
    return lax.ppermute(a, axis, first), lax.ppermute(b, axis, second)


def sds(*shape):
    return jax.ShapeDtypeStruct(shape, F32)


def interior_first(vel, strs, con, RB=64, L1=64, L2=128):
    _, R, C = con.shape
    vmem = pl.BlockSpec(memory_space=pltpu.VMEM)
    return pl.pallas_call(
        functools.partial(first_kernel, RB=RB, L1=L1, L2=L2),
        in_specs=[vmem] * 3,
        out_specs=vmem,
        out_shape=sds(5, R, C),
        scratch_shapes=[pltpu.VMEM((C // 128, R + 2 * PAD, 128), F32)] * 8,
        compiler_params=pltpu.CompilerParams(vmem_limit_bytes=12 * 2**20),
        name="first",
    )(vel, strs, con)


def interior_rest(x, con, RB=64, L1=64, L2=128):
    _, R, C = con.shape
    hbm = pl.BlockSpec(memory_space=pltpu.HBM)
    vmem = pl.BlockSpec(memory_space=pltpu.VMEM)
    return pl.pallas_call(
        functools.partial(rest_kernel, RB=RB, L1=L1, L2=L2),
        in_specs=[vmem] * 2,
        out_specs=(vmem, hbm, hbm, vmem),
        out_shape=(sds(5, R, C), sds(2, R, C), sds(3, R, C), sds(2, 8, 128)),
        scratch_shapes=[pltpu.VMEM((C // 128, R + 2 * PAD, 128), F32)] * 8 + [pltpu.SemaphoreType.DMA(())],
        input_output_aliases={0: 0},
        compiler_params=pltpu.CompilerParams(vmem_limit_bytes=12 * 2**20),
        name="rest",
    )(x, con)


def per_device(velocity, stress, strength, ice_mass, wind_stress, current, ice_mask, open_water):
    args = (velocity, stress, strength, ice_mass, wind_stress, current, ice_mask, open_water)
    R, C = strength.shape
    hbm = pl.BlockSpec(memory_space=pltpu.HBM)
    vmem = pl.BlockSpec(memory_space=pltpu.VMEM)

    def limit(mib):
        return pltpu.CompilerParams(vmem_limit_bytes=mib * 2**20)

    def blocks(shape, where):
        return [pl.BlockSpec((v.shape[0],) * (v.ndim - 2) + shape, functools.partial(lambda nd, *g: (0,) * (nd - 2) + where(*g), v.ndim)) for v in args]

    edges = [pltpu.with_memory_space_constraint(v, pltpu.HBM) for v in args]
    own, xa, xb = pl.pallas_call(
        rows_kernel,
        grid=(1,),
        in_specs=blocks((8, C), lambda i: (0, 0)) + blocks((8, C), lambda i: (R // 8 - 1, 0)),
        out_specs=[pl.BlockSpec((NS, 16, C), lambda i: (0, 0, 0)), pl.BlockSpec((40, C), lambda i: (0, 0)), pl.BlockSpec((40, C), lambda i: (0, 0))],
        out_shape=[sds(NS, 16, C), sds(40, C), sds(40, C)],
        compiler_params=limit(6),
        name="row_edges",
    )(*edges, *edges)
    xa, xb, *args = lax.optimization_barrier((xa, xb, *args))
    xa, xb = exchange(xa, xb, "gx")
    con, cols = pl.pallas_call(
        load_kernel,
        in_specs=[vmem] * 8,
        out_specs=(vmem, vmem),
        out_shape=(sds(6, R, C), sds(16 * NS, R)),
        compiler_params=limit(16),
        name="load",
    )(*args)
    x = interior_first(args[0], args[1], con)
    cols, x = lax.optimization_barrier((cols, x))
    ya, yb, ext = pl.pallas_call(
        corners_kernel,
        in_specs=[vmem] * 3,
        out_specs=[vmem] * 3,
        out_shape=[sds(40, R + 128), sds(40, R + 128), sds(16 * NS, 128)],
        compiler_params=limit(6),
        name="corners",
    )(cols, xa, xb)
    ya, yb = exchange(ya, yb, "gy")
    _, nvel, nstr, isums = interior_rest(x, con)
    ND = lax.axis_size(ALL)
    rows_out, cols_out, msg = pl.pallas_call(
        functools.partial(strips_kernel, R=R, C=C),
        in_specs=[vmem] * 8,
        out_specs=(vmem, vmem, vmem),
        out_shape=(sds(5, 16, C), sds(5, 16, R), sds(ND, 128)),
        scratch_shapes=[
            pltpu.VMEM((NF, 24, C), F32),
            pltpu.VMEM((NF, 24, R + 128), F32),
        ],
        compiler_params=limit(12),
        name="strips",
    )(own, cols, ext, xa, xb, ya, yb, isums)
    parts = lax.all_to_all(msg, ALL, 0, 0, tiled=True)
    nvel, nstr = pl.pallas_call(
        merge_kernel,
        in_specs=[vmem] * 2 + [hbm] * 2,
        out_specs=(hbm, hbm),
        out_shape=(sds(2, R, C), sds(3, R, C)),
        scratch_shapes=[pltpu.VMEM((2, 5, R, 128), F32), pltpu.VMEM((2, 5, 8, C - 256), F32), pltpu.SemaphoreType.DMA((2, 2))],
        input_output_aliases={2: 0, 3: 1},
        compiler_params=limit(12),
        name="merge",
    )(rows_out, cols_out, nvel, nstr)
    cells = R * lax.axis_size("gx") * C * lax.axis_size("gy")
    smem = pl.BlockSpec(memory_space=pltpu.SMEM)
    residual, kinetic = pl.pallas_call(
        functools.partial(total_kernel, cells=cells),
        in_specs=[vmem],
        out_specs=(smem, smem),
        out_shape=(sds(1), sds(1)),
        compiler_params=limit(2),
        name="total",
    )(parts)
    return nvel, nstr, residual.reshape(()), kinetic.reshape(())


def solution(mesh):
    whole, plane = P(None, "gx", "gy"), P("gx", "gy")
    return jax.shard_map(
        per_device,
        mesh=mesh,
        in_specs=(whole, whole, plane, plane, whole, whole, plane, plane),
        out_specs=(whole, whole, P(), P()),
        check_vma=False,
    )
```

```python
import functools

import jax
import jax.numpy as jnp
from jax import lax
from jax.experimental import pallas as pl
from jax.experimental.pallas import tpu as pltpu
from jax.sharding import PartitionSpec as P

ITERS = 4
RELAX = 0.8
GROW = 1.0 / (1.0 + RELAX)
KAPPA = RELAX / (1.0 + RELAX)
PAD = 8
TAIL = 32
F32 = jnp.float32
(U_, V_, H1, H2, H12, K_, M8, FU, FV, CA, CB) = range(11)
NS = 9
NF = 11
ALL = ("gx", "gy")


def weight_of(mask, openw):
    return mask.astype(F32) * (1.0 - openw.astype(F32))


def consts(strength, mass, wind, cur, weight):
    return (KAPPA * strength) * weight, mass * 8.0, 4.0 * (wind[0] + cur[0]), 4.0 * (wind[1] + cur[1])


def coefs(m8, weight):
    a = m8 * 0.25 + 1.0
    b = m8 * 0.0375
    scale = (0.25 * weight) / (a * a + b * b)
    return a * scale, b * scale


def strain(u, v, um, vm):
    su = u + um
    du = u - um
    sv = v + vm
    dv = v - vm
    return su + dv, su - dv, du + sv, du - sv


def stress_rate(alpha, beta, gamma, alpha_m, beta_m, delta_m, k):
    d = alpha - beta_m
    t = beta - alpha_m
    s = gamma + delta_m
    q = d * d + 0.25 * (t * t + s * s) + 0.01
    r = lax.rsqrt(q)
    z = k * r
    z4 = 0.25 * z
    return z * (d - q * r), z4 * t, z4 * s


def mixes(h1, h2, h12):
    return h1 + h2, h1 - h2, h12


def spread(m, p):
    xs, xd = p[0] + m[0], p[2] - m[2]
    ys, yd = p[2] + m[2], p[1] - m[1]
    return xs + xd, xs - xd, ys + yd, ys - yd


def drift(u, v, fx, fy, m8, fu, fv, ca, cb):
    ru = m8 * u + (fx + fu)
    rv = m8 * v + (fy + fv)
    return ca * ru + cb * rv, ca * rv - cb * ru


def pair_rows(parts, high):
    half = lax.broadcasted_iota(jnp.int32, parts[0].shape, 0) < 4
    tiles = []
    for f in range(0, NS, 2):
        a = parts[f]
        b = parts[f + 1] if f + 1 < NS else jnp.zeros_like(a)
        if high:
            tiles.append(jnp.where(half, pltpu.roll(a, 4, 0), b))
        else:
            tiles.append(jnp.where(half, a, pltpu.roll(b, 4, 0)))
    return jnp.concatenate(tiles, 0)


def unpair(tiles, f, high):
    x = tiles[8 * (f // 2) : 8 * (f // 2) + 8]
    return x if (f % 2 == 1) == high else pltpu.roll(x, 4, 0)


def is_even(axis):
    return lax.axis_index(axis) % 2 == 0


def strip_fields(vel, strs, strength, mass, wind, cur, mask, openw):
    w = weight_of(mask[...], openw[...])
    k, m8, fu, fv = consts(strength[...], mass[...], (wind[0], wind[1]), (cur[0], cur[1]), w)
    return [vel[0], vel[1], strs[0], strs[1], 2.0 * strs[2], k, m8, fu, fv]


def rows_kernel(*refs):
    own, msg_a, msg_b = refs[16:]
    top = strip_fields(*refs[:8])
    bot = strip_fields(*refs[8:16])
    for f in range(NS):
        own[f, 0:8, :] = top[f]
        own[f, 8:16, :] = bot[f]
    low = pair_rows(top, False)
    high = pair_rows(bot, True)
    even = is_even("gx")
    msg_a[...] = jnp.where(even, high, low)
    msg_b[...] = jnp.where(even, low, high)


def load_kernel(vel, strs, strength, mass, wind, cur, mask, openw, x, cols):
    R, C = strength.shape

    def prepare(r0):
        rows = pl.ds(r0, 8)
        for t in range(C // 128):
            at = (rows, slice(128 * t, 128 * t + 128))
            w = weight_of(mask[at], openw[at])
            k, m8, fu, fv = consts(strength[at], mass[at], (wind[(0, *at)], wind[(1, *at)]), (cur[(0, *at)], cur[(1, *at)]), w)
            ca, cb = coefs(m8, w)
            for f, value in enumerate((k, m8, fu, fv, ca, cb)):
                x[(f, *at)] = value

    def body(i, carry):
        for n in range(4):
            prepare(pl.multiple_of(i * 32 + 8 * n, 8))
        return carry

    lax.fori_loop(0, R // 32, body, 0)
    lane = lax.broadcasted_iota(jnp.int32, (8, 128), 1)
    low = lane < 64
    fields = [(vel, 0), (vel, 1), (strs, 0), (strs, 1), (strs, 2)] + [(x, f - K_) for f in range(K_, NS)]

    def pack(p, carry):
        groups = ([], [])
        for g in range(16):
            rows = pl.ds(pl.multiple_of(p * 128 + 8 * g, 8), 8)
            packed = [None, None]
            for f, (ref, lead) in enumerate(fields):
                y = jnp.where(low, ref[lead, rows, 0:128], ref[lead, rows, C - 128 : C])
                if f == H12:
                    y = 2.0 * y
                if f:
                    y = pltpu.roll(y, 8 * f, 1)
                for side in range(2):
                    begin = 8 * (f - side) % 128
                    hit = (lane >= begin) & (lane < begin + 8)
                    packed[side] = y if packed[side] is None else jnp.where(hit, y, packed[side])
            for side in range(2):
                groups[side].append(packed[side])
        at = pl.ds(pl.multiple_of(p * 128, 128), 128)
        y = jnp.concatenate(groups[0], 0).T
        cols[0 : 8 * NS, at] = y[0 : 8 * NS]
        y = jnp.concatenate(groups[1], 0).T
        cols[8 * NS : 8 * NS + 8, at] = y[120:128]
        cols[8 * NS + 8 : 16 * NS, at] = y[0 : 8 * (NS - 1)]
        return carry

    lax.fori_loop(0, R // 128, pack, 0)


def corners_kernel(cols, xa, xb, ya, yb, ext):
    even = is_even("gx")
    a, b = xa[...], xb[...]
    top = jnp.where(even, b, a)
    bot = jnp.where(even, a, b)
    C = cols.shape[1]
    lane = lax.broadcasted_iota(jnp.int32, (8, 128), 1)
    strips = []
    for side in range(2):
        at = side * (C - 128)
        t = jnp.concatenate([top[:, at : at + 128], bot[:, at : at + 128], jnp.zeros((48, 128), F32)], 0).T
        t = t[120 * side : 120 * side + 8]
        own = []
        for f in range(NS):
            e = jnp.where(lane >= 124, pltpu.roll(t, 124 - 4 * f, 1), 0.0)
            e = jnp.where(lane < 4, pltpu.roll(t, 128 - 40 - 4 * f, 1), e)
            base = 8 * (NS * side + f)
            ext[base : base + 8, :] = e
            own.append(jnp.concatenate([cols[base : base + 8, :], e], 1))
        strips.append(pair_rows(own, side == 1))
    low, high = strips
    even = is_even("gy")
    ya[...] = jnp.where(even, high, low)
    yb[...] = jnp.where(even, low, high)


def sweep_subcycles(its, vel, strs, con, x, nvel, nstr, sums, tail, al, be, ga, de, tx, ty, nx, ny, sem, *, RB, L1, L2):
    R, C = x.shape[1:]
    NT = C // 128
    k, m8_, fu_, fv_, ca_, cb_ = range(6)
    zero = jnp.zeros((8, 128), F32)
    for t in range(NT):
        for ref in (al, be, de):
            ref[t, 0:PAD, :] = zero
        for ref in (tx, ty):
            ref[t, PAD + R : PAD + R + 8, :] = zero
    lane = lax.broadcasted_iota(jnp.int32, (8, 128), 1)
    row_in = lax.broadcasted_iota(jnp.int32, (8, 128), 0)
    first = lane == 0
    last = lane == 127

    def tile(t):
        return slice(128 * t, 128 * t + 128)

    def strain_rows(r0, src):
        own = pl.ds(r0, 8)
        rows = pl.ds(PAD + r0, 8)
        ru = rv = None
        for t in range(NT):
            u, v = src[0, own, tile(t)], src[1, own, tile(t)]
            qu, qv = pltpu.roll(u, 1, 1), pltpu.roll(v, 1, 1)
            um = jnp.where(first, ru, qu) if t else qu
            vm = jnp.where(first, rv, qv) if t else qv
            ru, rv = qu, qv
            al[t, rows, :], be[t, rows, :], ga[t, rows, :], de[t, rows, :] = strain(u, v, um, vm)

    def rate_rows(r0, it):
        own = pl.ds(r0, 8)
        rows = pl.ds(PAD + r0, 8)
        above = pl.ds(PAD + r0 - 1, 8)

        def emit(t, m, q, nq):
            p = [jnp.where(last, nq[i], q[i]) if nq else q[i] for i in range(3)]
            tx[t, rows, :], nx[t, rows, :], ty[t, rows, :], ny[t, rows, :] = spread(m, p)

        held = None
        for t in range(NT):
            d1, d2, d12 = stress_rate(al[t, rows, :], be[t, rows, :], ga[t, rows, :], al[t, above, :], be[t, above, :], de[t, above, :], con[k, own, tile(t)])
            if it:
                old = [x[f, own, tile(t)] for f in (H1, H2, H12)]
            else:
                old = [strs[f, own, tile(t)] for f in range(3)]
            h1 = old[0] * GROW + d1
            h2 = old[1] * GROW + d2
            h12 = old[2] * (GROW if it else 2.0 * GROW) + d12
            x[H1, own, tile(t)] = h1
            x[H2, own, tile(t)] = h2
            x[H12, own, tile(t)] = 0.5 * h12 if it == ITERS - 1 else h12
            m = mixes(h1, h2, h12)
            q = [pltpu.roll(v, 127, 1) for v in m]
            if held:
                emit(t - 1, *held, q)
            held = (m, q)
        emit(NT - 1, *held, None)

    def velocity_rows(r0, src, acc, may_start=False):
        own = pl.ds(r0, 8)
        rows = pl.ds(PAD + r0, 8)
        below = pl.ds(PAD + r0 + 1, 8)
        for t in range(NT):
            u, v, m8 = src[0, own, tile(t)], src[1, own, tile(t)], con[m8_, own, tile(t)]
            fx = tx[t, below, :] - nx[t, rows, :]
            fy = ty[t, below, :] - ny[t, rows, :]
            nu, nv = drift(u, v, fx, fy, m8, con[fu_, own, tile(t)], con[fv_, own, tile(t)], con[ca_, own, tile(t)], con[cb_, own, tile(t)])
            x[U_, own, tile(t)] = nu
            x[V_, own, tile(t)] = nv
            if acc is not None:
                keep = con[k, own, tile(t)] > 0.0
                if may_start if not isinstance(r0, int) else r0 == 0:
                    keep = keep & (row_in + r0 >= ITERS)
                if isinstance(r0, int) and r0 == R - 8:
                    keep = keep & (row_in < 8 - ITERS)
                if t == 0:
                    keep = keep & (lane >= ITERS)
                if t == NT - 1:
                    keep = keep & (lane < 128 - ITERS)
                cu, cv = nu - u, nv - v
                acc[2 * (t % 2)] += jnp.where(keep, cu * cu + cv * cv, 0.0)
                acc[2 * (t % 2) + 1] += jnp.where(keep, m8 * (nu * nu + nv * nv), 0.0)

    sent = [0]

    def send(end):
        rows = pl.ds(sent[0], end - sent[0])
        for f, (ref, lead) in enumerate(((nvel, 0), (nvel, 1), (nstr, 0), (nstr, 1), (nstr, 2))):
            pltpu.make_async_copy(x.at[f, rows], ref.at[lead, rows], sem).start()
        sent[0] = end

    acc = [zero] * 4
    peel = -(-L2 // RB) * RB
    for it in its:
        start = it == its[0]
        final = it == ITERS - 1
        src, before = (x if n > 0 else vel for n in (it, it - 1))
        for r in range(0, peel, 8):
            strain_rows(r, src)
            if r >= L1:
                rate_rows(r - L1, it)
            elif not start:
                rate_rows(R + r - L1, it - 1)
            if r >= L2:
                velocity_rows(r - L2, src, acc if final else None)
            elif not start:
                velocity_rows(R + r - L2, before, None)

        def body(j, acc):
            r0 = pl.multiple_of(j * RB, RB)
            acc = list(acc) if final else None
            for r in range(0, RB, 8):
                strain_rows(r0 + r, src)
                rate_rows(r0 + (r - L1), it)
                velocity_rows(r0 + (r - L2), src, acc, r == L2 % RB)
            return tuple(acc) if final else ()

        if not final:
            lax.fori_loop(peel // RB, R // RB, body, ())
            continue
        for j in range(peel // RB, R // RB, 2):
            acc = list(lax.fori_loop(j, min(j + 2, R // RB), body, tuple(acc)))
            send(min((j + 2) * RB, R) - L2)
    for r in range(0, L2, 8):
        if r < L1:
            rate_rows(R + r - L1, its[-1])
        velocity_rows(R + r - L2, src, acc if final else None)
        if final and (r + 8) % TAIL == 0 and r + 8 < L2:
            send(R - L2 + r + 8)
    if not final:
        return
    for f in range(5):
        tail[f] = x[f, R - TAIL : R, :]
    sums[0] = acc[0] + acc[2]
    sums[1] = acc[1] + acc[3]
    whole = x.at[:, pl.ds(0, R - TAIL)]
    pltpu.make_async_copy(whole, whole, sem).wait()


def first_kernel(vel, strs, con, x, *work, **kw):
    sweep_subcycles([0], vel, strs, con, x, None, None, None, None, *work, None, **kw)


def rest_kernel(x_in, con, x, nvel, nstr, sums, tail, *work, **kw):
    sweep_subcycles(list(range(1, ITERS)), None, None, con, x, nvel, nstr, sums, tail, *work, **kw)


def strip_begin(ref):
    w = jnp.where(ref[K_] > 0.0, 1.0, 0.0)
    ref[CA], ref[CB] = coefs(ref[M8], w)


def strip_subcycle(ref, rows_axis, keep=None):
    cols_axis = 1 - rows_axis
    back = lambda x, axis: pltpu.roll(x, 1, axis)
    ahead = lambda x, axis: pltpu.roll(x, x.shape[axis] - 1, axis)
    u, v = ref[U_], ref[V_]
    a, b, g, d = strain(u, v, back(u, cols_axis), back(v, cols_axis))
    d1, d2, d12 = stress_rate(a, b, g, back(a, rows_axis), back(b, rows_axis), back(d, rows_axis), ref[K_])
    h1 = ref[H1] * GROW + d1
    h2 = ref[H2] * GROW + d2
    h12 = ref[H12] * GROW + d12
    ref[H1], ref[H2], ref[H12] = h1, h2, h12
    m = mixes(h1, h2, h12)
    xt, xn, yt, yn = spread(m, [ahead(v, cols_axis) for v in m])
    fx = ahead(xt, rows_axis) - xn
    fy = ahead(yt, rows_axis) - yn
    m8 = ref[M8]
    nu, nv = drift(u, v, fx, fy, m8, ref[FU], ref[FV], ref[CA], ref[CB])
    ref[U_], ref[V_] = nu, nv
    if keep is None:
        return None
    cu, cv = nu - u, nv - v
    inside = keep & (ref[K_] > 0.0)
    pair = (jnp.where(inside, cu * cu + cv * cv, 0.0), jnp.where(inside, m8 * (nu * nu + nv * nv), 0.0))
    return [sum(p[i : i + 8, j : j + 128] for i in range(0, p.shape[0], 8) for j in range(0, p.shape[1], 128)) for p in pair]


def strips_kernel(own, cols, ext, xa, xb, ya, yb, isums, rows_out, cols_out, msg, rs, cs, *, R, C):
    even = is_even("gx")
    a, b = xa[...], xb[...]
    top = jnp.where(even, b, a)
    bot = jnp.where(even, a, b)
    even = is_even("gy")
    a, b = ya[...], yb[...]
    left = jnp.where(even, b, a)
    right = jnp.where(even, a, b)
    half_r = lax.broadcasted_iota(jnp.int32, (8, C), 0) < 4
    half_c = lax.broadcasted_iota(jnp.int32, (8, R + 128), 0) < 4
    for f in range(NS):
        rs[f, 0:8, :] = jnp.where(half_r, unpair(bot, f, False), unpair(top, f, True))
        rs[f, 8:24, :] = own[f]
        cs[f, 0:8, :] = jnp.where(half_c, unpair(right, f, False), unpair(left, f, True))
        for side in range(2):
            base = 8 * (NS * side + f)
            cs[f, 8 + 8 * side : 16 + 8 * side, 0:R] = cols[base : base + 8, :]
            cs[f, 8 + 8 * side : 16 + 8 * side, R : R + 128] = ext[base : base + 8, :]

    def rim(shape):
        sub = lax.broadcasted_iota(jnp.int32, shape, 0)
        return ((sub >= 8) & (sub < 12)) | ((sub >= 20) & (sub < 24)), lax.broadcasted_iota(jnp.int32, shape, 1)

    strip_begin(rs)
    strip_begin(cs)

    def body(_, carry):
        strip_subcycle(rs, 0)
        strip_subcycle(cs, 1)
        return carry

    lax.fori_loop(0, ITERS - 1, body, 0)
    band, lane = rim(rs.shape[1:])
    row_sums = strip_subcycle(rs, 0, band & (lane >= ITERS) & (lane < C - ITERS))
    band, lane = rim(cs.shape[1:])
    col_sums = strip_subcycle(cs, 1, band & (lane < R))
    lane = lax.broadcasted_iota(jnp.int32, msg.shape, 1)
    totals = [jnp.sum(isums[n] + row_sums[n] + col_sums[n]) for n in range(2)]
    msg[...] = jnp.where(lane == 0, totals[0], jnp.where(lane == 1, totals[1], 0.0))
    for f in range(5):
        half = 0.5 if f == H12 else 1.0
        rows_out[f] = half * rs[f, 8:24, :]
        cols_out[f] = half * cs[f, 8:24, 0:R]


def merge_kernel(rows_in, cols_in, tail, nvel_in, nstr_in, nvel, nstr, edge, mid, sem):
    R, C = nvel.shape[1:]
    outs = ((nvel, 0), (nvel, 1), (nstr, 0), (nstr, 1), (nstr, 2))
    inner = pl.ds(128, C - 256)

    def places(f):
        ref, lead = outs[f]
        full = ref.at[lead]
        return (
            (full.at[:, pl.ds(0, 128)], edge.at[0, f]),
            (full.at[:, pl.ds(C - 128, 128)], edge.at[1, f]),
            (full.at[pl.ds(0, 8), inner], mid.at[0, f]),
            (full.at[pl.ds(R - 8, 8), inner], mid.at[1, f]),
        )

    for f in range(5):
        for n, (there, here) in enumerate(places(f)):
            pltpu.make_async_copy(there, here, sem.at[0, n // 2]).start()
    held = tail.at[:, pl.ds(0, TAIL - 8), inner]
    for f, (ref, lead) in enumerate(outs):
        pltpu.make_async_copy(held.at[f], ref.at[lead, pl.ds(R - TAIL, TAIL - 8), inner], sem.at[2, 0]).start()
    for n, buf in enumerate((edge, mid)):
        pltpu.make_async_copy(buf, buf, sem.at[0, n]).wait()
    for f in range(5):
        mid[1, f] = tail[f, TAIL - 8 : TAIL, 128 : C - 128]
        edge[0, f, R - TAIL : R, :] = tail[f, :, 0:128]
        edge[1, f, R - TAIL : R, :] = tail[f, :, C - 128 : C]
    low = lax.broadcasted_iota(jnp.int32, (8, C), 0) < 4
    for f in range(5):
        for part in range(2):
            x = rows_in[f, 8 * part : 8 * part + 8, :]
            keep = ~low if part == 0 else low
            rows = slice(part * (R - 8), part * (R - 8) + 8)
            mid[part, f] = jnp.where(keep[:, 128 : C - 128], mid[part, f], x[:, 128 : C - 128])
            for side in range(2):
                at = slice(side * (C - 128), side * (C - 128) + 128)
                edge[side, f, rows, :] = jnp.where(keep[:, at], edge[side, f, rows, :], x[:, at])
    lane = lax.broadcasted_iota(jnp.int32, (128, 128), 1)
    for c in range(R // 128):
        rows = slice(c * 128, c * 128 + 128)
        parts = [cols_in[f, 8 * side : 8 * side + 8, rows] for side in range(2) for f in range(5)]
        x = jnp.concatenate(parts + [jnp.zeros((48, 128), F32)], 0).T
        for side in range(2):
            for f in range(5):
                shift = (120 * side - 8 * (5 * side + f)) % 128
                y = pltpu.roll(x, shift, 1) if shift else x
                hit = lane >= 124 if side else lane < 4
                edge[side, f, rows, :] = jnp.where(hit, y, edge[side, f, rows, :])
    for f in range(5):
        for n, (there, here) in enumerate(places(f)):
            pltpu.make_async_copy(here, there, sem.at[1, n // 2]).start()
    for n, buf in enumerate((edge, mid)):
        pltpu.make_async_copy(buf, buf, sem.at[1, n]).wait()
    pltpu.make_async_copy(held, held, sem.at[2, 0]).wait()


def total_kernel(parts, residual, kinetic, *, cells):
    lane = lax.broadcasted_iota(jnp.int32, parts.shape, 1)
    x = parts[...]
    residual[0] = jnp.sum(jnp.where(lane == 0, x, 0.0)) * (1.0 / cells)
    kinetic[0] = jnp.sum(jnp.where(lane == 1, x, 0.0)) * (0.0625 / cells)


def swaps(count):
    first = [(i, i ^ 1) for i in range(count)]
    second = [(i, i + 1) for i in range(1, count - 1, 2)] + [(i + 1, i) for i in range(1, count - 1, 2)]
    return first, second


def exchange(a, b, axis):
    first, second = swaps(lax.axis_size(axis))
    return lax.ppermute(a, axis, first), lax.ppermute(b, axis, second)


def sds(*shape):
    return jax.ShapeDtypeStruct(shape, F32)


def interior_first(vel, strs, con, RB=64, L1=64, L2=128):
    _, R, C = con.shape
    vmem = pl.BlockSpec(memory_space=pltpu.VMEM)
    return pl.pallas_call(
        functools.partial(first_kernel, RB=RB, L1=L1, L2=L2),
        in_specs=[vmem] * 3,
        out_specs=vmem,
        out_shape=sds(5, R, C),
        scratch_shapes=[pltpu.VMEM((C // 128, R + 2 * PAD, 128), F32)] * 8,
        compiler_params=pltpu.CompilerParams(vmem_limit_bytes=12 * 2**20),
        name="first",
    )(vel, strs, con)


def interior_rest(x, con, RB=64, L1=64, L2=128):
    _, R, C = con.shape
    hbm = pl.BlockSpec(memory_space=pltpu.HBM)
    vmem = pl.BlockSpec(memory_space=pltpu.VMEM)
    return pl.pallas_call(
        functools.partial(rest_kernel, RB=RB, L1=L1, L2=L2),
        in_specs=[vmem] * 2,
        out_specs=(vmem, hbm, hbm, vmem, vmem),
        out_shape=(sds(5, R, C), sds(2, R, C), sds(3, R, C), sds(2, 8, 128), sds(5, TAIL, C)),
        scratch_shapes=[pltpu.VMEM((C // 128, R + 2 * PAD, 128), F32)] * 8 + [pltpu.SemaphoreType.DMA(())],
        input_output_aliases={0: 0},
        compiler_params=pltpu.CompilerParams(vmem_limit_bytes=12 * 2**20),
        name="rest",
    )(x, con)


def per_device(velocity, stress, strength, ice_mass, wind_stress, current, ice_mask, open_water):
    args = (velocity, stress, strength, ice_mass, wind_stress, current, ice_mask, open_water)
    R, C = strength.shape
    hbm = pl.BlockSpec(memory_space=pltpu.HBM)
    vmem = pl.BlockSpec(memory_space=pltpu.VMEM)

    def limit(mib):
        return pltpu.CompilerParams(vmem_limit_bytes=mib * 2**20)

    def blocks(shape, where):
        return [pl.BlockSpec((v.shape[0],) * (v.ndim - 2) + shape, functools.partial(lambda nd, *g: (0,) * (nd - 2) + where(*g), v.ndim)) for v in args]

    edges = [pltpu.with_memory_space_constraint(v, pltpu.HBM) for v in args]
    own, xa, xb = pl.pallas_call(
        rows_kernel,
        grid=(1,),
        in_specs=blocks((8, C), lambda i: (0, 0)) + blocks((8, C), lambda i: (R // 8 - 1, 0)),
        out_specs=[pl.BlockSpec((NS, 16, C), lambda i: (0, 0, 0)), pl.BlockSpec((40, C), lambda i: (0, 0)), pl.BlockSpec((40, C), lambda i: (0, 0))],
        out_shape=[sds(NS, 16, C), sds(40, C), sds(40, C)],
        compiler_params=limit(6),
        name="row_edges",
    )(*edges, *edges)
    xa, xb, *args = lax.optimization_barrier((xa, xb, *args))
    xa, xb = exchange(xa, xb, "gx")
    con, cols = pl.pallas_call(
        load_kernel,
        in_specs=[vmem] * 8,
        out_specs=(vmem, vmem),
        out_shape=(sds(6, R, C), sds(16 * NS, R)),
        compiler_params=limit(16),
        name="load",
    )(*args)
    x = interior_first(args[0], args[1], con)
    cols, x = lax.optimization_barrier((cols, x))
    ya, yb, ext = pl.pallas_call(
        corners_kernel,
        in_specs=[vmem] * 3,
        out_specs=[vmem] * 3,
        out_shape=[sds(40, R + 128), sds(40, R + 128), sds(16 * NS, 128)],
        compiler_params=limit(6),
        name="corners",
    )(cols, xa, xb)
    ya, yb = exchange(ya, yb, "gy")
    _, nvel, nstr, isums, tail = interior_rest(x, con)
    ND = lax.axis_size(ALL)
    rows_out, cols_out, msg = pl.pallas_call(
        functools.partial(strips_kernel, R=R, C=C),
        in_specs=[vmem] * 8,
        out_specs=(vmem, vmem, vmem),
        out_shape=(sds(5, 16, C), sds(5, 16, R), sds(ND, 128)),
        scratch_shapes=[
            pltpu.VMEM((NF, 24, C), F32),
            pltpu.VMEM((NF, 24, R + 128), F32),
        ],
        compiler_params=limit(12),
        name="strips",
    )(own, cols, ext, xa, xb, ya, yb, isums)
    parts = lax.all_to_all(msg, ALL, 0, 0, tiled=True)
    nvel, nstr = pl.pallas_call(
        merge_kernel,
        in_specs=[vmem] * 3 + [hbm] * 2,
        out_specs=(hbm, hbm),
        out_shape=(sds(2, R, C), sds(3, R, C)),
        scratch_shapes=[pltpu.VMEM((2, 5, R, 128), F32), pltpu.VMEM((2, 5, 8, C - 256), F32), pltpu.SemaphoreType.DMA((3, 2))],
        input_output_aliases={3: 0, 4: 1},
        compiler_params=limit(12),
        name="merge",
    )(rows_out, cols_out, tail, nvel, nstr)
    cells = R * lax.axis_size("gx") * C * lax.axis_size("gy")
    smem = pl.BlockSpec(memory_space=pltpu.SMEM)
    residual, kinetic = pl.pallas_call(
        functools.partial(total_kernel, cells=cells),
        in_specs=[vmem],
        out_specs=(smem, smem),
        out_shape=(sds(1), sds(1)),
        compiler_params=limit(2),
        name="total",
    )(parts)
    return nvel, nstr, residual.reshape(()), kinetic.reshape(())


def solution(mesh):
    whole, plane = P(None, "gx", "gy"), P("gx", "gy")
    return jax.shard_map(
        per_device,
        mesh=mesh,
        in_specs=(whole, whole, plane, plane, whole, whole, plane, plane),
        out_specs=(whole, whole, P(), P()),
        check_vma=False,
    )
```
